32 devices in a mesh: grp: 2 (over y), brick: 4 (over z), vec: 2 (over x), sub: 2 (over core).
Axes of the slice: x: 2, y: 2, z: 4, core: 2. Of those that a mesh axis runs over, the one named last changes fastest.
Arguments:
- vectors: float32 [128, 3, 2, 16384], P(('vec', 'sub'), None, None, ('grp', 'brick')), parts along dimension 3, may hold values from -6 to 6
- gauge_links: float32 [3, 3, 3, 2, 16384], P(None, None, None, None, ('grp', 'brick')), parts along dimension 4, may hold values from -1 to 1, as said below
- momenta: int32 [27, 3], replicated, may hold values from -3 to 3
Outputs:
- elementals: float32 [128, 54, 2, 128], P(('vec', 'sub'), 'grp', None, 'brick'), parts along dimension 1
The draws below stay inside these ranges and needn't reach their ends.
There are 2 independent parts, one for each index of `grp`. The reference program is written for one: setup_inputs(seed, part) draws one part's arguments, and reference() takes and returns one part's arrays. A program takes and returns all parts, laid end to end along the dimension named above; an argument that names none is the same for every part. Nothing has to cross between parts.
Inputs may be any that keep to these rules, and one draw needn't show every extreme that they name: Each gauge_links[mu, :, :, :, s] is a unitary 3x3 complex matrix.
All inputs are finite; a program needn't handle non-finite values.
Results may differ from the reference program's by a relative error of at most 0.0049.
Values may be sent and summed in bfloat16 or wider, within the bound.
A program may use at most 128 MiB of HBM per device.

```python
import math
import jax
import jax.numpy as jnp
from jax import lax

NV = 128
P_SIZE = 27
LY = 64
LZ = 8
ITERS = 2
NX = 16
SITES = 8192


def inner_product(first, second):
    real_part = jnp.sum(first[:, :, 0] * second[:, :, 0] + first[:, :, 1] * second[:, :, 1], axis=1)
    imag_part = jnp.sum(first[:, :, 0] * second[:, :, 1] - first[:, :, 1] * second[:, :, 0], axis=1)
    return (real_part[:, None], imag_part[:, None])


def remove_along(first, second):
    real_part, imag_part = inner_product(first, second)
    new_real = second[:, :, 0] - (real_part * first[:, :, 0] - imag_part * first[:, :, 1])
    new_imag = second[:, :, 1] - (real_part * first[:, :, 1] + imag_part * first[:, :, 0])
    return jnp.stack([new_real, new_imag], axis=2)


def normalize(matrix_row):
    length = jnp.sum(matrix_row * matrix_row, axis=(1, 2))
    return matrix_row * jax.lax.rsqrt(length + 1e-06)[:, None, None, :]


def draw_gauge_links(key, part):
    noise = jax.random.normal(jax.random.fold_in(key, 7), (3, 3, 3, 2, SITES), jnp.float32)
    first = normalize(noise[:, 0])
    second = normalize(remove_along(first, noise[:, 1]))
    third = remove_along(second, remove_along(first, noise[:, 2]))
    third = normalize(third)
    return jnp.stack([first, second, third], axis=1)


def place_ends(values, own_key, least, largest):
    place = [jax.random.randint(jax.random.fold_in(own_key, axis), (), 0, length) for axis, length in enumerate(values.shape)]
    widest = values.shape.index(max(values.shape))
    next_to = place[:widest] + [(place[widest] + 1) % values.shape[widest]] + place[widest + 1:]
    return values.at[tuple(place)].set(least).at[tuple(next_to)].set(largest)


def steps_of(rng, shape, cuts, smallest, top_value):
    loudness, own = 1.0, jax.random.fold_in(rng, 6)
    for position, parts in cuts:
        heights = jnp.exp(jax.random.uniform(jax.random.fold_in(own, position), (parts,), jnp.float32, smallest / len(cuts), top_value / len(cuts)))
        loudness = loudness * jnp.repeat(heights, shape[position] // parts).reshape([-1 if axis == position else 1 for axis in range(len(shape))])
    return loudness


def scatter_about(key, shape, width, reach, cuts=(), held_as=jnp.bfloat16):
    result = width * jax.random.normal(key, shape, jnp.float32)
    if cuts:
        result = result * steps_of(key, shape, cuts, -0.22, 0.18)
    return jnp.clip(result, -reach, reach).astype(held_as)


def setup_inputs(seed: int = 0, part: int = 0) -> dict:
    keys = jax.random.split(jax.random.key(seed), 4)
    part_keys = jax.random.split(jax.random.fold_in(keys[3], part), 4)
    vectors = scatter_about(part_keys[0], (NV, 3, 2, SITES), 1.0, 6.0, ((0, 4), (3, 4)), jnp.float32)
    gauge_links = draw_gauge_links(jax.random.fold_in(jax.random.fold_in(keys[3], part), 71), part)
    momenta = place_ends(jax.random.randint(keys[2], (P_SIZE, 3), -3, 4), jax.random.fold_in(keys[2], 1), -3, 3).astype(jnp.int32)
    return {"vectors": vectors, "gauge_links": gauge_links, "momenta": momenta}


KAPPA = 0.125


def matrix_apply(matrix, source):
    matrix_real = matrix[:, :, 0][None]
    matrix_imag = matrix[:, :, 1][None]
    source_real = source[:, None, :, 0]
    source_imag = source[:, None, :, 1]
    real_part = jnp.sum(matrix_real * source_real - matrix_imag * source_imag, axis=2)
    imag_part = jnp.sum(matrix_real * source_imag + matrix_imag * source_real, axis=2)
    return jnp.stack([real_part, imag_part], axis=2)


def adjoint(matrix):
    return jnp.stack([jnp.swapaxes(matrix[:, :, 0], 0, 1), -jnp.swapaxes(matrix[:, :, 1], 0, 1)], axis=2)


def smear_step(field, gauge):
    total = None
    for direction in range(3):
        axis = 3 + direction
        forward = matrix_apply(gauge[direction], jnp.roll(field, -1, axis=axis))
        behind = adjoint(jnp.roll(gauge[direction], 1, axis=axis))
        backward = matrix_apply(behind, jnp.roll(field, 1, axis=axis))
        term = forward + backward
        total = term if total is None else total + term
    return field + KAPPA * (total - 6.0 * field)


def reference(vectors, gauge_links, momenta):
    field = vectors.reshape((NV, 3, 2, NX, LY, LZ))
    gauge = gauge_links.reshape((3, 3, 3, 2, NX, LY, LZ))
    for step in range(ITERS):
        field = smear_step(field, gauge)
    smeared_low = field.reshape((NV, 3, 2, SITES)).astype(jnp.bfloat16)
    smeared_wide = lax.optimization_barrier(smeared_low).astype(jnp.float32)
    raw_wide = lax.optimization_barrier(vectors.astype(jnp.bfloat16)).astype(jnp.float32)
    right = smeared_wide.reshape((NV, 6 * SITES))
    site = jnp.arange(SITES, dtype=jnp.int32)
    layer_index = site // (LY * LZ)
    column_index = (site // LZ) % LY
    depth_index = site % LZ

    def one_momentum(triple):
        fraction = (jnp.mod(triple[0] * layer_index, NX).astype(jnp.float32) / NX
                    + jnp.mod(triple[1] * column_index, LY).astype(jnp.float32) / LY
                    + jnp.mod(triple[2] * depth_index, LZ).astype(jnp.float32) / LZ)
        angle = (2.0 * math.pi) * fraction
        cosine = jnp.cos(angle)
        sine = jnp.sin(angle)
        real_part = raw_wide[:, :, 0] * cosine - raw_wide[:, :, 1] * sine
        imag_part = raw_wide[:, :, 0] * sine + raw_wide[:, :, 1] * cosine
        phased = jnp.stack([real_part, imag_part], axis=2).astype(jnp.bfloat16)
        phased = lax.optimization_barrier(phased).astype(jnp.float32)
        turned = jnp.stack([-phased[:, :, 1], phased[:, :, 0]], axis=2)
        left = jnp.concatenate([phased.reshape((NV, 6 * SITES)), turned.reshape((NV, 6 * SITES))], axis=0)
        product = lax.dot_general(left, right, (((1,), (1,)), ((), ())),
                                  precision=lax.Precision.HIGHEST, preferred_element_type=jnp.float32)
        return product.reshape((2, NV, NV))

    blocks = lax.map(one_momentum, momenta)
    scale = (3.0 * SITES) ** -0.5
    return jnp.transpose(blocks, (2, 0, 1, 3)) * scale
```

```python
import functools
import math

import jax
import jax.numpy as jnp
from jax import lax
from jax.experimental import pallas as pl
from jax.experimental.pallas import tpu as pltpu
from jax.sharding import PartitionSpec as P

LY = 64
LZ = 8
ITERS = 2


KAPPA = 0.125


def from_behind(array, axis, by):
    peers = lax.axis_size(axis)
    return lax.ppermute(array, axis, [(i, (i + by) % peers) for i in range(peers)])


def padded_2(array, sides, width):
    for axis, dim in sides:
        peers, length = (lax.axis_size(axis), array.shape[dim])
        up = [(i, (i + 1) % peers) for i in range(peers)]
        down = [(j, i) for i, j in up]
        last = lax.slice_in_dim(array, length - width, length, axis=dim)
        initial = lax.slice_in_dim(array, 0, width, axis=dim)
        before = lax.ppermute(last, axis, up)
        after = lax.ppermute(initial, axis, down)
        array = jnp.concatenate([before, array, after], axis=dim)
    return array


def matrix_apply(matrix, source):
    matrix_real = matrix[:, :, 0][None]
    matrix_imag = matrix[:, :, 1][None]
    source_real = source[:, None, :, 0]
    source_imag = source[:, None, :, 1]
    real_part = jnp.sum(matrix_real * source_real - matrix_imag * source_imag, axis=2)
    imag_part = jnp.sum(matrix_real * source_imag + matrix_imag * source_real, axis=2)
    return jnp.stack([real_part, imag_part], axis=2)


def adjoint(matrix):
    return jnp.stack(
        [jnp.swapaxes(matrix[:, :, 0], 0, 1), -jnp.swapaxes(matrix[:, :, 1], 0, 1)], axis=2
    )


def step_depth(values, offset):
    depth_index = lax.iota(jnp.int32, values.shape[-1]) % LZ
    if offset > 0:
        return jnp.where(
            depth_index == LZ - 1, jnp.roll(values, LZ - 1, -1), jnp.roll(values, -1, -1)
        )
    return jnp.where(depth_index == 0, jnp.roll(values, 1 - LZ, -1), jnp.roll(values, 1, -1))


def step_column(values, offset):
    plane = LY * LZ
    column_index = lax.iota(jnp.int32, values.shape[-1]) // LZ % LY
    if offset > 0:
        return jnp.where(
            column_index == LY - 1, jnp.roll(values, plane - LZ, -1), jnp.roll(values, -LZ, -1)
        )
    return jnp.where(column_index == 0, jnp.roll(values, LZ - plane, -1), jnp.roll(values, LZ, -1))


def laplace_step(center, ahead, behind, here_links, back_links):
    forward = matrix_apply(here_links[0], ahead)
    backward = matrix_apply(adjoint(back_links), behind)
    total = forward + backward
    for direction, stepper in ((1, step_column), (2, step_depth)):
        forward = matrix_apply(here_links[direction], stepper(center, 1))
        backward = matrix_apply(adjoint(stepper(here_links[direction], -1)), stepper(center, -1))
        total = total + (forward + backward)
    return center + KAPPA * (total - 6.0 * center)


def shards(vectors, gauge_links, momenta):
    plane = LY * LZ
    local_sites = vectors.shape[3]
    raw_low = vectors.astype(jnp.bfloat16)
    field = vectors
    x_links = gauge_links[0]
    rim = from_behind(x_links[..., local_sites - plane :], "brick", 1)
    back_links = jnp.concatenate([rim, x_links[..., : local_sites - plane]], axis=3)
    for step in range(ITERS):
        padded = padded_2(field, (("brick", 3),), plane)
        field = laplace_step(
            padded[..., plane : plane + local_sites],
            padded[..., 2 * plane :],
            padded[..., :local_sites],
            gauge_links,
            back_links,
        )
    smeared_low = field.astype(jnp.bfloat16)
    raw_sites, smeared_sites = (
        lax.all_to_all(raw_low, ("vec", "sub"), split_axis=3, concat_axis=0, tiled=True),
        lax.all_to_all(smeared_low, ("vec", "sub"), split_axis=3, concat_axis=0, tiled=True),
    )
    groups = lax.axis_size(("vec", "sub"))
    total_vec = raw_sites.shape[0]
    width = raw_sites.shape[3]
    total_x = lax.axis_size("brick") * (local_sites // plane)
    first_site = lax.axis_index("brick") * local_sites + lax.axis_index(("vec", "sub")) * width
    site = first_site + lax.iota(jnp.int32, width)
    layer_index = (site // plane)[None]
    column_index = (site // LZ % LY)[None]
    depth_index = (site % LZ)[None]
    fraction = (
        jnp.mod(momenta[:, 0:1] * layer_index, total_x).astype(jnp.float32) / total_x
        + jnp.mod(momenta[:, 1:2] * column_index, LY).astype(jnp.float32) / LY
        + jnp.mod(momenta[:, 2:3] * depth_index, LZ).astype(jnp.float32) / LZ
    )
    angle = 2.0 * math.pi * fraction
    cosines = jnp.cos(angle)
    sines = jnp.sin(angle)
    right = smeared_sites.reshape((total_vec, 6 * width))
    scale = (3.0 * total_x * plane) ** (-0.5)

    def one_momentum(angles):
        cosine, sine = angles
        real_part = raw_sites[:, :, 0] * cosine - raw_sites[:, :, 1] * sine
        imag_part = raw_sites[:, :, 0] * sine + raw_sites[:, :, 1] * cosine
        phased = jnp.stack([real_part, imag_part], axis=2).astype(jnp.bfloat16)
        turned = jnp.stack([-phased[:, :, 1], phased[:, :, 0]], axis=2)
        left = jnp.concatenate(
            [
                phased.reshape((lax.axis_size(("vec", "sub")) * (total_vec // groups), 6 * width)),
                turned.reshape((lax.axis_size(("vec", "sub")) * (total_vec // groups), 6 * width)),
            ],
            axis=0,
        )
        product = lax.dot_general(
            left, right, (((1,), (1,)), ((), ())), preferred_element_type=jnp.float32
        )
        return product.reshape(
            (2, lax.axis_size(("vec", "sub")) * (total_vec // groups), total_vec)
        )

    blocks = lax.map(one_momentum, (cosines, sines))
    shares = lax.psum_scatter(
        jnp.transpose(blocks, (2, 0, 1, 3)) * scale, ("vec", "sub"), scatter_dimension=0, tiled=True
    )
    return lax.psum_scatter(shares, "brick", scatter_dimension=3, tiled=True)


def fused_kernel(plan, mom_ref, v_ref, g_ref, out_ref, *scratch):
    (vst, gst, field, table, moved, right, smeared, left0, left1, cosb, sinb, total, obuf, relay,
     rx, halo, hsend, lsend, lrecv, load_sem, halo_sem, link_sem, raw_sem, out_sem, last_sem) = scratch
    planes, rows, count, bricks, per, blocks_q, scale = plan
    plane = LY * LZ
    tiles = plane // 128
    all_tiles = planes * tiles
    f32, low = jnp.float32, jnp.bfloat16
    wide = 2 * plane
    last = planes - 1
    inner = list(range(1, last))
    outer = [0, last]
    position = {t: i for i, t in enumerate(inner + outer)}
    cut = len(inner) * 3 * wide
    span = planes * 3 * wide
    blocks = rows // 8
    half_blocks = blocks // 2
    trips = half_blocks * tiles
    b, v, s = (lax.axis_index(a) for a in ("brick", "vec", "sub"))
    left = (left0, left1)

    def remote(src, dst, sems, **ids):
        return pltpu.make_async_remote_copy(
            src_ref=src, dst_ref=dst, send_sem=sems.at[0], recv_sem=sems.at[1],
            device_id=ids, device_id_type=pl.DeviceIdType.MESH,
        )

    loads = {}
    for t in outer + inner:
        loads[t] = pltpu.make_async_copy(v_ref.at[:, t], vst.at[t], load_sem.at[t])
        loads[t].start()
    load_links = pltpu.make_async_copy(g_ref, gst.at[pl.ds(0, 54 * all_tiles)], load_sem.at[planes])
    load_links.start()
    barrier = pltpu.get_barrier_semaphore()
    for db in range(bricks):
        for ds in range(2):
            if db or ds:
                pl.semaphore_signal(
                    barrier, inc=1, device_id={"brick": (b + db) % bricks, "sub": (s + ds) % 2},
                    device_id_type=pl.DeviceIdType.MESH,
                )
    pl.semaphore_signal(
        barrier, inc=1, device_id={"vec": 1 - v}, device_id_type=pl.DeviceIdType.MESH
    )

    def unpack(t):
        flat = vst.at[t].reshape(rows * 3 * tiles * 2, 128)
        step = 3 * tiles * 2
        for c in range(3):
            for first in range(0, rows, 16):
                for part in range(2):
                    for lane in range(tiles):
                        start = first * step + c * tiles * 2 + lane * 2 + part
                        at = part * plane + lane * 128
                        pair = [flat[pl.ds(start + h * 8 * step, 8, stride=step), :] for h in range(2)]
                        for h in range(2):
                            field[0, t + 1, c, first + 8 * h : first + 8 * h + 8, at : at + 128] = pair[h]
                        k = (position[t] * 3 + c) * wide + at
                        right[first : first + 16, k : k + 128] = jnp.concatenate(pair, axis=0).astype(low)

    def link_rows(t, part, group):
        return jnp.concatenate(
            [
                gst[pl.ds(group * 16 * all_tiles + (t * tiles + lane) * 2 + part, 8, stride=2 * all_tiles), :]
                for lane in range(tiles)
            ],
            axis=1,
        ) * KAPPA

    for t in outer:
        loads[t].wait()
        unpack(t)
    load_links.wait()
    for part in range(2):
        both = jnp.concatenate([link_rows(last, part, 0), link_rows(last, part, 1)], axis=0)
        lsend[16 * part : 16 * part + 16, :] = both.astype(low)
    pl.semaphore_wait(barrier, 2 * bricks)
    up, down = (b + 1) % bricks, (b + bricks - 1) % bricks

    def halos(step, low_src, high_src):
        return (
            remote(high_src, halo.at[step, 0], halo_sem.at[step, 0], brick=up),
            remote(low_src, halo.at[step, 1], halo_sem.at[step, 1], brick=down),
        )

    def own(t):
        return right.at[0:rows, position[t] * 3 * wide : (position[t] + 1) * 3 * wide]

    first_halos = halos(0, own(0), own(last))
    links_up = remote(lsend, lrecv, link_sem, brick=up)
    links_up.start()
    for copy in first_halos:
        copy.start()
    for t in inner:
        loads[t].wait()
        unpack(t)
    parts = (slice(0, cut), slice(cut, span))
    unit = 2 * rows

    def raw_copy(index, from_slot, to_slot, ks, **ids):
        return remote(
            right.at[from_slot * unit : from_slot * unit + rows, ks],
            right.at[to_slot * unit : to_slot * unit + rows, ks],
            raw_sem.at[index], **ids,
        )

    across = [raw_copy(i, 0, 2, parts[i], vec=1 - v) for i in range(2)]
    beside = raw_copy(2, 0, 1, slice(0, span), sub=1 - s)
    onward = [raw_copy(3 + i, 2, 3, parts[i], sub=1 - s) for i in range(2)]
    for copy in across + [beside]:
        copy.start()

    depth_wide = lax.broadcasted_iota(jnp.int32, (8, plane), 1) % LZ
    depth = lax.broadcasted_iota(jnp.int32, (8, 128), 1) % LZ

    def spread(t, carry):
        for part in range(2):
            for group in range(4):
                here = link_rows(t, part, group)
                if group > 0:
                    by = pltpu.roll(here, LZ, 1)
                    bz = jnp.where(
                        depth_wide == 0, pltpu.roll(here, plane - (LZ - 1), 1), pltpu.roll(here, 1, 1)
                    )
                for j in range(min(8, 27 - 8 * group)):
                    index = group * 8 + j
                    row = jnp.broadcast_to(here[j : j + 1], (8, plane))
                    table[t, index * 2 + part] = row
                    if index < 9:
                        table[t + 1, 54 + index * 2 + part] = row
                    else:
                        back = by if index < 18 else bz
                        table[t, 54 + index * 2 + part] = jnp.broadcast_to(back[j : j + 1], (8, plane))
        return carry

    lax.fori_loop(0, planes, spread, 0)

    def phases(q, carry):
        n = [mom_ref[d, jnp.minimum(q, count - 1)].astype(f32) for d in range(3)]
        for group in range(0, all_tiles, 8):
            height = min(8, all_tiles - group)
            site = (
                lax.broadcasted_iota(jnp.int32, (height, 128), 0) * 128
                + lax.broadcasted_iota(jnp.int32, (height, 128), 1)
                + group * 128
            )
            x = (site // plane + b * planes).astype(f32)
            y = (site // LZ % LY).astype(f32)
            z = (site % LZ).astype(f32)
            turns = n[0] * x / (bricks * planes) + n[1] * y / LY + n[2] * z / LZ
            angle = (2.0 * math.pi) * (turns - jnp.round(turns))
            cosine, sine = jnp.cos(angle), jnp.sin(angle)
            for j in range(height):
                at = (group + j) * 128
                cosb[q, :, at : at + 128] = jnp.broadcast_to(cosine[j : j + 1], (16, 128)).astype(low)
                sinb[q, :, at : at + 128] = jnp.broadcast_to(sine[j : j + 1], (16, 128)).astype(low)
        return carry

    lax.fori_loop(0, per * blocks_q, phases, 0)

    def shift(stage, k, to):
        step, t = stage
        rows_at = pl.ds(pl.multiple_of(k % blocks * 8, 8), 8)
        first_lane = k // blocks * plane
        lanes = pl.ds(pl.multiple_of(first_lane, plane), plane)
        for c in range(3):
            w = field[step, t + 1, c, rows_at, lanes]
            moved[to, 0, c, rows_at, lanes] = pltpu.roll(w, plane - LZ, 1)
            moved[to, 1, c, rows_at, lanes] = pltpu.roll(w, LZ, 1)
            for part in range(tiles):
                u = w[:, part * 128 : part * 128 + 128]
                here = pl.ds(pl.multiple_of(first_lane + part * 128, 128), 128)
                moved[to, 2, c, rows_at, here] = jnp.where(
                    depth == LZ - 1, pltpu.roll(u, LZ - 1, 1), pltpu.roll(u, 127, 1)
                )
                moved[to, 3, c, rows_at, here] = jnp.where(
                    depth == 0, pltpu.roll(u, 128 - (LZ - 1), 1), pltpu.roll(u, 1, 1)
                )

    def block(stage, k, at_moved):
        step, t = stage
        lane, first = k // half_blocks, k % half_blocks * 16
        lanes = (
            pl.ds(pl.multiple_of(lane * 128, 128), 128),
            pl.ds(pl.multiple_of(plane + lane * 128, 128), 128),
        )
        at_rows = [pl.ds(pl.multiple_of(first + 8 * h, 8), 8) for h in range(2)]
        acc = {}
        for h in range(2):
            for r in range(3):
                for part in range(2):
                    mid = field[step, t + 1, r, at_rows[h], lanes[part]]
                    acc[h, r, part] = (1.0 - 6.0 * KAPPA) * mid
        for way in range(6):
            direction, back = way // 2, way % 2
            for c in range(3):
                sources = []
                for h in range(2):
                    if direction == 0:
                        p = t + 2 - 2 * back
                        sources.append([field[step, p, c, at_rows[h], lanes[i]] for i in range(2)])
                    else:
                        sources.append([moved[at_moved, way - 2, c, at_rows[h], lanes[i]] for i in range(2)])
                for r in range(3):
                    row = direction * 18 + (54 + c * 6 + r * 2 if back else r * 6 + c * 2)
                    ur = table[t, row, :, lanes[0]]
                    ui = table[t, row + 1, :, lanes[0]]
                    for h, (sr, si) in enumerate(sources):
                        if back:
                            acc[h, r, 0] = acc[h, r, 0] + (ur * sr + ui * si)
                            acc[h, r, 1] = acc[h, r, 1] + (ur * si - ui * sr)
                        else:
                            acc[h, r, 0] = acc[h, r, 0] + (ur * sr - ui * si)
                            acc[h, r, 1] = acc[h, r, 1] + (ur * si + ui * sr)
        both = pl.ds(pl.multiple_of(first, 16), 16)
        for r in range(3):
            for part in range(2):
                if step == 0:
                    for h in range(2):
                        field[1, t + 1, r, at_rows[h], lanes[part]] = acc[h, r, part]
                if step == 1 or t in outer:
                    pair = jnp.concatenate([acc[0, r, part], acc[1, r, part]], axis=0).astype(low)
                    if step == 1:
                        smeared[position[t] * 3 + r, both, lanes[part]] = pair
                    else:
                        k_at = pl.ds(pl.multiple_of((2 * r + part) * plane + lane * 128, 128), 128)
                        hsend[outer.index(t), both, k_at] = pair

    stages = [(step, t) for step in range(2) for t in inner + outer]

    def run(i):
        def trip(k, carry):
            if i + 1 < len(stages):
                shift(stages[i + 1], k, (i + 1) % 2)
            block(stages[i], k, i % 2)
            return carry

        lax.fori_loop(0, trips, trip, 0)

    def begin(k, carry):
        shift(stages[0], k, 0)
        return carry

    lax.fori_loop(0, trips, begin, 0)
    for i in range(len(inner)):
        run(i)

    def take(step, side):
        to = planes + 1 if side else 0
        for c in range(3):
            field[step, to, c] = halo[step, side, :, c * wide : (c + 1) * wide].astype(f32)

    links_up.wait_recv()
    for part in range(2):
        got = lrecv[16 * part : 16 * part + 16, :].astype(f32)
        for index in range(9):
            table[0, 54 + index * 2 + part] = jnp.broadcast_to(got[index : index + 1], (8, plane))
    at = len(inner)
    second_halos = halos(1, hsend.at[0], hsend.at[1])
    for side in range(2):
        first_halos[side].wait_recv()
        take(0, side)
        run(at + side)
        second_halos[1 - side].start()
    across[0].wait_recv()
    onward[0].start()
    for i in range(len(inner)):
        run(at + 2 + i)
    beside.wait_recv()
    onward[0].wait_recv()

    def fill(k, carry):
        re = pl.ds(pl.multiple_of(k * wide, wide), plane)
        im = pl.ds(pl.multiple_of(k * wide + plane, plane), plane)
        for slot in range(4):
            at_raw = slice(slot * unit, slot * unit + rows)
            at_turned = slice(slot * unit + rows, (slot + 1) * unit)
            right[at_turned, re] = -right[at_raw, im]
            right[at_turned, im] = right[at_raw, re]
        return carry

    def turn(half, qb, to):
        for j in range(per):
            q = qb * per + j
            for i, t in enumerate(half):
                for lane in range(0, plane, 128):
                    cosine = cosb[q, :, t * plane + lane : t * plane + lane + 128]
                    sine = sinb[q, :, t * plane + lane : t * plane + lane + 128]
                    for c in range(3):
                        for row in range(0, rows, 16):
                            k = position[t] * 3 + c
                            sr = smeared[k, row : row + 16, lane : lane + 128]
                            si = smeared[k, row : row + 16, plane + lane : plane + lane + 128]
                            at_rows = slice(j * rows + row, j * rows + row + 16)
                            col = (i * 3 + c) * wide + lane
                            to[at_rows, col : col + 128] = cosine * sr + sine * si
                            to[at_rows, col + plane : col + plane + 128] = cosine * si - sine * sr

    def product(half, qb, following, side, finish):
        ks = parts[0] if half is inner else parts[1]
        part = lax.dot_general(
            right[:, ks], left[side][:, 0 : ks.stop - ks.start], (((1,), (1,)), ((), ())),
            preferred_element_type=f32,
        )
        turn(half, following, left[1 - side])
        finish(qb, part)

    def products(half, finish):
        turn(half, 0, left[0])

        def two(h, carry):
            product(half, 2 * h, 2 * h + 1, 0, finish)
            product(half, 2 * h + 1, jnp.minimum(2 * h + 2, blocks_q - 1), 1, finish)
            return carry

        lax.fori_loop(0, blocks_q // 2, two, 0)

    def keep(qb, part):
        total[qb] = part

    lax.fori_loop(0, len(inner) * 3, fill, 0)
    products(inner, keep)
    across[1].wait_recv()
    onward[1].start()
    for side in range(2):
        second_halos[side].wait_recv()
        take(1, side)
        run(at + len(inner) + 2 + side)
    onward[1].wait_recv()
    lax.fori_loop(len(inner) * 3, planes * 3, fill, 0)

    def cross(qb):
        return remote(obuf.at[qb, 2 * unit : 4 * unit], relay.at[qb], out_sem.at[qb], vec=1 - v)

    def along(qb, hop, ds):
        root = (v if hop == 0 else 1 - v) * 2 + s
        source = obuf if hop == 0 else relay
        src = source.at[qb, ds * unit : (ds + 1) * unit]
        dst = rx.at[qb, b]
        sems = last_sem.at[qb]
        far = pltpu.make_async_remote_copy(
            src_ref=src, dst_ref=dst, send_sem=sems.at[bricks + hop * 2 + ds], recv_sem=sems.at[b],
            device_id={"brick": root, "sub": (s + ds) % 2}, device_id_type=pl.DeviceIdType.MESH,
        )
        near = pltpu.make_async_copy(src, dst, sems.at[b])
        return root, far, near

    def depart(qb, hop):
        for ds in range(2):
            root, far, near = along(qb, hop, ds)
            if ds:
                far.start()
            else:
                pl.when(root == b)(near.start)
                pl.when(root != b)(far.start)

    def hand_on(qb):
        cross(qb).wait_recv()
        depart(qb, 1)

    def ship(qb, part):
        obuf[qb] = ((total[qb] + part) * scale).astype(low)
        cross(qb).start()
        depart(qb, 0)
        pl.when(qb > 0)(lambda: hand_on(qb - 1))

    products(outer, ship)
    hand_on(blocks_q - 1)
    for qb in range(blocks_q):
        acc = None
        for i in range(bricks):
            pltpu.make_async_copy(rx.at[qb, i], rx.at[qb, i], last_sem.at[qb, i]).wait()
            got = rx[qb, i].astype(f32)
            acc = got if acc is None else acc + got
        out_ref[:, qb * per * rows : (qb + 1) * per * rows] = acc
    for copy in (links_up, *first_halos, *second_halos, *across, beside, *onward):
        copy.wait_send()
    for qb in range(blocks_q):
        cross(qb).wait_send()
        for hop in range(2):
            for ds in range(2):
                root, far, near = along(qb, hop, ds)
                if ds:
                    far.wait_send()
                else:
                    pl.when(root != b)(far.wait_send)


def shards_fused(vectors, gauge_links, momenta):
    plane = LY * LZ
    rows, local_sites = vectors.shape[0], vectors.shape[3]
    planes = local_sites // plane
    tiles = plane // 128
    bricks = lax.axis_size("brick")
    count = momenta.shape[0]
    per = 256 // rows
    blocks_q = 2 * (-(-count // (2 * per)))
    low, f32 = jnp.bfloat16, jnp.float32
    v = vectors.reshape((rows, 3, 2, planes * tiles, 128)).transpose((0, 1, 3, 2, 4))
    v = v.reshape((rows * 3, planes, tiles * 2, 128))
    g = gauge_links.reshape((27, 2, planes * tiles, 128)).transpose((0, 2, 1, 3))
    g = g.reshape((54 * planes * tiles, 128))
    wide = 2 * plane
    most = max(2, planes - 2) * 3 * wide
    scale = (3.0 * bricks * local_sites) ** (-0.5)
    vmem, dma = pltpu.VMEM, pltpu.SemaphoreType.DMA
    plan = (planes, rows, count, bricks, per, blocks_q, scale)
    out = pl.pallas_call(
        functools.partial(fused_kernel, plan),
        out_shape=jax.ShapeDtypeStruct((2 * rows, blocks_q * per * rows), f32),
        in_specs=[
            pl.BlockSpec(memory_space=pltpu.SMEM),
            pl.BlockSpec(memory_space=pl.ANY),
            pl.BlockSpec(memory_space=pl.ANY),
        ],
        out_specs=pl.BlockSpec(memory_space=pltpu.VMEM),
        scratch_shapes=[
            vmem((planes, rows * 3, tiles * 2, 128), f32),
            vmem((64 * planes * tiles, 128), f32),
            vmem((2, planes + 2, 3, rows, wide), f32),
            vmem((planes + 1, 108, 8, plane), f32),
            vmem((2, 4, 3, rows, wide), f32),
            vmem((8 * rows, planes * 3 * wide), low),
            vmem((planes * 3, rows, wide), low),
            vmem((per * rows, most), low),
            vmem((per * rows, most), low),
            vmem((per * blocks_q, 16, local_sites), low),
            vmem((per * blocks_q, 16, local_sites), low),
            vmem((blocks_q, 8 * rows, per * rows), f32),
            vmem((blocks_q, 8 * rows, per * rows), low),
            vmem((blocks_q, 4 * rows, per * rows), low),
            vmem((blocks_q, bricks, 2 * rows, per * rows), low),
            vmem((2, 2, rows, 3 * wide), low),
            vmem((2, rows, 3 * wide), low),
            vmem((32, plane), low),
            vmem((32, plane), low),
            dma((planes + 1,)),
            dma((2, 2, 2)),
            dma((2,)),
            dma((5, 2)),
            dma((blocks_q, 2)),
            dma((blocks_q, bricks + 4)),
        ],
        compiler_params=pltpu.CompilerParams(
            vmem_limit_bytes=60 * 2**20, collective_id=0, has_side_effects=True
        ),
        name="elementals",
    )(momenta.T, v, g)
    out = out.reshape((2, rows, blocks_q * per, rows))[:, :, :count]
    return jnp.transpose(out, (1, 2, 0, 3))


def choose(vectors, gauge_links, momenta):
    plane = LY * LZ
    bricks, vecs, subs = (lax.axis_size(a) for a in ("brick", "vec", "sub"))
    rows, local_sites = vectors.shape[0], vectors.shape[3]
    fits = local_sites % plane == 0 and 3 <= local_sites // plane <= 4 and rows == 32
    if fits and vecs == 2 and subs == 2 and bricks == 4:
        return shards_fused(vectors, gauge_links, momenta)
    return shards(vectors, gauge_links, momenta)


def solution(mesh):
    in_specs = (
        P(("vec", "sub"), None, None, ("grp", "brick")),
        P(None, None, None, None, ("grp", "brick")),
        P(),
    )
    out_specs = P(("vec", "sub"), "grp", None, "brick")
    return jax.shard_map(choose, mesh=mesh, in_specs=in_specs, out_specs=out_specs, check_vma=False)
```

```python
import functools
import math

import jax
import jax.numpy as jnp
from jax import lax
from jax.experimental import pallas as pl
from jax.experimental.pallas import tpu as pltpu
from jax.sharding import PartitionSpec as P

LY = 64
LZ = 8
ITERS = 2


KAPPA = 0.125


def from_behind(array, axis, by):
    peers = lax.axis_size(axis)
    return lax.ppermute(array, axis, [(i, (i + by) % peers) for i in range(peers)])


def padded_2(array, sides, width):
    for axis, dim in sides:
        peers, length = (lax.axis_size(axis), array.shape[dim])
        up = [(i, (i + 1) % peers) for i in range(peers)]
        down = [(j, i) for i, j in up]
        last = lax.slice_in_dim(array, length - width, length, axis=dim)
        initial = lax.slice_in_dim(array, 0, width, axis=dim)
        before = lax.ppermute(last, axis, up)
        after = lax.ppermute(initial, axis, down)
        array = jnp.concatenate([before, array, after], axis=dim)
    return array


def matrix_apply(matrix, source):
    matrix_real = matrix[:, :, 0][None]
    matrix_imag = matrix[:, :, 1][None]
    source_real = source[:, None, :, 0]
    source_imag = source[:, None, :, 1]
    real_part = jnp.sum(matrix_real * source_real - matrix_imag * source_imag, axis=2)
    imag_part = jnp.sum(matrix_real * source_imag + matrix_imag * source_real, axis=2)
    return jnp.stack([real_part, imag_part], axis=2)


def adjoint(matrix):
    return jnp.stack(
        [jnp.swapaxes(matrix[:, :, 0], 0, 1), -jnp.swapaxes(matrix[:, :, 1], 0, 1)], axis=2
    )


def step_depth(values, offset):
    depth_index = lax.iota(jnp.int32, values.shape[-1]) % LZ
    if offset > 0:
        return jnp.where(
            depth_index == LZ - 1, jnp.roll(values, LZ - 1, -1), jnp.roll(values, -1, -1)
        )
    return jnp.where(depth_index == 0, jnp.roll(values, 1 - LZ, -1), jnp.roll(values, 1, -1))


def step_column(values, offset):
    plane = LY * LZ
    column_index = lax.iota(jnp.int32, values.shape[-1]) // LZ % LY
    if offset > 0:
        return jnp.where(
            column_index == LY - 1, jnp.roll(values, plane - LZ, -1), jnp.roll(values, -LZ, -1)
        )
    return jnp.where(column_index == 0, jnp.roll(values, LZ - plane, -1), jnp.roll(values, LZ, -1))


def laplace_step(center, ahead, behind, here_links, back_links):
    forward = matrix_apply(here_links[0], ahead)
    backward = matrix_apply(adjoint(back_links), behind)
    total = forward + backward
    for direction, stepper in ((1, step_column), (2, step_depth)):
        forward = matrix_apply(here_links[direction], stepper(center, 1))
        backward = matrix_apply(adjoint(stepper(here_links[direction], -1)), stepper(center, -1))
        total = total + (forward + backward)
    return center + KAPPA * (total - 6.0 * center)


def shards(vectors, gauge_links, momenta):
    plane = LY * LZ
    local_sites = vectors.shape[3]
    raw_low = vectors.astype(jnp.bfloat16)
    field = vectors
    x_links = gauge_links[0]
    rim = from_behind(x_links[..., local_sites - plane :], "brick", 1)
    back_links = jnp.concatenate([rim, x_links[..., : local_sites - plane]], axis=3)
    for step in range(ITERS):
        padded = padded_2(field, (("brick", 3),), plane)
        field = laplace_step(
            padded[..., plane : plane + local_sites],
            padded[..., 2 * plane :],
            padded[..., :local_sites],
            gauge_links,
            back_links,
        )
    smeared_low = field.astype(jnp.bfloat16)
    raw_sites, smeared_sites = (
        lax.all_to_all(raw_low, ("vec", "sub"), split_axis=3, concat_axis=0, tiled=True),
        lax.all_to_all(smeared_low, ("vec", "sub"), split_axis=3, concat_axis=0, tiled=True),
    )
    groups = lax.axis_size(("vec", "sub"))
    total_vec = raw_sites.shape[0]
    width = raw_sites.shape[3]
    total_x = lax.axis_size("brick") * (local_sites // plane)
    first_site = lax.axis_index("brick") * local_sites + lax.axis_index(("vec", "sub")) * width
    site = first_site + lax.iota(jnp.int32, width)
    layer_index = (site // plane)[None]
    column_index = (site // LZ % LY)[None]
    depth_index = (site % LZ)[None]
    fraction = (
        jnp.mod(momenta[:, 0:1] * layer_index, total_x).astype(jnp.float32) / total_x
        + jnp.mod(momenta[:, 1:2] * column_index, LY).astype(jnp.float32) / LY
        + jnp.mod(momenta[:, 2:3] * depth_index, LZ).astype(jnp.float32) / LZ
    )
    angle = 2.0 * math.pi * fraction
    cosines = jnp.cos(angle)
    sines = jnp.sin(angle)
    right = smeared_sites.reshape((total_vec, 6 * width))
    scale = (3.0 * total_x * plane) ** (-0.5)

    def one_momentum(angles):
        cosine, sine = angles
        real_part = raw_sites[:, :, 0] * cosine - raw_sites[:, :, 1] * sine
        imag_part = raw_sites[:, :, 0] * sine + raw_sites[:, :, 1] * cosine
        phased = jnp.stack([real_part, imag_part], axis=2).astype(jnp.bfloat16)
        turned = jnp.stack([-phased[:, :, 1], phased[:, :, 0]], axis=2)
        left = jnp.concatenate(
            [
                phased.reshape((lax.axis_size(("vec", "sub")) * (total_vec // groups), 6 * width)),
                turned.reshape((lax.axis_size(("vec", "sub")) * (total_vec // groups), 6 * width)),
            ],
            axis=0,
        )
        product = lax.dot_general(
            left, right, (((1,), (1,)), ((), ())), preferred_element_type=jnp.float32
        )
        return product.reshape(
            (2, lax.axis_size(("vec", "sub")) * (total_vec // groups), total_vec)
        )

    blocks = lax.map(one_momentum, (cosines, sines))
    shares = lax.psum_scatter(
        jnp.transpose(blocks, (2, 0, 1, 3)) * scale, ("vec", "sub"), scatter_dimension=0, tiled=True
    )
    return lax.psum_scatter(shares, "brick", scatter_dimension=3, tiled=True)


def fused_kernel(plan, mom_ref, v_ref, g_ref, out_ref, *scratch):
    (vst, gst, field0, field1, table, moved0, moved1, right, smeared, left0, left1, cosb, sinb, total, obuf,
     relay, rx, halo, hsend, lsend, lrecv, load_sem, halo_sem, link_sem, raw_sem, out_sem, last_sem) = scratch
    planes, rows, count, bricks, per, blocks_q, scale = plan
    fields, moved = (field0, field1), (moved0, moved1)
    halves = rows // 16
    plane = LY * LZ
    tiles = plane // 128
    all_tiles = planes * tiles
    f32, low = jnp.float32, jnp.bfloat16
    wide = 2 * plane
    last = planes - 1
    inner = list(range(1, last))
    outer = [0, last]
    position = {t: i for i, t in enumerate(inner + outer)}
    cut = len(inner) * 3 * wide
    span = planes * 3 * wide
    b, v, s = (lax.axis_index(a) for a in ("brick", "vec", "sub"))
    left = (left0, left1)

    def remote(src, dst, sems, **ids):
        return pltpu.make_async_remote_copy(
            src_ref=src, dst_ref=dst, send_sem=sems.at[0], recv_sem=sems.at[1],
            device_id=ids, device_id_type=pl.DeviceIdType.MESH,
        )

    loads = {}
    for t in outer + inner:
        loads[t] = pltpu.make_async_copy(v_ref.at[:, t], vst.at[t], load_sem.at[t])
        loads[t].start()
    load_links = pltpu.make_async_copy(g_ref, gst.at[pl.ds(0, 54 * all_tiles)], load_sem.at[planes])
    load_links.start()
    barrier = pltpu.get_barrier_semaphore()
    for db in range(bricks):
        for ds in range(2):
            if db or ds:
                pl.semaphore_signal(
                    barrier, inc=1, device_id={"brick": (b + db) % bricks, "sub": (s + ds) % 2},
                    device_id_type=pl.DeviceIdType.MESH,
                )
    pl.semaphore_signal(
        barrier, inc=1, device_id={"vec": 1 - v}, device_id_type=pl.DeviceIdType.MESH
    )

    def unpack(t):
        flat = vst.at[t].reshape(rows * 3 * tiles * 2, 128)
        step = 3 * tiles * 2
        for c in range(3):
            for first in range(0, rows, 16):
                for part in range(2):
                    for lane in range(0, tiles, 2):
                        at = part * plane + lane * 128
                        quad = []
                        for h in range(2):
                            start = (first + 8 * h) * step + c * tiles * 2 + lane * 2 + part
                            quad.append(
                                jnp.concatenate(
                                    [flat[pl.ds(start + 2 * i, 8, stride=step), :] for i in range(2)], axis=1
                                )
                            )
                            field0[t + 1, c, first + 8 * h : first + 8 * h + 8, at : at + 256] = quad[h]
                        k = (position[t] * 3 + c) * wide + at
                        right[first : first + 16, k : k + 256] = jnp.concatenate(quad, axis=0).astype(low)

    def link_rows(t, part, group):
        return jnp.concatenate(
            [
                gst[pl.ds(group * 16 * all_tiles + (t * tiles + lane) * 2 + part, 8, stride=2 * all_tiles), :]
                for lane in range(tiles)
            ],
            axis=1,
        ) * KAPPA

    for t in outer:
        loads[t].wait()
        unpack(t)
    load_links.wait()
    for part in range(2):
        both = jnp.concatenate([link_rows(last, part, 0), link_rows(last, part, 1)], axis=0)
        lsend[16 * part : 16 * part + 16, :] = both.astype(low)
    pl.semaphore_wait(barrier, 2 * bricks)
    up, down = (b + 1) % bricks, (b + bricks - 1) % bricks

    def halos(step, h, low_src, high_src):
        sems = halo_sem.at[step, h]
        return (
            remote(high_src, halo.at[step, h, 0], sems.at[0], brick=up),
            remote(low_src, halo.at[step, h, 1], sems.at[1], brick=down),
        )

    def own(t, h):
        at = position[t] * 3 * wide
        return right.at[16 * h : 16 * h + 16, at : at + 3 * wide]

    copies = {}
    links_up = remote(lsend, lrecv, link_sem, brick=up)
    for h in range(halves):
        copies[0, h] = halos(0, h, own(0, h), own(last, h))
        copies[1, h] = halos(1, h, hsend.at[h, 0], hsend.at[h, 1])
        for copy in copies[0, h]:
            copy.start()
        if h == 0:
            links_up.start()
    for t in inner:
        loads[t].wait()
        unpack(t)
    parts = (slice(0, cut), slice(cut, span))
    unit = 2 * rows

    def raw_copy(index, from_slot, to_slot, ks, **ids):
        return remote(
            right.at[from_slot * unit : from_slot * unit + rows, ks],
            right.at[to_slot * unit : to_slot * unit + rows, ks],
            raw_sem.at[index], **ids,
        )

    across = [raw_copy(i, 0, 2, parts[i], vec=1 - v) for i in range(2)]
    beside = raw_copy(2, 0, 1, slice(0, span), sub=1 - s)
    onward = [raw_copy(3 + i, 2, 3, parts[i], sub=1 - s) for i in range(2)]
    for copy in across + [beside]:
        copy.start()

    depth_wide = lax.broadcasted_iota(jnp.int32, (8, plane), 1) % LZ
    depth = lax.broadcasted_iota(jnp.int32, (8, 128), 1) % LZ

    def spread(t, carry):
        for part in range(2):
            for group in range(4):
                here = link_rows(t, part, group)
                if group > 0:
                    by = pltpu.roll(here, LZ, 1)
                    bz = jnp.where(
                        depth_wide == 0, pltpu.roll(here, plane - (LZ - 1), 1), pltpu.roll(here, 1, 1)
                    )
                for j in range(min(8, 27 - 8 * group)):
                    index = group * 8 + j
                    row = jnp.broadcast_to(here[j : j + 1], (8, plane))
                    table[t, index * 2 + part] = row
                    if index < 9:
                        table[t + 1, 54 + index * 2 + part] = row
                    else:
                        back = by if index < 18 else bz
                        table[t, 54 + index * 2 + part] = jnp.broadcast_to(back[j : j + 1], (8, plane))
        return carry

    lax.fori_loop(0, planes, spread, 0)

    places = []
    for group in range(0, all_tiles, 8):
        height = min(8, all_tiles - group)
        site = (
            lax.broadcasted_iota(jnp.int32, (height, 128), 0) * 128
            + lax.broadcasted_iota(jnp.int32, (height, 128), 1)
            + group * 128
        )
        places.append(
            (
                (site // plane + b * planes).astype(f32) * (1.0 / (bricks * planes)),
                (site // LZ % LY).astype(f32) * (1.0 / LY),
                (site % LZ).astype(f32) * (1.0 / LZ),
            )
        )

    def phases(q, carry):
        n = [mom_ref[d, jnp.minimum(q, count - 1)].astype(f32) for d in range(3)]
        for group, (x, y, z) in enumerate(places):
            turns = n[0] * x + n[1] * y + n[2] * z
            half = jnp.round(2.0 * turns)
            sign = 1.0 - 2.0 * jnp.abs(half - 2.0 * jnp.round(0.5 * half))
            angle = (2.0 * math.pi) * (turns - 0.5 * half)
            square = angle * angle
            cosine, sine = 0.0, 0.0
            for i in range(7, 0, -1):
                cosine = (cosine * square) + (-1.0) ** i / math.factorial(2 * i)
            cosine = sign * (1.0 + cosine * square)
            for i in range(6, 0, -1):
                sine = (sine * square) + (-1.0) ** i / math.factorial(2 * i + 1)
            sine = sign * (angle + angle * (sine * square))
            for j in range(x.shape[0]):
                at = (group * 8 + j) * 128
                cosb[q, :, at : at + 128] = jnp.broadcast_to(cosine[j : j + 1], (16, 128)).astype(low)
                sinb[q, :, at : at + 128] = jnp.broadcast_to(sine[j : j + 1], (16, 128)).astype(low)
        return carry

    lax.fori_loop(0, count, phases, 0)

    def shift(stage, k, to):
        step, t, h = stage
        rows_to = pl.ds(pl.multiple_of(k % 2 * 8, 8), 8)
        rows_at = pl.ds(pl.multiple_of(h * 16 + k % 2 * 8, 8), 8)
        first_lane = k // 2 * plane
        lanes = pl.ds(pl.multiple_of(first_lane, plane), plane)
        for c in range(3):
            w = fields[step][t + 1, c, rows_at, lanes]
            to[0, c, rows_to, lanes] = pltpu.roll(w, plane - LZ, 1)
            to[1, c, rows_to, lanes] = pltpu.roll(w, LZ, 1)
            for part in range(tiles):
                u = w[:, part * 128 : part * 128 + 128]
                here = pl.ds(pl.multiple_of(first_lane + part * 128, 128), 128)
                to[2, c, rows_to, here] = jnp.where(
                    depth == LZ - 1, pltpu.roll(u, LZ - 1, 1), pltpu.roll(u, 127, 1)
                )
                to[3, c, rows_to, here] = jnp.where(
                    depth == 0, pltpu.roll(u, 128 - (LZ - 1), 1), pltpu.roll(u, 1, 1)
                )

    def block(stage, lane, now):
        step, t, half = stage
        field = fields[step]
        lanes = (
            pl.ds(pl.multiple_of(lane * 128, 128), 128),
            pl.ds(pl.multiple_of(plane + lane * 128, 128), 128),
        )
        at_rows = [slice(half * 16 + 8 * h, half * 16 + 8 * h + 8) for h in range(2)]
        acc = {}
        for h in range(2):
            for r in range(3):
                for part in range(2):
                    mid = field[t + 1, r, at_rows[h], lanes[part]]
                    acc[h, r, part] = (1.0 - 6.0 * KAPPA) * mid
        for way in range(6):
            direction, back = way // 2, way % 2
            for c in range(3):
                sources = []
                for h in range(2):
                    if direction == 0:
                        p = t + 2 - 2 * back
                        sources.append([field[p, c, at_rows[h], lanes[i]] for i in range(2)])
                    else:
                        sources.append([now[way - 2, c, 8 * h : 8 * h + 8, lanes[i]] for i in range(2)])
                for r in range(3):
                    row = direction * 18 + (54 + c * 6 + r * 2 if back else r * 6 + c * 2)
                    ur = table[t, row, :, lanes[0]]
                    ui = table[t, row + 1, :, lanes[0]]
                    for h, (sr, si) in enumerate(sources):
                        if back:
                            acc[h, r, 0] = acc[h, r, 0] + (ur * sr + ui * si)
                            acc[h, r, 1] = acc[h, r, 1] + (ur * si - ui * sr)
                        else:
                            acc[h, r, 0] = acc[h, r, 0] + (ur * sr - ui * si)
                            acc[h, r, 1] = acc[h, r, 1] + (ur * si + ui * sr)
        both = slice(half * 16, half * 16 + 16)
        for r in range(3):
            for part in range(2):
                if step == 0:
                    for h in range(2):
                        field1[t + 1, r, at_rows[h], lanes[part]] = acc[h, r, part]
                if step == 1 or t in outer:
                    pair = jnp.concatenate([acc[0, r, part], acc[1, r, part]], axis=0).astype(low)
                    if step == 1:
                        smeared[position[t] * 3 + r, both, lanes[part]] = pair
                    else:
                        k_at = pl.ds(pl.multiple_of((2 * r + part) * plane + lane * 128, 128), 128)
                        hsend[half, outer.index(t), :, k_at] = pair

    stages = [(0, t, h) for h in range(halves) for t in inner]
    for h in range(halves):
        stages += [(0, t, h) for t in outer] + [(1, t, h) for t in inner]
    stages += [(1, t, h) for h in range(halves) for t in outer]

    def run(step, ts, h):
        for t in ts:
            i = stages.index((step, t, h))

            def trip(k, carry):
                if i + 1 < len(stages):
                    shift(stages[i + 1], k, moved[(i + 1) % 2])
                block(stages[i], k, moved[i % 2])
                return carry

            lax.fori_loop(0, tiles, trip, 0)

    def begin(k, carry):
        shift(stages[0], k, moved[0])
        return carry

    lax.fori_loop(0, tiles, begin, 0)
    for h in range(halves):
        run(0, inner, h)

    def take(step, h, side):
        copies[step, h][side].wait_recv()
        for c in range(3):
            fields[step][planes + 1 if side else 0, c, 16 * h : 16 * h + 16] = (
                halo[step, h, side, :, c * wide : (c + 1) * wide].astype(f32)
            )

    links_up.wait_recv()
    for part in range(2):
        got = lrecv[16 * part : 16 * part + 16, :].astype(f32)
        for index in range(9):
            table[0, 54 + index * 2 + part] = jnp.broadcast_to(got[index : index + 1], (8, plane))
    for h in range(halves):
        for side in range(2):
            take(0, h, side)
            run(0, [outer[side]], h)
            copies[1, h][1 - side].start()
        if h == halves - 1:
            across[0].wait_recv()
            onward[0].start()
        run(1, inner, h)
    beside.wait_recv()
    onward[0].wait_recv()

    def fill(k, carry):
        re = pl.ds(pl.multiple_of(k * wide, wide), plane)
        im = pl.ds(pl.multiple_of(k * wide + plane, plane), plane)
        for slot in range(4):
            at_raw = slice(slot * unit, slot * unit + rows)
            at_turned = slice(slot * unit + rows, (slot + 1) * unit)
            right[at_turned, re] = -right[at_raw, im]
            right[at_turned, im] = right[at_raw, re]
        return carry

    blocks = [(h, half, qb) for h in range(halves) for half in range(2) for qb in range(blocks_q)]
    members = (inner, outer)

    def turn(i):
        h, half, qb = blocks[i]
        to = left[i % 2]
        for j in range(min(per, count - qb * per)):
            q = qb * per + j
            for n, t in enumerate(members[half]):
                for lane in range(0, plane, 256):
                    cosine = cosb[q, :, t * plane + lane : t * plane + lane + 256]
                    sine = sinb[q, :, t * plane + lane : t * plane + lane + 256]
                    for c in range(3):
                        k = position[t] * 3 + c
                        sr = smeared[k, 16 * h : 16 * h + 16, lane : lane + 256]
                        si = smeared[k, 16 * h : 16 * h + 16, plane + lane : plane + lane + 256]
                        col = (n * 3 + c) * wide + lane
                        to[16 * j : 16 * j + 16, col : col + 256] = cosine * sr + sine * si
                        to[16 * j : 16 * j + 16, col + plane : col + plane + 256] = cosine * si - sine * sr

    def product(i):
        h, half, qb = blocks[i]
        columns = 16 * min(per, count - qb * per)
        first = parts[half].start
        length = parts[half].stop - first
        pieces = []
        for k in range(0, length, length // 2):
            pieces.append(
                lax.dot_general(
                    right[:, first + k : first + k + length // 2],
                    left[i % 2][0:columns, k : k + length // 2],
                    (((1,), (1,)), ((), ())), preferred_element_type=f32,
                )
            )
        if i + 1 < len(blocks) and not (blocks[i + 1][1] == 1 and blocks[i + 1][2] == 0):
            turn(i + 1)
        part = pieces[0] + pieces[1]
        e = h * blocks_q + qb
        if half == 0:
            total[e, :, 0:columns] = part
        else:
            obuf[e, :, 0:columns] = ((total[e, :, 0:columns] + part) * scale).astype(low)

    def cross(e):
        return remote(obuf.at[e, 2 * unit : 4 * unit], relay.at[e], out_sem.at[e], vec=1 - v)

    roots = (v * 2 + s, (1 - v) * 2 + s)

    def ends(e, hop, ds):
        source = relay if hop else obuf
        return source.at[e, ds * unit : (ds + 1) * unit], rx.at[e, b], last_sem.at[e]

    def far(e, hop, ds):
        src, dst, sems = ends(e, hop, ds)
        return pltpu.make_async_remote_copy(
            src_ref=src, dst_ref=dst, send_sem=sems.at[bricks + hop * 2 + ds], recv_sem=sems.at[b],
            device_id={"brick": roots[hop], "sub": (s + ds) % 2}, device_id_type=pl.DeviceIdType.MESH,
        )

    def depart(e, hop):
        far(e, hop, 1).start()

        @pl.when(roots[hop] != b)
        def _():
            far(e, hop, 0).start()

        @pl.when(roots[hop] == b)
        def _():
            src, dst, sems = ends(e, hop, 0)
            pltpu.make_async_copy(src, dst, sems.at[b]).start()

    def hand_on(e):
        cross(e).wait_recv()
        depart(e, 1)

    def ship(e):
        cross(e).start()
        depart(e, 0)
        if e > 0:
            hand_on(e - 1)

    def fill_half(half):
        first = len(inner) * 3 if half else 0
        count_k = len(members[half]) * 3
        lax.fori_loop(first, first + count_k, fill, 0)

    for h in range(halves):
        for half in range(2):
            if half:
                if h == 0:
                    across[1].wait_recv()
                    onward[1].start()
                for side in range(2):
                    take(1, h, side)
                    run(1, [outer[side]], h)
                if h == 0:
                    onward[1].wait_recv()
            if h == 0:
                fill_half(half)
            for qb in range(blocks_q):
                i = blocks.index((h, half, qb))
                if qb == 0 and (half or h == 0):
                    turn(i)
                product(i)
                if half:
                    ship(h * blocks_q + qb)
    ships = halves * blocks_q
    hand_on(ships - 1)
    for e in range(ships):
        acc = None
        for i in range(bricks):
            pltpu.make_async_copy(rx.at[e, i], rx.at[e, i], last_sem.at[e, i]).wait()
            got = rx[e, i].astype(f32)
            acc = got if acc is None else acc + got
        out_ref[:, e * per * 16 : (e + 1) * per * 16] = acc
    sent = [links_up, *across, beside, *onward]
    for copy in copies.values():
        sent += copy
    for copy in sent:
        copy.wait_send()
    for e in range(ships):
        cross(e).wait_send()
        for hop in range(2):
            far(e, hop, 1).wait_send()

            @pl.when(roots[hop] != b)
            def _():
                far(e, hop, 0).wait_send()


def shards_fused(vectors, gauge_links, momenta):
    plane = LY * LZ
    rows, local_sites = vectors.shape[0], vectors.shape[3]
    planes = local_sites // plane
    tiles = plane // 128
    bricks = lax.axis_size("brick")
    count = momenta.shape[0]
    per = 256 // 16
    blocks_q = -(-count // per)
    halves = rows // 16
    ships = halves * blocks_q
    low, f32 = jnp.bfloat16, jnp.float32
    v = vectors.reshape((rows, 3, 2, planes * tiles, 128)).transpose((0, 1, 3, 2, 4))
    v = v.reshape((rows * 3, planes, tiles * 2, 128))
    g = gauge_links.reshape((27, 2, planes * tiles, 128)).transpose((0, 2, 1, 3))
    g = g.reshape((54 * planes * tiles, 128))
    wide = 2 * plane
    most = max(2, planes - 2) * 3 * wide
    scale = (3.0 * bricks * local_sites) ** (-0.5)
    vmem, dma = pltpu.VMEM, pltpu.SemaphoreType.DMA
    plan = (planes, rows, count, bricks, per, blocks_q, scale)
    out = pl.pallas_call(
        functools.partial(fused_kernel, plan),
        out_shape=jax.ShapeDtypeStruct((2 * rows, ships * per * 16), f32),
        in_specs=[
            pl.BlockSpec(memory_space=pltpu.SMEM),
            pl.BlockSpec(memory_space=pl.ANY),
            pl.BlockSpec(memory_space=pl.ANY),
        ],
        out_specs=pl.BlockSpec(memory_space=pltpu.VMEM),
        scratch_shapes=[
            vmem((planes, rows * 3, tiles * 2, 128), f32),
            vmem((64 * planes * tiles, 128), f32),
            vmem((planes + 2, 3, rows, wide), f32),
            vmem((planes + 2, 3, rows, wide), f32),
            vmem((planes + 1, 108, 8, plane), f32),
            vmem((4, 3, 16, wide), f32),
            vmem((4, 3, 16, wide), f32),
            vmem((8 * rows, planes * 3 * wide), low),
            vmem((planes * 3, rows, wide), low),
            vmem((per * 16, most), low),
            vmem((per * 16, most), low),
            vmem((count, 16, local_sites), low),
            vmem((count, 16, local_sites), low),
            vmem((ships, 8 * rows, per * 16), f32),
            vmem((ships, 8 * rows, per * 16), low),
            vmem((ships, 4 * rows, per * 16), low),
            vmem((ships, bricks, 2 * rows, per * 16), low),
            vmem((2, halves, 2, 16, 3 * wide), low),
            vmem((halves, 2, 16, 3 * wide), low),
            vmem((32, plane), low),
            vmem((32, plane), low),
            dma((planes + 1,)),
            dma((2, halves, 2, 2)),
            dma((2,)),
            dma((5, 2)),
            dma((ships, 2)),
            dma((ships, bricks + 4)),
        ],
        compiler_params=pltpu.CompilerParams(
            vmem_limit_bytes=60 * 2**20, collective_id=0, has_side_effects=True
        ),
        name="elementals",
    )(momenta.T, v, g)
    out = out.reshape((2, rows, halves, blocks_q * per, 16))[:, :, :, :count]
    return jnp.transpose(out, (1, 3, 0, 2, 4)).reshape((rows, count, 2, rows))


def choose(vectors, gauge_links, momenta):
    plane = LY * LZ
    bricks, vecs, subs = (lax.axis_size(a) for a in ("brick", "vec", "sub"))
    rows, local_sites = vectors.shape[0], vectors.shape[3]
    fits = local_sites % plane == 0 and 3 <= local_sites // plane <= 4 and rows == 32
    if fits and vecs == 2 and subs == 2 and bricks == 4:
        return shards_fused(vectors, gauge_links, momenta)
    return shards(vectors, gauge_links, momenta)


def solution(mesh):
    in_specs = (
        P(("vec", "sub"), None, None, ("grp", "brick")),
        P(None, None, None, None, ("grp", "brick")),
        P(),
    )
    out_specs = P(("vec", "sub"), "grp", None, "brick")
    return jax.shard_map(choose, mesh=mesh, in_specs=in_specs, out_specs=out_specs, check_vma=False)
```

```python
import functools
import math

import jax
import jax.numpy as jnp
from jax import lax
from jax.experimental import pallas as pl
from jax.experimental.pallas import tpu as pltpu
from jax.sharding import PartitionSpec as P

LY = 64
LZ = 8
ITERS = 2


KAPPA = 0.125


def from_behind(array, axis, by):
    peers = lax.axis_size(axis)
    return lax.ppermute(array, axis, [(i, (i + by) % peers) for i in range(peers)])


def padded_2(array, sides, width):
    for axis, dim in sides:
        peers, length = (lax.axis_size(axis), array.shape[dim])
        up = [(i, (i + 1) % peers) for i in range(peers)]
        down = [(j, i) for i, j in up]
        last = lax.slice_in_dim(array, length - width, length, axis=dim)
        initial = lax.slice_in_dim(array, 0, width, axis=dim)
        before = lax.ppermute(last, axis, up)
        after = lax.ppermute(initial, axis, down)
        array = jnp.concatenate([before, array, after], axis=dim)
    return array


def matrix_apply(matrix, source):
    matrix_real = matrix[:, :, 0][None]
    matrix_imag = matrix[:, :, 1][None]
    source_real = source[:, None, :, 0]
    source_imag = source[:, None, :, 1]
    real_part = jnp.sum(matrix_real * source_real - matrix_imag * source_imag, axis=2)
    imag_part = jnp.sum(matrix_real * source_imag + matrix_imag * source_real, axis=2)
    return jnp.stack([real_part, imag_part], axis=2)


def adjoint(matrix):
    return jnp.stack(
        [jnp.swapaxes(matrix[:, :, 0], 0, 1), -jnp.swapaxes(matrix[:, :, 1], 0, 1)], axis=2
    )


def step_depth(values, offset):
    depth_index = lax.iota(jnp.int32, values.shape[-1]) % LZ
    if offset > 0:
        return jnp.where(
            depth_index == LZ - 1, jnp.roll(values, LZ - 1, -1), jnp.roll(values, -1, -1)
        )
    return jnp.where(depth_index == 0, jnp.roll(values, 1 - LZ, -1), jnp.roll(values, 1, -1))


def step_column(values, offset):
    plane = LY * LZ
    column_index = lax.iota(jnp.int32, values.shape[-1]) // LZ % LY
    if offset > 0:
        return jnp.where(
            column_index == LY - 1, jnp.roll(values, plane - LZ, -1), jnp.roll(values, -LZ, -1)
        )
    return jnp.where(column_index == 0, jnp.roll(values, LZ - plane, -1), jnp.roll(values, LZ, -1))


def laplace_step(center, ahead, behind, here_links, back_links):
    forward = matrix_apply(here_links[0], ahead)
    backward = matrix_apply(adjoint(back_links), behind)
    total = forward + backward
    for direction, stepper in ((1, step_column), (2, step_depth)):
        forward = matrix_apply(here_links[direction], stepper(center, 1))
        backward = matrix_apply(adjoint(stepper(here_links[direction], -1)), stepper(center, -1))
        total = total + (forward + backward)
    return center + KAPPA * (total - 6.0 * center)


def shards(vectors, gauge_links, momenta):
    plane = LY * LZ
    local_sites = vectors.shape[3]
    raw_low = vectors.astype(jnp.bfloat16)
    field = vectors
    x_links = gauge_links[0]
    rim = from_behind(x_links[..., local_sites - plane :], "brick", 1)
    back_links = jnp.concatenate([rim, x_links[..., : local_sites - plane]], axis=3)
    for step in range(ITERS):
        padded = padded_2(field, (("brick", 3),), plane)
        field = laplace_step(
            padded[..., plane : plane + local_sites],
            padded[..., 2 * plane :],
            padded[..., :local_sites],
            gauge_links,
            back_links,
        )
    smeared_low = field.astype(jnp.bfloat16)
    raw_sites, smeared_sites = (
        lax.all_to_all(raw_low, ("vec", "sub"), split_axis=3, concat_axis=0, tiled=True),
        lax.all_to_all(smeared_low, ("vec", "sub"), split_axis=3, concat_axis=0, tiled=True),
    )
    groups = lax.axis_size(("vec", "sub"))
    total_vec = raw_sites.shape[0]
    width = raw_sites.shape[3]
    total_x = lax.axis_size("brick") * (local_sites // plane)
    first_site = lax.axis_index("brick") * local_sites + lax.axis_index(("vec", "sub")) * width
    site = first_site + lax.iota(jnp.int32, width)
    layer_index = (site // plane)[None]
    column_index = (site // LZ % LY)[None]
    depth_index = (site % LZ)[None]
    fraction = (
        jnp.mod(momenta[:, 0:1] * layer_index, total_x).astype(jnp.float32) / total_x
        + jnp.mod(momenta[:, 1:2] * column_index, LY).astype(jnp.float32) / LY
        + jnp.mod(momenta[:, 2:3] * depth_index, LZ).astype(jnp.float32) / LZ
    )
    angle = 2.0 * math.pi * fraction
    cosines = jnp.cos(angle)
    sines = jnp.sin(angle)
    right = smeared_sites.reshape((total_vec, 6 * width))
    scale = (3.0 * total_x * plane) ** (-0.5)

    def one_momentum(angles):
        cosine, sine = angles
        real_part = raw_sites[:, :, 0] * cosine - raw_sites[:, :, 1] * sine
        imag_part = raw_sites[:, :, 0] * sine + raw_sites[:, :, 1] * cosine
        phased = jnp.stack([real_part, imag_part], axis=2).astype(jnp.bfloat16)
        turned = jnp.stack([-phased[:, :, 1], phased[:, :, 0]], axis=2)
        left = jnp.concatenate(
            [
                phased.reshape((lax.axis_size(("vec", "sub")) * (total_vec // groups), 6 * width)),
                turned.reshape((lax.axis_size(("vec", "sub")) * (total_vec // groups), 6 * width)),
            ],
            axis=0,
        )
        product = lax.dot_general(
            left, right, (((1,), (1,)), ((), ())), preferred_element_type=jnp.float32
        )
        return product.reshape(
            (2, lax.axis_size(("vec", "sub")) * (total_vec // groups), total_vec)
        )

    blocks = lax.map(one_momentum, (cosines, sines))
    shares = lax.psum_scatter(
        jnp.transpose(blocks, (2, 0, 1, 3)) * scale, ("vec", "sub"), scatter_dimension=0, tiled=True
    )
    return lax.psum_scatter(shares, "brick", scatter_dimension=3, tiled=True)


def fused_kernel(plan, mom_ref, v_ref, g_ref, out_ref, *scratch):
    (vst, gst, field0, field1, table, moved0, moved1, right, smeared, left0, left1, cosb, sinb, total, parted,
     crossing, paired, summed, rx, halo, hsend, lsend, lrecv, load_sem, halo_sem, link_sem, raw_sem, cross_sem, pair_sem, last_sem) = scratch
    planes, rows, count, bricks, units, scale = plan
    fields, moved = (field0, field1), (moved0, moved1)
    halves = rows // 16
    plane = LY * LZ
    tiles = plane // 128
    all_tiles = planes * tiles
    f32, low = jnp.float32, jnp.bfloat16
    wide = 2 * plane
    last = planes - 1
    inner = list(range(1, last))
    outer = [0, last]
    position = {t: i for i, t in enumerate(inner + outer)}
    cut = len(inner) * 3 * wide
    span = planes * 3 * wide
    b, v, s = (lax.axis_index(a) for a in ("brick", "vec", "sub"))
    left = (left0, left1)

    def remote(src, dst, sems, **ids):
        return pltpu.make_async_remote_copy(
            src_ref=src, dst_ref=dst, send_sem=sems.at[0], recv_sem=sems.at[1],
            device_id=ids, device_id_type=pl.DeviceIdType.MESH,
        )

    loads = {}
    for t in outer + inner:
        loads[t] = pltpu.make_async_copy(v_ref.at[:, t], vst.at[t], load_sem.at[t])
        loads[t].start()
    load_links = pltpu.make_async_copy(g_ref, gst.at[pl.ds(0, 54 * all_tiles)], load_sem.at[planes])
    load_links.start()
    barrier = pltpu.get_barrier_semaphore()
    for db in range(bricks):
        for ds in range(2):
            if db or ds:
                pl.semaphore_signal(
                    barrier, inc=1, device_id={"brick": (b + db) % bricks, "sub": (s + ds) % 2},
                    device_id_type=pl.DeviceIdType.MESH,
                )
    pl.semaphore_signal(
        barrier, inc=1, device_id={"vec": 1 - v}, device_id_type=pl.DeviceIdType.MESH
    )

    def unpack(t):
        flat = vst.at[t].reshape(rows * 3 * tiles * 2, 128)
        step = 3 * tiles * 2
        for c in range(3):
            for first in range(0, rows, 16):
                for part in range(2):
                    for lane in range(0, tiles, 2):
                        at = part * plane + lane * 128
                        quad = []
                        for h in range(2):
                            start = (first + 8 * h) * step + c * tiles * 2 + lane * 2 + part
                            quad.append(
                                jnp.concatenate(
                                    [flat[pl.ds(start + 2 * i, 8, stride=step), :] for i in range(2)], axis=1
                                )
                            )
                            field0[t + 1, c, first + 8 * h : first + 8 * h + 8, at : at + 256] = quad[h]
                        k = (position[t] * 3 + c) * wide + at
                        right[first : first + 16, k : k + 256] = jnp.concatenate(quad, axis=0).astype(low)

    def link_rows(t, part, group):
        return jnp.concatenate(
            [
                gst[pl.ds(group * 16 * all_tiles + (t * tiles + lane) * 2 + part, 8, stride=2 * all_tiles), :]
                for lane in range(tiles)
            ],
            axis=1,
        ) * KAPPA

    for t in outer:
        loads[t].wait()
        unpack(t)
    load_links.wait()
    for part in range(2):
        both = jnp.concatenate([link_rows(last, part, 0), link_rows(last, part, 1)], axis=0)
        lsend[16 * part : 16 * part + 16, :] = both.astype(low)
    pl.semaphore_wait(barrier, 2 * bricks)
    up, down = (b + 1) % bricks, (b + bricks - 1) % bricks

    def halos(step, h, low_src, high_src):
        sems = halo_sem.at[step, h]
        return (
            remote(high_src, halo.at[step, h, 0], sems.at[0], brick=up),
            remote(low_src, halo.at[step, h, 1], sems.at[1], brick=down),
        )

    def own(t, h):
        at = position[t] * 3 * wide
        return right.at[16 * h : 16 * h + 16, at : at + 3 * wide]

    copies = {}
    links_up = remote(lsend, lrecv, link_sem, brick=up)
    for h in range(halves):
        copies[0, h] = halos(0, h, own(0, h), own(last, h))
        copies[1, h] = halos(1, h, hsend.at[h, 0], hsend.at[h, 1])
        for copy in copies[0, h]:
            copy.start()
        if h == 0:
            links_up.start()
    for t in inner:
        loads[t].wait()
        unpack(t)
    parts = (slice(0, cut), slice(cut, span))
    unit = 2 * rows

    def raw_copy(index, from_slot, to_slot, ks, **ids):
        return remote(
            right.at[from_slot * unit : from_slot * unit + rows, ks],
            right.at[to_slot * unit : to_slot * unit + rows, ks],
            raw_sem.at[index], **ids,
        )

    across = [raw_copy(i, 0, 2, parts[i], vec=1 - v) for i in range(2)]
    beside = raw_copy(2, 0, 1, slice(0, span), sub=1 - s)
    onward = [raw_copy(3 + i, 2, 3, parts[i], sub=1 - s) for i in range(2)]
    for copy in across + [beside]:
        copy.start()

    depth_wide = lax.broadcasted_iota(jnp.int32, (8, plane), 1) % LZ
    depth = lax.broadcasted_iota(jnp.int32, (8, 128), 1) % LZ

    def spread(t, carry):
        for part in range(2):
            for group in range(4):
                here = link_rows(t, part, group)
                if group > 0:
                    by = pltpu.roll(here, LZ, 1)
                    bz = jnp.where(
                        depth_wide == 0, pltpu.roll(here, plane - (LZ - 1), 1), pltpu.roll(here, 1, 1)
                    )
                for j in range(min(8, 27 - 8 * group)):
                    index = group * 8 + j
                    row = jnp.broadcast_to(here[j : j + 1], (8, plane))
                    table[t, index * 2 + part] = row
                    if index < 9:
                        table[t + 1, 54 + index * 2 + part] = row
                    else:
                        back = by if index < 18 else bz
                        table[t, 54 + index * 2 + part] = jnp.broadcast_to(back[j : j + 1], (8, plane))
        return carry

    lax.fori_loop(0, planes, spread, 0)

    places = []
    for group in range(0, all_tiles, 8):
        height = min(8, all_tiles - group)
        site = (
            lax.broadcasted_iota(jnp.int32, (height, 128), 0) * 128
            + lax.broadcasted_iota(jnp.int32, (height, 128), 1)
            + group * 128
        )
        places.append(
            (
                (site // plane + b * planes).astype(f32) * (1.0 / (bricks * planes)),
                (site // LZ % LY).astype(f32) * (1.0 / LY),
                (site % LZ).astype(f32) * (1.0 / LZ),
            )
        )

    def phases(q, carry):
        n = [mom_ref[d, jnp.minimum(q, count - 1)].astype(f32) for d in range(3)]
        for group, (x, y, z) in enumerate(places):
            turns = n[0] * x + n[1] * y + n[2] * z
            half = jnp.round(2.0 * turns)
            sign = 1.0 - 2.0 * jnp.abs(half - 2.0 * jnp.round(0.5 * half))
            angle = (2.0 * math.pi) * (turns - 0.5 * half)
            square = angle * angle
            cosine, sine = 0.0, 0.0
            for i in range(7, 0, -1):
                cosine = (cosine * square) + (-1.0) ** i / math.factorial(2 * i)
            cosine = sign * (1.0 + cosine * square)
            for i in range(6, 0, -1):
                sine = (sine * square) + (-1.0) ** i / math.factorial(2 * i + 1)
            sine = sign * (angle + angle * (sine * square))
            for j in range(x.shape[0]):
                at = (group * 8 + j) * 128
                cosb[q, :, at : at + 128] = jnp.broadcast_to(cosine[j : j + 1], (16, 128)).astype(low)
                sinb[q, :, at : at + 128] = jnp.broadcast_to(sine[j : j + 1], (16, 128)).astype(low)
        return carry

    lax.fori_loop(0, count, phases, 0)

    def shift(stage, k, to):
        step, t, h = stage
        rows_to = pl.ds(pl.multiple_of(k % 2 * 8, 8), 8)
        rows_at = pl.ds(pl.multiple_of(h * 16 + k % 2 * 8, 8), 8)
        first_lane = k // 2 * plane
        lanes = pl.ds(pl.multiple_of(first_lane, plane), plane)
        for c in range(3):
            w = fields[step][t + 1, c, rows_at, lanes]
            to[0, c, rows_to, lanes] = pltpu.roll(w, plane - LZ, 1)
            to[1, c, rows_to, lanes] = pltpu.roll(w, LZ, 1)
            for part in range(tiles):
                u = w[:, part * 128 : part * 128 + 128]
                here = pl.ds(pl.multiple_of(first_lane + part * 128, 128), 128)
                to[2, c, rows_to, here] = jnp.where(
                    depth == LZ - 1, pltpu.roll(u, LZ - 1, 1), pltpu.roll(u, 127, 1)
                )
                to[3, c, rows_to, here] = jnp.where(
                    depth == 0, pltpu.roll(u, 128 - (LZ - 1), 1), pltpu.roll(u, 1, 1)
                )

    def block(stage, lane, now):
        step, t, half = stage
        field = fields[step]
        lanes = (
            pl.ds(pl.multiple_of(lane * 128, 128), 128),
            pl.ds(pl.multiple_of(plane + lane * 128, 128), 128),
        )
        at_rows = [slice(half * 16 + 8 * h, half * 16 + 8 * h + 8) for h in range(2)]
        acc = {}
        for h in range(2):
            for r in range(3):
                for part in range(2):
                    mid = field[t + 1, r, at_rows[h], lanes[part]]
                    acc[h, r, part] = (1.0 - 6.0 * KAPPA) * mid
        for way in range(6):
            direction, back = way // 2, way % 2
            for c in range(3):
                sources = []
                for h in range(2):
                    if direction == 0:
                        p = t + 2 - 2 * back
                        sources.append([field[p, c, at_rows[h], lanes[i]] for i in range(2)])
                    else:
                        sources.append([now[way - 2, c, 8 * h : 8 * h + 8, lanes[i]] for i in range(2)])
                for r in range(3):
                    row = direction * 18 + (54 + c * 6 + r * 2 if back else r * 6 + c * 2)
                    ur = table[t, row, :, lanes[0]]
                    ui = table[t, row + 1, :, lanes[0]]
                    for h, (sr, si) in enumerate(sources):
                        if back:
                            acc[h, r, 0] = acc[h, r, 0] + (ur * sr + ui * si)
                            acc[h, r, 1] = acc[h, r, 1] + (ur * si - ui * sr)
                        else:
                            acc[h, r, 0] = acc[h, r, 0] + (ur * sr - ui * si)
                            acc[h, r, 1] = acc[h, r, 1] + (ur * si + ui * sr)
        both = slice(half * 16, half * 16 + 16)
        for r in range(3):
            for part in range(2):
                if step == 0:
                    for h in range(2):
                        field1[t + 1, r, at_rows[h], lanes[part]] = acc[h, r, part]
                if step == 1 or t in outer:
                    pair = jnp.concatenate([acc[0, r, part], acc[1, r, part]], axis=0).astype(low)
                    if step == 1:
                        smeared[position[t] * 3 + r, both, lanes[part]] = pair
                    else:
                        k_at = pl.ds(pl.multiple_of((2 * r + part) * plane + lane * 128, 128), 128)
                        hsend[half, outer.index(t), :, k_at] = pair

    stages = [(0, t, h) for h in range(halves) for t in inner]
    for h in range(halves):
        stages += [(0, t, h) for t in outer] + [(1, t, h) for t in inner]
    stages += [(1, t, h) for h in range(halves) for t in outer]

    def run(step, ts, h):
        for t in ts:
            i = stages.index((step, t, h))

            def trip(k, carry):
                shift(stages[(i + 1) % len(stages)], k, moved[(i + 1) % 2])
                block(stages[i], k, moved[i % 2])
                return carry

            lax.fori_loop(0, tiles, trip, 0)

    def begin(k, carry):
        shift(stages[0], k, moved[0])
        return carry

    lax.fori_loop(0, tiles, begin, 0)
    for h in range(halves):
        run(0, inner, h)

    def take(step, h, side):
        copies[step, h][side].wait_recv()
        for c in range(3):
            fields[step][planes + 1 if side else 0, c, 16 * h : 16 * h + 16] = (
                halo[step, h, side, :, c * wide : (c + 1) * wide].astype(f32)
            )

    links_up.wait_recv()
    for part in range(2):
        got = lrecv[16 * part : 16 * part + 16, :].astype(f32)
        for index in range(9):
            table[0, 54 + index * 2 + part] = jnp.broadcast_to(got[index : index + 1], (8, plane))
    for h in range(halves):
        for side in range(2):
            take(0, h, side)
            run(0, [outer[side]], h)
            copies[1, h][1 - side].start()
        if h == halves - 1:
            across[0].wait_recv()
            onward[0].start()
        run(1, inner, h)
    beside.wait_recv()
    onward[0].wait_recv()

    def fill(k, carry):
        re = pl.ds(pl.multiple_of(k * wide, wide), plane)
        im = pl.ds(pl.multiple_of(k * wide + plane, plane), plane)
        for slot in range(4):
            at_raw = slice(slot * unit, slot * unit + rows)
            at_turned = slice(slot * unit + rows, (slot + 1) * unit)
            right[at_turned, re] = -right[at_raw, im]
            right[at_turned, im] = right[at_raw, re]
        return carry

    ships = len(units)
    members = (inner, outer)
    order = [(half, e) for group in (range(0, 2), range(2, ships)) for half in range(2) for e in group]
    ready = lambda i: not (order[i][0] == 1 and order[i - 1][0] == 0)

    def turn(i):
        half, e = order[i]
        to = left[i % 2]
        for j, (q, h) in enumerate(units[e]):
            for n, t in enumerate(members[half]):
                for lane in range(0, plane, 256):
                    cosine = cosb[q, :, t * plane + lane : t * plane + lane + 256]
                    sine = sinb[q, :, t * plane + lane : t * plane + lane + 256]
                    for c in range(3):
                        k = position[t] * 3 + c
                        sr = smeared[k, 16 * h : 16 * h + 16, lane : lane + 256]
                        si = smeared[k, 16 * h : 16 * h + 16, plane + lane : plane + lane + 256]
                        col = (n * 3 + c) * wide + lane
                        to[16 * j : 16 * j + 16, col : col + 256] = cosine * sr + sine * si
                        to[16 * j : 16 * j + 16, col + plane : col + plane + 256] = cosine * si - sine * sr

    def product(i):
        half, e = order[i]
        columns = 16 * len(units[e])
        first = parts[half].start
        length = parts[half].stop - first
        pieces = []
        for k in range(0, length, length // 2):
            pieces.append(
                lax.dot_general(
                    right[:, first + k : first + k + length // 2],
                    left[i % 2][0:columns, k : k + length // 2],
                    (((1,), (1,)), ((), ())), preferred_element_type=f32,
                )
            )
        if i + 1 < len(order) and ready(i + 1):
            turn(i + 1)
        part = pieces[0] + pieces[1]
        if half == 0:
            total[e, :, 0:columns] = part
        else:
            part = ((total[e, :, 0:columns] + part) * scale).astype(low)
            parted[e, 0, :, 0:columns] = part[0 : 2 * unit]
            crossing[e, :, 0:columns] = part[2 * unit :]

    sizes = [128 * (-(-len(u) // 8)) for u in units]
    keeper = b % 2 == s
    pair_brick = b + 1 - 2 * (b % 2)
    far_brick = (b + 2) % 4
    near_hop = (v + b // 2) % 2

    def cross(e):
        return remote(
            crossing.at[e, :, 0 : sizes[e]], parted.at[e, 1, :, 0 : sizes[e]], cross_sem.at[e], vec=1 - v
        )

    def pair_up(e, hop):
        return remote(
            parted.at[e, hop, :, 0 : sizes[e]], paired.at[e, hop, :, 0 : sizes[e]],
            pair_sem.at[e, hop], brick=pair_brick,
        )

    def deliver(e, far, ds):
        src = summed.at[e, far, ds * unit : (ds + 1) * unit, 0 : sizes[e]]
        ids = {"brick": far_brick} if far else {}
        if ds:
            ids["sub"] = 1 - s
        return pltpu.make_async_remote_copy(
            src_ref=src, dst_ref=rx.at[e, far, :, 0 : sizes[e]],
            send_sem=last_sem.at[e, 2 * far + ds], recv_sem=last_sem.at[e, 4 + far],
            device_id=ids, device_id_type=pl.DeviceIdType.MESH,
        )

    def ship(e):
        cross(e).start()

        @pl.when(jnp.logical_not(keeper))
        def _():
            pair_up(e, 0).start()

    def hand_on(e):
        cross(e).wait_recv()

        @pl.when(jnp.logical_not(keeper))
        def _():
            pair_up(e, 1).start()

    def combine(e):
        @pl.when(keeper)
        def _():
            for hop in range(2):
                pair_up(e, hop).wait_recv()
            for far in (1, 0):
                hop = 1 - near_hop if far else near_hop
                both = parted[e, hop, :, 0 : sizes[e]].astype(f32) + paired[e, hop, :, 0 : sizes[e]].astype(f32)
                summed[e, far, :, 0 : sizes[e]] = both.astype(low)
                if far == 0:
                    rx[e, 0, :, 0 : sizes[e]] = both[0:unit].astype(low)
            deliver(e, 1, 0).start()
            deliver(e, 1, 1).start()
            deliver(e, 0, 1).start()

    def arrive(e):
        @pl.when(jnp.logical_not(keeper))
        def _():
            deliver(e, 0, 1).wait_recv()

        deliver(e, 1, 0).wait_recv()

    def fill_half(half):
        first = len(inner) * 3 if half else 0
        count_k = len(members[half]) * 3
        lax.fori_loop(first, first + count_k, fill, 0)

    hooks = {
        2: [(ship, 0)],
        3: [(ship, 1), (hand_on, 0)],
        4: [(hand_on, 1), (combine, 0)],
        5: [(combine, 1)],
        6: [(ship, 2)],
        7: [(ship, 3), (hand_on, 2), (combine, 2), (hand_on, 3), (combine, 3)],
    }
    for i, (half, e) in enumerate(order):
        if i == 0:
            fill_half(0)
        if i == 2:
            across[1].wait_recv()
            onward[1].start()
        if i in (2, 6):
            for side in range(2):
                take(1, i // 4, side)
                run(1, [outer[side]], i // 4)
        if i == 2:
            onward[1].wait_recv()
            fill_half(1)
        if i == 0 or not ready(i):
            turn(i)
        product(i)
        for act, which in hooks.get(i, ()):
            act(which)
    lane_at = lax.broadcasted_iota(jnp.int32, (8, 128), 1)
    places = {pair: (e, 16 * j) for e, u in enumerate(units) for j, pair in enumerate(u)}
    for e in range(ships):
        arrive(e)
    for q in range(count):
        for first in range(0, unit, 8):
            pieces = []
            for h in range(halves):
                e, at = places[q, h]
                tile = slice(at // 128 * 128, at // 128 * 128 + 128)
                rows_at = slice(first // 16 * 16, first // 16 * 16 + 16)
                got = rx[e, 0, rows_at, tile].astype(f32) + rx[e, 1, rows_at, tile].astype(f32)
                got = got[first % 16 : first % 16 + 8]
                turned = (16 * h - at) % 128
                pieces.append(pltpu.roll(got, turned, 1) if turned else got)
            value = jnp.where(lane_at < 16, pieces[0], pieces[1])
            start = (first % rows) * 2 * count + 2 * q + first // rows
            out_ref[pl.ds(start, 8, stride=2 * count), :] = value[:, 0:rows]
    sent = [links_up, *across, beside, *onward]
    for copy in copies.values():
        sent += copy
    sent += [cross(e) for e in range(ships)]
    for copy in sent:
        copy.wait_send()
    for e in range(ships):
        @pl.when(keeper)
        def _():
            deliver(e, 1, 0).wait_send()
            deliver(e, 1, 1).wait_send()
            deliver(e, 0, 1).wait_send()

        @pl.when(jnp.logical_not(keeper))
        def _():
            pair_up(e, 0).wait_send()
            pair_up(e, 1).wait_send()


def shards_fused(vectors, gauge_links, momenta):
    plane = LY * LZ
    rows, local_sites = vectors.shape[0], vectors.shape[3]
    planes = local_sites // plane
    tiles = plane // 128
    bricks = lax.axis_size("brick")
    count = momenta.shape[0]
    halves = rows // 16
    even = count // 8 * 8
    split = even * 2 // 3 // 8 * 8
    units = [[(q, 0) for q in range(split)], [(q, 0) for q in range(split, even)]]
    units += [[(q, 1) for q in range(split)], [(q, 1) for q in range(split, even)]]
    units[3] += [(q, h) for q in range(even, count) for h in range(halves)]
    ships, most_units = len(units), max(len(u) for u in units)
    width = 128 * (-(-most_units // 8))
    low, f32 = jnp.bfloat16, jnp.float32
    v = vectors.reshape((rows, 3, 2, planes * tiles, 128)).transpose((0, 1, 3, 2, 4))
    v = v.reshape((rows * 3, planes, tiles * 2, 128))
    g = gauge_links.reshape((27, 2, planes * tiles, 128)).transpose((0, 2, 1, 3))
    g = g.reshape((54 * planes * tiles, 128))
    wide = 2 * plane
    most = max(2, planes - 2) * 3 * wide
    scale = (3.0 * bricks * local_sites) ** (-0.5)
    vmem, dma = pltpu.VMEM, pltpu.SemaphoreType.DMA
    plan = (planes, rows, count, bricks, units, scale)
    out = pl.pallas_call(
        functools.partial(fused_kernel, plan),
        out_shape=jax.ShapeDtypeStruct((rows * count * 2, rows), f32),
        in_specs=[
            pl.BlockSpec(memory_space=pltpu.SMEM),
            pl.BlockSpec(memory_space=pl.ANY),
            pl.BlockSpec(memory_space=pl.ANY),
        ],
        out_specs=pl.BlockSpec(memory_space=pltpu.VMEM),
        scratch_shapes=[
            vmem((planes, rows * 3, tiles * 2, 128), f32),
            vmem((64 * planes * tiles, 128), f32),
            vmem((planes + 2, 3, rows, wide), f32),
            vmem((planes + 2, 3, rows, wide), f32),
            vmem((planes + 1, 108, 8, plane), f32),
            vmem((4, 3, 16, wide), f32),
            vmem((4, 3, 16, wide), f32),
            vmem((8 * rows, planes * 3 * wide), low),
            vmem((planes * 3, rows, wide), low),
            vmem((16 * most_units, most), low),
            vmem((16 * most_units, most), low),
            vmem((count, 16, local_sites), low),
            vmem((count, 16, local_sites), low),
            vmem((ships, 8 * rows, width), f32),
            vmem((ships, 2, 4 * rows, width), low),
            vmem((ships, 4 * rows, width), low),
            vmem((ships, 2, 4 * rows, width), low),
            vmem((ships, 2, 4 * rows, width), low),
            vmem((ships, 2, 2 * rows, width), low),
            vmem((2, halves, 2, 16, 3 * wide), low),
            vmem((halves, 2, 16, 3 * wide), low),
            vmem((32, plane), low),
            vmem((32, plane), low),
            dma((planes + 1,)),
            dma((2, halves, 2, 2)),
            dma((2,)),
            dma((5, 2)),
            dma((ships, 2)),
            dma((ships, 2, 2)),
            dma((ships, 6)),
        ],
        compiler_params=pltpu.CompilerParams(
            vmem_limit_bytes=60 * 2**20, collective_id=0, has_side_effects=True
        ),
        name="elementals",
    )(momenta.T, v, g)
    return out.reshape((rows, count, 2, rows))


def choose(vectors, gauge_links, momenta):
    plane = LY * LZ
    bricks, vecs, subs = (lax.axis_size(a) for a in ("brick", "vec", "sub"))
    rows, local_sites = vectors.shape[0], vectors.shape[3]
    fits = local_sites % plane == 0 and 3 <= local_sites // plane <= 4 and rows == 32
    if fits and vecs == 2 and subs == 2 and bricks == 4 and 24 <= momenta.shape[0] < 32:
        return shards_fused(vectors, gauge_links, momenta)
    return shards(vectors, gauge_links, momenta)


def solution(mesh):
    in_specs = (
        P(("vec", "sub"), None, None, ("grp", "brick")),
        P(None, None, None, None, ("grp", "brick")),
        P(),
    )
    out_specs = P(("vec", "sub"), "grp", None, "brick")
    return jax.shard_map(choose, mesh=mesh, in_specs=in_specs, out_specs=out_specs, check_vma=False)
```

```python
import functools
import math

import jax
import jax.numpy as jnp
from jax import lax
from jax.experimental import pallas as pl
from jax.experimental.pallas import tpu as pltpu
from jax.sharding import PartitionSpec as P

LY = 64
LZ = 8
ITERS = 2


KAPPA = 0.125


def from_behind(array, axis, by):
    peers = lax.axis_size(axis)
    return lax.ppermute(array, axis, [(i, (i + by) % peers) for i in range(peers)])


def padded_2(array, sides, width):
    for axis, dim in sides:
        peers, length = (lax.axis_size(axis), array.shape[dim])
        up = [(i, (i + 1) % peers) for i in range(peers)]
        down = [(j, i) for i, j in up]
        last = lax.slice_in_dim(array, length - width, length, axis=dim)
        initial = lax.slice_in_dim(array, 0, width, axis=dim)
        before = lax.ppermute(last, axis, up)
        after = lax.ppermute(initial, axis, down)
        array = jnp.concatenate([before, array, after], axis=dim)
    return array


def matrix_apply(matrix, source):
    matrix_real = matrix[:, :, 0][None]
    matrix_imag = matrix[:, :, 1][None]
    source_real = source[:, None, :, 0]
    source_imag = source[:, None, :, 1]
    real_part = jnp.sum(matrix_real * source_real - matrix_imag * source_imag, axis=2)
    imag_part = jnp.sum(matrix_real * source_imag + matrix_imag * source_real, axis=2)
    return jnp.stack([real_part, imag_part], axis=2)


def adjoint(matrix):
    return jnp.stack(
        [jnp.swapaxes(matrix[:, :, 0], 0, 1), -jnp.swapaxes(matrix[:, :, 1], 0, 1)], axis=2
    )


def step_depth(values, offset):
    depth_index = lax.iota(jnp.int32, values.shape[-1]) % LZ
    if offset > 0:
        return jnp.where(
            depth_index == LZ - 1, jnp.roll(values, LZ - 1, -1), jnp.roll(values, -1, -1)
        )
    return jnp.where(depth_index == 0, jnp.roll(values, 1 - LZ, -1), jnp.roll(values, 1, -1))


def step_column(values, offset):
    plane = LY * LZ
    column_index = lax.iota(jnp.int32, values.shape[-1]) // LZ % LY
    if offset > 0:
        return jnp.where(
            column_index == LY - 1, jnp.roll(values, plane - LZ, -1), jnp.roll(values, -LZ, -1)
        )
    return jnp.where(column_index == 0, jnp.roll(values, LZ - plane, -1), jnp.roll(values, LZ, -1))


def laplace_step(center, ahead, behind, here_links, back_links):
    forward = matrix_apply(here_links[0], ahead)
    backward = matrix_apply(adjoint(back_links), behind)
    total = forward + backward
    for direction, stepper in ((1, step_column), (2, step_depth)):
        forward = matrix_apply(here_links[direction], stepper(center, 1))
        backward = matrix_apply(adjoint(stepper(here_links[direction], -1)), stepper(center, -1))
        total = total + (forward + backward)
    return center + KAPPA * (total - 6.0 * center)


def shards(vectors, gauge_links, momenta):
    plane = LY * LZ
    local_sites = vectors.shape[3]
    raw_low = vectors.astype(jnp.bfloat16)
    field = vectors
    x_links = gauge_links[0]
    rim = from_behind(x_links[..., local_sites - plane :], "brick", 1)
    back_links = jnp.concatenate([rim, x_links[..., : local_sites - plane]], axis=3)
    for step in range(ITERS):
        padded = padded_2(field, (("brick", 3),), plane)
        field = laplace_step(
            padded[..., plane : plane + local_sites],
            padded[..., 2 * plane :],
            padded[..., :local_sites],
            gauge_links,
            back_links,
        )
    smeared_low = field.astype(jnp.bfloat16)
    raw_sites, smeared_sites = (
        lax.all_to_all(raw_low, ("vec", "sub"), split_axis=3, concat_axis=0, tiled=True),
        lax.all_to_all(smeared_low, ("vec", "sub"), split_axis=3, concat_axis=0, tiled=True),
    )
    groups = lax.axis_size(("vec", "sub"))
    total_vec = raw_sites.shape[0]
    width = raw_sites.shape[3]
    total_x = lax.axis_size("brick") * (local_sites // plane)
    first_site = lax.axis_index("brick") * local_sites + lax.axis_index(("vec", "sub")) * width
    site = first_site + lax.iota(jnp.int32, width)
    layer_index = (site // plane)[None]
    column_index = (site // LZ % LY)[None]
    depth_index = (site % LZ)[None]
    fraction = (
        jnp.mod(momenta[:, 0:1] * layer_index, total_x).astype(jnp.float32) / total_x
        + jnp.mod(momenta[:, 1:2] * column_index, LY).astype(jnp.float32) / LY
        + jnp.mod(momenta[:, 2:3] * depth_index, LZ).astype(jnp.float32) / LZ
    )
    angle = 2.0 * math.pi * fraction
    cosines = jnp.cos(angle)
    sines = jnp.sin(angle)
    right = smeared_sites.reshape((total_vec, 6 * width))
    scale = (3.0 * total_x * plane) ** (-0.5)

    def one_momentum(angles):
        cosine, sine = angles
        real_part = raw_sites[:, :, 0] * cosine - raw_sites[:, :, 1] * sine
        imag_part = raw_sites[:, :, 0] * sine + raw_sites[:, :, 1] * cosine
        phased = jnp.stack([real_part, imag_part], axis=2).astype(jnp.bfloat16)
        turned = jnp.stack([-phased[:, :, 1], phased[:, :, 0]], axis=2)
        left = jnp.concatenate(
            [
                phased.reshape((lax.axis_size(("vec", "sub")) * (total_vec // groups), 6 * width)),
                turned.reshape((lax.axis_size(("vec", "sub")) * (total_vec // groups), 6 * width)),
            ],
            axis=0,
        )
        product = lax.dot_general(
            left, right, (((1,), (1,)), ((), ())), preferred_element_type=jnp.float32
        )
        return product.reshape(
            (2, lax.axis_size(("vec", "sub")) * (total_vec // groups), total_vec)
        )

    blocks = lax.map(one_momentum, (cosines, sines))
    shares = lax.psum_scatter(
        jnp.transpose(blocks, (2, 0, 1, 3)) * scale, ("vec", "sub"), scatter_dimension=0, tiled=True
    )
    return lax.psum_scatter(shares, "brick", scatter_dimension=3, tiled=True)


def fused_kernel(plan, mom_ref, v_ref, g_ref, out_ref, *scratch):
    (vst, gst, field0, field1, table, moved0, moved1, right, smeared, left0, left1, cosb, sinb, total, parted,
     crossing, rx, halo, hsend, lsend, lrecv, load_sem, halo_sem, link_sem, raw_sem, cross_sem, last_sem) = scratch
    planes, rows, count, bricks, units, scale = plan
    fields, moved = (field0, field1), (moved0, moved1)
    halves = rows // 16
    plane = LY * LZ
    tiles = plane // 128
    all_tiles = planes * tiles
    f32, low = jnp.float32, jnp.bfloat16
    wide = 2 * plane
    last = planes - 1
    inner = list(range(1, last))
    outer = [0, last]
    position = {t: i for i, t in enumerate(inner + outer)}
    cut = len(inner) * 3 * wide
    span = planes * 3 * wide
    b, v, s = (lax.axis_index(a) for a in ("brick", "vec", "sub"))
    left = (left0, left1)

    def remote(src, dst, sems, **ids):
        return pltpu.make_async_remote_copy(
            src_ref=src, dst_ref=dst, send_sem=sems.at[0], recv_sem=sems.at[1],
            device_id=ids, device_id_type=pl.DeviceIdType.MESH,
        )

    loads = {}
    for t in outer + inner:
        loads[t] = pltpu.make_async_copy(v_ref.at[:, t], vst.at[t], load_sem.at[t])
        loads[t].start()
    load_links = pltpu.make_async_copy(g_ref, gst.at[pl.ds(0, 54 * all_tiles)], load_sem.at[planes])
    load_links.start()
    barrier = pltpu.get_barrier_semaphore()
    for db in range(bricks):
        for ds in range(2):
            if db or ds:
                pl.semaphore_signal(
                    barrier, inc=1, device_id={"brick": (b + db) % bricks, "sub": (s + ds) % 2},
                    device_id_type=pl.DeviceIdType.MESH,
                )
    pl.semaphore_signal(
        barrier, inc=1, device_id={"vec": 1 - v}, device_id_type=pl.DeviceIdType.MESH
    )

    def unpack(t):
        flat = vst.at[t].reshape(rows * 3 * tiles * 2, 128)
        step = 3 * tiles * 2
        for c in range(3):
            for first in range(0, rows, 16):
                for part in range(2):
                    for lane in range(0, tiles, 2):
                        at = part * plane + lane * 128
                        quad = []
                        for h in range(2):
                            start = (first + 8 * h) * step + c * tiles * 2 + lane * 2 + part
                            quad.append(
                                jnp.concatenate(
                                    [flat[pl.ds(start + 2 * i, 8, stride=step), :] for i in range(2)], axis=1
                                )
                            )
                            field0[t + 1, c, first + 8 * h : first + 8 * h + 8, at : at + 256] = quad[h]
                        k = (position[t] * 3 + c) * wide + at
                        right[first : first + 16, k : k + 256] = jnp.concatenate(quad, axis=0).astype(low)

    def link_rows(t, part, group):
        return jnp.concatenate(
            [
                gst[pl.ds(group * 16 * all_tiles + (t * tiles + lane) * 2 + part, 8, stride=2 * all_tiles), :]
                for lane in range(tiles)
            ],
            axis=1,
        ) * KAPPA

    for t in outer:
        loads[t].wait()
        unpack(t)
    load_links.wait()
    for part in range(2):
        both = jnp.concatenate([link_rows(last, part, 0), link_rows(last, part, 1)], axis=0)
        lsend[16 * part : 16 * part + 16, :] = both.astype(low)
    pl.semaphore_wait(barrier, 2 * bricks)
    up, down = (b + 1) % bricks, (b + bricks - 1) % bricks

    def halos(step, h, low_src, high_src):
        sems = halo_sem.at[step, h]
        return (
            remote(high_src, halo.at[step, h, 0], sems.at[0], brick=up),
            remote(low_src, halo.at[step, h, 1], sems.at[1], brick=down),
        )

    def own(t, h):
        at = position[t] * 3 * wide
        return right.at[16 * h : 16 * h + 16, at : at + 3 * wide]

    copies = {}
    links_up = remote(lsend, lrecv, link_sem, brick=up)
    for h in range(halves):
        copies[0, h] = halos(0, h, own(0, h), own(last, h))
        copies[1, h] = halos(1, h, hsend.at[h, 0], hsend.at[h, 1])
        for copy in copies[0, h]:
            copy.start()
        if h == 0:
            links_up.start()
    for t in inner:
        loads[t].wait()
        unpack(t)
    parts = (slice(0, cut), slice(cut, span))
    unit = 2 * rows

    def raw_copy(index, from_slot, to_slot, ks, **ids):
        return remote(
            right.at[from_slot * unit : from_slot * unit + rows, ks],
            right.at[to_slot * unit : to_slot * unit + rows, ks],
            raw_sem.at[index], **ids,
        )

    across = [raw_copy(i, 0, 2, parts[i], vec=1 - v) for i in range(2)]
    beside = raw_copy(2, 0, 1, slice(0, span), sub=1 - s)
    onward = [raw_copy(3 + i, 2, 3, parts[i], sub=1 - s) for i in range(2)]
    for copy in across + [beside]:
        copy.start()

    depth_wide = lax.broadcasted_iota(jnp.int32, (8, plane), 1) % LZ
    depth = lax.broadcasted_iota(jnp.int32, (8, 128), 1) % LZ

    def spread(t, carry):
        for part in range(2):
            for group in range(4):
                here = link_rows(t, part, group)
                if group > 0:
                    by = pltpu.roll(here, LZ, 1)
                    bz = jnp.where(
                        depth_wide == 0, pltpu.roll(here, plane - (LZ - 1), 1), pltpu.roll(here, 1, 1)
                    )
                for j in range(min(8, 27 - 8 * group)):
                    index = group * 8 + j
                    row = jnp.broadcast_to(here[j : j + 1], (8, plane))
                    table[t, index * 2 + part] = row
                    if index < 9:
                        table[t + 1, 54 + index * 2 + part] = row
                    else:
                        back = by if index < 18 else bz
                        table[t, 54 + index * 2 + part] = jnp.broadcast_to(back[j : j + 1], (8, plane))
        return carry

    lax.fori_loop(0, planes, spread, 0)

    places = []
    for group in range(0, all_tiles, 8):
        height = min(8, all_tiles - group)
        site = (
            lax.broadcasted_iota(jnp.int32, (height, 128), 0) * 128
            + lax.broadcasted_iota(jnp.int32, (height, 128), 1)
            + group * 128
        )
        places.append(
            (
                (site // plane + b * planes).astype(f32) * (1.0 / (bricks * planes)),
                (site // LZ % LY).astype(f32) * (1.0 / LY),
                (site % LZ).astype(f32) * (1.0 / LZ),
            )
        )

    def phases(q, carry):
        n = [mom_ref[d, jnp.minimum(q, count - 1)].astype(f32) for d in range(3)]
        for group, (x, y, z) in enumerate(places):
            turns = n[0] * x + n[1] * y + n[2] * z
            half = jnp.round(2.0 * turns)
            sign = 1.0 - 2.0 * jnp.abs(half - 2.0 * jnp.round(0.5 * half))
            angle = (2.0 * math.pi) * (turns - 0.5 * half)
            square = angle * angle
            cosine, sine = 0.0, 0.0
            for i in range(7, 0, -1):
                cosine = (cosine * square) + (-1.0) ** i / math.factorial(2 * i)
            cosine = sign * (1.0 + cosine * square)
            for i in range(6, 0, -1):
                sine = (sine * square) + (-1.0) ** i / math.factorial(2 * i + 1)
            sine = sign * (angle + angle * (sine * square))
            for j in range(x.shape[0]):
                at = (group * 8 + j) * 128
                cosb[q, :, at : at + 128] = jnp.broadcast_to(cosine[j : j + 1], (16, 128)).astype(low)
                sinb[q, :, at : at + 128] = jnp.broadcast_to(sine[j : j + 1], (16, 128)).astype(low)
        return carry

    lax.fori_loop(0, count, phases, 0)

    def shift(stage, k, to):
        step, t, h = stage
        rows_to = pl.ds(pl.multiple_of(k % 2 * 8, 8), 8)
        rows_at = pl.ds(pl.multiple_of(h * 16 + k % 2 * 8, 8), 8)
        first_lane = k // 2 * plane
        lanes = pl.ds(pl.multiple_of(first_lane, plane), plane)
        for c in range(3):
            w = fields[step][t + 1, c, rows_at, lanes]
            to[0, c, rows_to, lanes] = pltpu.roll(w, plane - LZ, 1)
            to[1, c, rows_to, lanes] = pltpu.roll(w, LZ, 1)
            for part in range(tiles):
                u = w[:, part * 128 : part * 128 + 128]
                here = pl.ds(pl.multiple_of(first_lane + part * 128, 128), 128)
                to[2, c, rows_to, here] = jnp.where(
                    depth == LZ - 1, pltpu.roll(u, LZ - 1, 1), pltpu.roll(u, 127, 1)
                )
                to[3, c, rows_to, here] = jnp.where(
                    depth == 0, pltpu.roll(u, 128 - (LZ - 1), 1), pltpu.roll(u, 1, 1)
                )

    def block(stage, lane, now):
        step, t, half = stage
        field = fields[step]
        lanes = (
            pl.ds(pl.multiple_of(lane * 128, 128), 128),
            pl.ds(pl.multiple_of(plane + lane * 128, 128), 128),
        )
        at_rows = [slice(half * 16 + 8 * h, half * 16 + 8 * h + 8) for h in range(2)]
        acc = {}
        for h in range(2):
            for r in range(3):
                for part in range(2):
                    mid = field[t + 1, r, at_rows[h], lanes[part]]
                    acc[h, r, part] = (1.0 - 6.0 * KAPPA) * mid
        for way in range(6):
            direction, back = way // 2, way % 2
            for c in range(3):
                sources = []
                for h in range(2):
                    if direction == 0:
                        p = t + 2 - 2 * back
                        sources.append([field[p, c, at_rows[h], lanes[i]] for i in range(2)])
                    else:
                        sources.append([now[way - 2, c, 8 * h : 8 * h + 8, lanes[i]] for i in range(2)])
                for r in range(3):
                    row = direction * 18 + (54 + c * 6 + r * 2 if back else r * 6 + c * 2)
                    ur = table[t, row, :, lanes[0]]
                    ui = table[t, row + 1, :, lanes[0]]
                    for h, (sr, si) in enumerate(sources):
                        if back:
                            acc[h, r, 0] = acc[h, r, 0] + (ur * sr + ui * si)
                            acc[h, r, 1] = acc[h, r, 1] + (ur * si - ui * sr)
                        else:
                            acc[h, r, 0] = acc[h, r, 0] + (ur * sr - ui * si)
                            acc[h, r, 1] = acc[h, r, 1] + (ur * si + ui * sr)
        both = slice(half * 16, half * 16 + 16)
        for r in range(3):
            for part in range(2):
                if step == 0:
                    for h in range(2):
                        field1[t + 1, r, at_rows[h], lanes[part]] = acc[h, r, part]
                if step == 1 or t in outer:
                    pair = jnp.concatenate([acc[0, r, part], acc[1, r, part]], axis=0).astype(low)
                    if step == 1:
                        smeared[position[t] * 3 + r, both, lanes[part]] = pair
                    else:
                        k_at = pl.ds(pl.multiple_of((2 * r + part) * plane + lane * 128, 128), 128)
                        hsend[half, outer.index(t), :, k_at] = pair

    stages = [(0, t, h) for h in range(halves) for t in inner]
    for h in range(halves):
        stages += [(0, t, h) for t in outer] + [(1, t, h) for t in inner]
    stages += [(1, t, h) for h in range(halves) for t in outer]

    def run(step, ts, h):
        for t in ts:
            i = stages.index((step, t, h))

            def trip(k, carry):
                shift(stages[(i + 1) % len(stages)], k, moved[(i + 1) % 2])
                block(stages[i], k, moved[i % 2])
                return carry

            lax.fori_loop(0, tiles, trip, 0)

    def begin(k, carry):
        shift(stages[0], k, moved[0])
        return carry

    lax.fori_loop(0, tiles, begin, 0)
    for h in range(halves):
        run(0, inner, h)

    def take(step, h, side):
        copies[step, h][side].wait_recv()
        for c in range(3):
            fields[step][planes + 1 if side else 0, c, 16 * h : 16 * h + 16] = (
                halo[step, h, side, :, c * wide : (c + 1) * wide].astype(f32)
            )

    links_up.wait_recv()
    for part in range(2):
        got = lrecv[16 * part : 16 * part + 16, :].astype(f32)
        for index in range(9):
            table[0, 54 + index * 2 + part] = jnp.broadcast_to(got[index : index + 1], (8, plane))
    for h in range(halves):
        for side in range(2):
            take(0, h, side)
            run(0, [outer[side]], h)
            copies[1, h][1 - side].start()
        if h == halves - 1:
            across[0].wait_recv()
            onward[0].start()
        run(1, inner, h)
    beside.wait_recv()
    onward[0].wait_recv()

    def fill(k, carry):
        re = pl.ds(pl.multiple_of(k * wide, wide), plane)
        im = pl.ds(pl.multiple_of(k * wide + plane, plane), plane)
        for slot in range(4):
            at_raw = slice(slot * unit, slot * unit + rows)
            at_turned = slice(slot * unit + rows, (slot + 1) * unit)
            right[at_turned, re] = -right[at_raw, im]
            right[at_turned, im] = right[at_raw, re]
        return carry

    ships = len(units)
    members = (inner, outer)
    order = [(half, e) for group in (range(0, 2), range(2, ships)) for half in range(2) for e in group]
    ready = lambda i: not (order[i][0] == 1 and order[i - 1][0] == 0)

    def turn(i):
        half, e = order[i]
        to = left[i % 2]
        for j, (q, h) in enumerate(units[e]):
            for n, t in enumerate(members[half]):
                for lane in range(0, plane, 256):
                    cosine = cosb[q, :, t * plane + lane : t * plane + lane + 256]
                    sine = sinb[q, :, t * plane + lane : t * plane + lane + 256]
                    for c in range(3):
                        k = position[t] * 3 + c
                        sr = smeared[k, 16 * h : 16 * h + 16, lane : lane + 256]
                        si = smeared[k, 16 * h : 16 * h + 16, plane + lane : plane + lane + 256]
                        col = (n * 3 + c) * wide + lane
                        to[16 * j : 16 * j + 16, col : col + 256] = cosine * sr + sine * si
                        to[16 * j : 16 * j + 16, col + plane : col + plane + 256] = cosine * si - sine * sr

    def product(i):
        half, e = order[i]
        columns = 16 * len(units[e])
        first = parts[half].start
        length = parts[half].stop - first
        pieces = []
        for k in range(0, length, length // 2):
            pieces.append(
                lax.dot_general(
                    right[:, first + k : first + k + length // 2],
                    left[i % 2][0:columns, k : k + length // 2],
                    (((1,), (1,)), ((), ())), preferred_element_type=f32,
                )
            )
        if i + 1 < len(order) and ready(i + 1):
            turn(i + 1)
        part = pieces[0] * scale + pieces[1] * scale
        if half == 0:
            total[e, :, 0:columns] = part
        else:
            part = (total[e, :, 0:columns] + part).astype(low)
            parted[e, 0, :, 0:columns] = part[0 : 2 * unit]
            crossing[e, :, 0:columns] = part[2 * unit :]

    sizes = [128 * (-(-len(u) // 8)) for u in units]
    roots = (v * 2 + s, (1 - v) * 2 + s)

    def cross(e):
        return remote(
            crossing.at[e, :, 0 : sizes[e]], parted.at[e, 1, :, 0 : sizes[e]], cross_sem.at[e], vec=1 - v
        )

    def ends(e, hop, ds):
        src = parted.at[e, hop, ds * unit : (ds + 1) * unit, 0 : sizes[e]]
        return src, rx.at[e, b, :, 0 : sizes[e]]

    def far(e, hop, ds):
        src, dst = ends(e, hop, ds)
        return pltpu.make_async_remote_copy(
            src_ref=src, dst_ref=dst,
            send_sem=last_sem.at[e, bricks + hop * 2 + ds], recv_sem=last_sem.at[e, b],
            device_id={"brick": roots[hop], "sub": (s + ds) % 2}, device_id_type=pl.DeviceIdType.MESH,
        )

    def depart(e, hop):
        far(e, hop, 1).start()

        @pl.when(roots[hop] != b)
        def _():
            far(e, hop, 0).start()

        @pl.when(roots[hop] == b)
        def _():
            src, dst = ends(e, hop, 0)
            pltpu.make_async_copy(src, dst, last_sem.at[e, b]).start()

    def ship(e):
        cross(e).start()
        depart(e, 0)

    def hand_on(e):
        cross(e).wait_recv()
        depart(e, 1)

    def arrive(e):
        for i in range(bricks):
            dst = rx.at[e, i, :, 0 : sizes[e]]
            pltpu.make_async_copy(dst, dst, last_sem.at[e, i]).wait()

    def fill_half(half):
        first = len(inner) * 3 if half else 0
        count_k = len(members[half]) * 3
        lax.fori_loop(first, first + count_k, fill, 0)

    hooks = {
        2: [(ship, 0)],
        3: [(ship, 1), (hand_on, 0)],
        4: [(hand_on, 1)],
        6: [(ship, 2)],
        7: [(ship, 3), (hand_on, 2), (hand_on, 3)],
    }
    for i, (half, e) in enumerate(order):
        if i == 0:
            fill_half(0)
        if i == 2:
            across[1].wait_recv()
            onward[1].start()
        if i in (2, 6):
            for side in range(2):
                take(1, i // 4, side)
                run(1, [outer[side]], i // 4)
        if i == 2:
            onward[1].wait_recv()
            fill_half(1)
        if i == 0 or not ready(i):
            turn(i)
        product(i)
        for act, which in hooks.get(i, ()):
            act(which)
    lane_at = lax.broadcasted_iota(jnp.int32, (8, 128), 1)
    places = {pair: (e, 16 * j) for e, u in enumerate(units) for j, pair in enumerate(u)}
    for e in range(ships):
        arrive(e)
    for q in range(count):
        for first in range(0, unit, 8):
            pieces = []
            for h in range(halves):
                e, at = places[q, h]
                tile = slice(at // 128 * 128, at // 128 * 128 + 128)
                rows_at = slice(first // 16 * 16, first // 16 * 16 + 16)
                got = [rx[e, i, rows_at, tile].astype(f32) for i in range(bricks)]
                got = (got[0] + got[1]) + (got[2] + got[3])
                got = got[first % 16 : first % 16 + 8]
                turned = (16 * h - at) % 128
                pieces.append(pltpu.roll(got, turned, 1) if turned else got)
            value = jnp.where(lane_at < 16, pieces[0], pieces[1])
            start = (first % rows) * 2 * count + 2 * q + first // rows
            out_ref[pl.ds(start, 8, stride=2 * count), :] = value[:, 0:rows]
    sent = [links_up, *across, beside, *onward]
    for copy in copies.values():
        sent += copy
    sent += [cross(e) for e in range(ships)]
    for copy in sent:
        copy.wait_send()
    for e in range(ships):
        for hop in range(2):
            far(e, hop, 1).wait_send()

            @pl.when(roots[hop] != b)
            def _():
                far(e, hop, 0).wait_send()


def shards_fused(vectors, gauge_links, momenta):
    plane = LY * LZ
    rows, local_sites = vectors.shape[0], vectors.shape[3]
    planes = local_sites // plane
    tiles = plane // 128
    bricks = lax.axis_size("brick")
    count = momenta.shape[0]
    halves = rows // 16
    even = count // 8 * 8
    split = even * 2 // 3 // 8 * 8
    units = [[(q, 0) for q in range(split)], [(q, 0) for q in range(split, even)]]
    units += [[(q, 1) for q in range(split)], [(q, 1) for q in range(split, even)]]
    units[3] += [(q, h) for q in range(even, count) for h in range(halves)]
    ships, most_units = len(units), max(len(u) for u in units)
    width = 128 * (-(-most_units // 8))
    low, f32 = jnp.bfloat16, jnp.float32
    v = vectors.reshape((rows, 3, 2, planes * tiles, 128)).transpose((0, 1, 3, 2, 4))
    v = v.reshape((rows * 3, planes, tiles * 2, 128))
    g = gauge_links.reshape((27, 2, planes * tiles, 128)).transpose((0, 2, 1, 3))
    g = g.reshape((54 * planes * tiles, 128))
    wide = 2 * plane
    most = max(2, planes - 2) * 3 * wide
    scale = (3.0 * bricks * local_sites) ** (-0.5)
    vmem, dma = pltpu.VMEM, pltpu.SemaphoreType.DMA
    plan = (planes, rows, count, bricks, units, scale)
    out = pl.pallas_call(
        functools.partial(fused_kernel, plan),
        out_shape=jax.ShapeDtypeStruct((rows * count * 2, rows), f32),
        in_specs=[
            pl.BlockSpec(memory_space=pltpu.SMEM),
            pl.BlockSpec(memory_space=pl.ANY),
            pl.BlockSpec(memory_space=pl.ANY),
        ],
        out_specs=pl.BlockSpec(memory_space=pltpu.VMEM),
        scratch_shapes=[
            vmem((planes, rows * 3, tiles * 2, 128), f32),
            vmem((64 * planes * tiles, 128), f32),
            vmem((planes + 2, 3, rows, wide), f32),
            vmem((planes + 2, 3, rows, wide), f32),
            vmem((planes + 1, 108, 8, plane), f32),
            vmem((4, 3, 16, wide), f32),
            vmem((4, 3, 16, wide), f32),
            vmem((8 * rows, planes * 3 * wide), low),
            vmem((planes * 3, rows, wide), low),
            vmem((16 * most_units, most), low),
            vmem((16 * most_units, most), low),
            vmem((count, 16, local_sites), low),
            vmem((count, 16, local_sites), low),
            vmem((ships, 8 * rows, width), f32),
            vmem((ships, 2, 4 * rows, width), low),
            vmem((ships, 4 * rows, width), low),
            vmem((ships, bricks, 2 * rows, width), low),
            vmem((2, halves, 2, 16, 3 * wide), low),
            vmem((halves, 2, 16, 3 * wide), low),
            vmem((32, plane), low),
            vmem((32, plane), low),
            dma((planes + 1,)),
            dma((2, halves, 2, 2)),
            dma((2,)),
            dma((5, 2)),
            dma((ships, 2)),
            dma((ships, bricks + 4)),
        ],
        compiler_params=pltpu.CompilerParams(
            vmem_limit_bytes=60 * 2**20, collective_id=0, has_side_effects=True
        ),
        name="elementals",
    )(momenta.T, v, g)
    return out.reshape((rows, count, 2, rows))


def choose(vectors, gauge_links, momenta):
    plane = LY * LZ
    bricks, vecs, subs = (lax.axis_size(a) for a in ("brick", "vec", "sub"))
    rows, local_sites = vectors.shape[0], vectors.shape[3]
    fits = local_sites % plane == 0 and 3 <= local_sites // plane <= 4 and rows == 32
    if fits and vecs == 2 and subs == 2 and bricks == 4 and 24 <= momenta.shape[0] < 32:
        return shards_fused(vectors, gauge_links, momenta)
    return shards(vectors, gauge_links, momenta)


def solution(mesh):
    in_specs = (
        P(("vec", "sub"), None, None, ("grp", "brick")),
        P(None, None, None, None, ("grp", "brick")),
        P(),
    )
    out_specs = P(("vec", "sub"), "grp", None, "brick")
    return jax.shard_map(choose, mesh=mesh, in_specs=in_specs, out_specs=out_specs, check_vma=False)
```

```python
import functools
import math

import jax
import jax.numpy as jnp
from jax import lax
from jax.experimental import pallas as pl
from jax.experimental.pallas import tpu as pltpu
from jax.sharding import PartitionSpec as P

LY = 64
LZ = 8
ITERS = 2


KAPPA = 0.125


def from_behind(array, axis, by):
    peers = lax.axis_size(axis)
    return lax.ppermute(array, axis, [(i, (i + by) % peers) for i in range(peers)])


def padded_2(array, sides, width):
    for axis, dim in sides:
        peers, length = (lax.axis_size(axis), array.shape[dim])
        up = [(i, (i + 1) % peers) for i in range(peers)]
        down = [(j, i) for i, j in up]
        last = lax.slice_in_dim(array, length - width, length, axis=dim)
        initial = lax.slice_in_dim(array, 0, width, axis=dim)
        before = lax.ppermute(last, axis, up)
        after = lax.ppermute(initial, axis, down)
        array = jnp.concatenate([before, array, after], axis=dim)
    return array


def matrix_apply(matrix, source):
    matrix_real = matrix[:, :, 0][None]
    matrix_imag = matrix[:, :, 1][None]
    source_real = source[:, None, :, 0]
    source_imag = source[:, None, :, 1]
    real_part = jnp.sum(matrix_real * source_real - matrix_imag * source_imag, axis=2)
    imag_part = jnp.sum(matrix_real * source_imag + matrix_imag * source_real, axis=2)
    return jnp.stack([real_part, imag_part], axis=2)


def adjoint(matrix):
    return jnp.stack(
        [jnp.swapaxes(matrix[:, :, 0], 0, 1), -jnp.swapaxes(matrix[:, :, 1], 0, 1)], axis=2
    )


def step_depth(values, offset):
    depth_index = lax.iota(jnp.int32, values.shape[-1]) % LZ
    if offset > 0:
        return jnp.where(
            depth_index == LZ - 1, jnp.roll(values, LZ - 1, -1), jnp.roll(values, -1, -1)
        )
    return jnp.where(depth_index == 0, jnp.roll(values, 1 - LZ, -1), jnp.roll(values, 1, -1))


def step_column(values, offset):
    plane = LY * LZ
    column_index = lax.iota(jnp.int32, values.shape[-1]) // LZ % LY
    if offset > 0:
        return jnp.where(
            column_index == LY - 1, jnp.roll(values, plane - LZ, -1), jnp.roll(values, -LZ, -1)
        )
    return jnp.where(column_index == 0, jnp.roll(values, LZ - plane, -1), jnp.roll(values, LZ, -1))


def laplace_step(center, ahead, behind, here_links, back_links):
    forward = matrix_apply(here_links[0], ahead)
    backward = matrix_apply(adjoint(back_links), behind)
    total = forward + backward
    for direction, stepper in ((1, step_column), (2, step_depth)):
        forward = matrix_apply(here_links[direction], stepper(center, 1))
        backward = matrix_apply(adjoint(stepper(here_links[direction], -1)), stepper(center, -1))
        total = total + (forward + backward)
    return center + KAPPA * (total - 6.0 * center)


def shards(vectors, gauge_links, momenta):
    plane = LY * LZ
    local_sites = vectors.shape[3]
    raw_low = vectors.astype(jnp.bfloat16)
    field = vectors
    x_links = gauge_links[0]
    rim = from_behind(x_links[..., local_sites - plane :], "brick", 1)
    back_links = jnp.concatenate([rim, x_links[..., : local_sites - plane]], axis=3)
    for step in range(ITERS):
        padded = padded_2(field, (("brick", 3),), plane)
        field = laplace_step(
            padded[..., plane : plane + local_sites],
            padded[..., 2 * plane :],
            padded[..., :local_sites],
            gauge_links,
            back_links,
        )
    smeared_low = field.astype(jnp.bfloat16)
    raw_sites, smeared_sites = (
        lax.all_to_all(raw_low, ("vec", "sub"), split_axis=3, concat_axis=0, tiled=True),
        lax.all_to_all(smeared_low, ("vec", "sub"), split_axis=3, concat_axis=0, tiled=True),
    )
    groups = lax.axis_size(("vec", "sub"))
    total_vec = raw_sites.shape[0]
    width = raw_sites.shape[3]
    total_x = lax.axis_size("brick") * (local_sites // plane)
    first_site = lax.axis_index("brick") * local_sites + lax.axis_index(("vec", "sub")) * width
    site = first_site + lax.iota(jnp.int32, width)
    layer_index = (site // plane)[None]
    column_index = (site // LZ % LY)[None]
    depth_index = (site % LZ)[None]
    fraction = (
        jnp.mod(momenta[:, 0:1] * layer_index, total_x).astype(jnp.float32) / total_x
        + jnp.mod(momenta[:, 1:2] * column_index, LY).astype(jnp.float32) / LY
        + jnp.mod(momenta[:, 2:3] * depth_index, LZ).astype(jnp.float32) / LZ
    )
    angle = 2.0 * math.pi * fraction
    cosines = jnp.cos(angle)
    sines = jnp.sin(angle)
    right = smeared_sites.reshape((total_vec, 6 * width))
    scale = (3.0 * total_x * plane) ** (-0.5)

    def one_momentum(angles):
        cosine, sine = angles
        real_part = raw_sites[:, :, 0] * cosine - raw_sites[:, :, 1] * sine
        imag_part = raw_sites[:, :, 0] * sine + raw_sites[:, :, 1] * cosine
        phased = jnp.stack([real_part, imag_part], axis=2).astype(jnp.bfloat16)
        turned = jnp.stack([-phased[:, :, 1], phased[:, :, 0]], axis=2)
        left = jnp.concatenate(
            [
                phased.reshape((lax.axis_size(("vec", "sub")) * (total_vec // groups), 6 * width)),
                turned.reshape((lax.axis_size(("vec", "sub")) * (total_vec // groups), 6 * width)),
            ],
            axis=0,
        )
        product = lax.dot_general(
            left, right, (((1,), (1,)), ((), ())), preferred_element_type=jnp.float32
        )
        return product.reshape(
            (2, lax.axis_size(("vec", "sub")) * (total_vec // groups), total_vec)
        )

    blocks = lax.map(one_momentum, (cosines, sines))
    shares = lax.psum_scatter(
        jnp.transpose(blocks, (2, 0, 1, 3)) * scale, ("vec", "sub"), scatter_dimension=0, tiled=True
    )
    return lax.psum_scatter(shares, "brick", scatter_dimension=3, tiled=True)


def fused_kernel(plan, mom_ref, v_ref, g_ref, out_ref, *scratch):
    (vst, gst, field0, field1, table, moved0, moved1, right, smeared, left0, left1, cosb, sinb, total, parted,
     crossing, rx, halo, hsend, lsend, lrecv, load_sem, halo_sem, link_sem, raw_sem, cross_sem, last_sem) = scratch
    planes, rows, count, bricks, ships, width, scale = plan
    fields, moved = (field0, field1), (moved0, moved1)
    halves = rows // 16
    plane = LY * LZ
    tiles = plane // 128
    all_tiles = planes * tiles
    f32, low = jnp.float32, jnp.bfloat16
    wide = 2 * plane
    last = planes - 1
    inner = list(range(1, last))
    outer = [0, last]
    position = {t: i for i, t in enumerate(inner + outer)}
    cut = len(inner) * 3 * wide
    span = planes * 3 * wide
    b, v, s = (lax.axis_index(a) for a in ("brick", "vec", "sub"))
    left = (left0, left1)

    def remote(src, dst, sems, **ids):
        return pltpu.make_async_remote_copy(
            src_ref=src, dst_ref=dst, send_sem=sems.at[0], recv_sem=sems.at[1],
            device_id=ids, device_id_type=pl.DeviceIdType.MESH,
        )

    loads = {}
    for t in outer + inner:
        loads[t] = pltpu.make_async_copy(v_ref.at[:, t], vst.at[t], load_sem.at[t])
        loads[t].start()
    load_links = pltpu.make_async_copy(g_ref, gst.at[pl.ds(0, 54 * all_tiles)], load_sem.at[planes])
    load_links.start()
    barrier = pltpu.get_barrier_semaphore()
    for db in range(bricks):
        for ds in range(2):
            if db or ds:
                pl.semaphore_signal(
                    barrier, inc=1, device_id={"brick": (b + db) % bricks, "sub": (s + ds) % 2},
                    device_id_type=pl.DeviceIdType.MESH,
                )
    pl.semaphore_signal(
        barrier, inc=1, device_id={"vec": 1 - v}, device_id_type=pl.DeviceIdType.MESH
    )

    def unpack(t):
        flat = vst.at[t].reshape(rows * 3 * tiles * 2, 128)
        step = 3 * tiles * 2
        for c in range(3):
            for first in range(0, rows, 16):
                for part in range(2):
                    for lane in range(0, tiles, 2):
                        at = part * plane + lane * 128
                        quad = []
                        for h in range(2):
                            start = (first + 8 * h) * step + c * tiles * 2 + lane * 2 + part
                            quad.append(
                                jnp.concatenate(
                                    [flat[pl.ds(start + 2 * i, 8, stride=step), :] for i in range(2)], axis=1
                                )
                            )
                            field0[t + 1, c, first + 8 * h : first + 8 * h + 8, at : at + 256] = quad[h]
                        k = (position[t] * 3 + c) * wide + at
                        right[first : first + 16, k : k + 256] = jnp.concatenate(quad, axis=0).astype(low)

    def link_rows(t, part, group):
        return jnp.concatenate(
            [
                gst[pl.ds(group * 16 * all_tiles + (t * tiles + lane) * 2 + part, 8, stride=2 * all_tiles), :]
                for lane in range(tiles)
            ],
            axis=1,
        ) * KAPPA

    for t in outer:
        loads[t].wait()
        unpack(t)
    load_links.wait()
    for part in range(2):
        both = jnp.concatenate([link_rows(last, part, 0), link_rows(last, part, 1)], axis=0)
        lsend[16 * part : 16 * part + 16, :] = both.astype(low)
    pl.semaphore_wait(barrier, 2 * bricks)
    up, down = (b + 1) % bricks, (b + bricks - 1) % bricks

    def halos(step, h, low_src, high_src):
        sems = halo_sem.at[step, h]
        return (
            remote(high_src, halo.at[step, h, 0], sems.at[0], brick=up),
            remote(low_src, halo.at[step, h, 1], sems.at[1], brick=down),
        )

    def own(t, h):
        at = position[t] * 3 * wide
        return right.at[16 * h : 16 * h + 16, at : at + 3 * wide]

    copies = {}
    links_up = remote(lsend, lrecv, link_sem, brick=up)
    for h in range(halves):
        copies[0, h] = halos(0, h, own(0, h), own(last, h))
        copies[1, h] = halos(1, h, hsend.at[h, 0], hsend.at[h, 1])
        for copy in copies[0, h]:
            copy.start()
        if h == 0:
            links_up.start()
    for t in inner:
        loads[t].wait()
        unpack(t)
    parts = (slice(0, cut), slice(cut, span))
    unit = 2 * rows

    def raw_copy(index, from_slot, to_slot, ks, **ids):
        return remote(
            right.at[from_slot * unit : from_slot * unit + rows, ks],
            right.at[to_slot * unit : to_slot * unit + rows, ks],
            raw_sem.at[index], **ids,
        )

    across = [raw_copy(i, 0, 2, parts[i], vec=1 - v) for i in range(2)]
    beside = raw_copy(2, 0, 1, slice(0, span), sub=1 - s)
    onward = [raw_copy(3 + i, 2, 3, parts[i], sub=1 - s) for i in range(2)]
    for copy in across + [beside]:
        copy.start()

    depth_wide = lax.broadcasted_iota(jnp.int32, (8, plane), 1) % LZ
    depth = lax.broadcasted_iota(jnp.int32, (8, 128), 1) % LZ

    def spread(t, carry):
        for part in range(2):
            for group in range(4):
                here = link_rows(t, part, group)
                if group > 0:
                    by = pltpu.roll(here, LZ, 1)
                    bz = jnp.where(
                        depth_wide == 0, pltpu.roll(here, plane - (LZ - 1), 1), pltpu.roll(here, 1, 1)
                    )
                for j in range(min(8, 27 - 8 * group)):
                    index = group * 8 + j
                    row = jnp.broadcast_to(here[j : j + 1], (8, plane))
                    table[t, index * 2 + part] = row
                    if index < 9:
                        table[t + 1, 54 + index * 2 + part] = row
                    else:
                        back = by if index < 18 else bz
                        table[t, 54 + index * 2 + part] = jnp.broadcast_to(back[j : j + 1], (8, plane))
        return carry

    lax.fori_loop(0, planes, spread, 0)

    places = []
    for group in range(0, all_tiles, 8):
        height = min(8, all_tiles - group)
        site = (
            lax.broadcasted_iota(jnp.int32, (height, 128), 0) * 128
            + lax.broadcasted_iota(jnp.int32, (height, 128), 1)
            + group * 128
        )
        places.append(
            (
                (site // plane + b * planes).astype(f32) * (1.0 / (bricks * planes)),
                (site // LZ % LY).astype(f32) * (1.0 / LY),
                (site % LZ).astype(f32) * (1.0 / LZ),
            )
        )

    def phases(q, carry):
        n = [mom_ref[d, jnp.minimum(q, count - 1)].astype(f32) for d in range(3)]
        for group, (x, y, z) in enumerate(places):
            turns = n[0] * x + n[1] * y + n[2] * z
            half = jnp.round(2.0 * turns)
            sign = 1.0 - 2.0 * jnp.abs(half - 2.0 * jnp.round(0.5 * half))
            angle = (2.0 * math.pi) * (turns - 0.5 * half)
            square = angle * angle
            cosine, sine = 0.0, 0.0
            for i in range(7, 0, -1):
                cosine = (cosine * square) + (-1.0) ** i / math.factorial(2 * i)
            cosine = sign * (1.0 + cosine * square)
            for i in range(6, 0, -1):
                sine = (sine * square) + (-1.0) ** i / math.factorial(2 * i + 1)
            sine = sign * (angle + angle * (sine * square))
            for j in range(x.shape[0]):
                at = (group * 8 + j) * 128
                cosb[q, :, at : at + 128] = jnp.broadcast_to(cosine[j : j + 1], (16, 128)).astype(low)
                sinb[q, :, at : at + 128] = jnp.broadcast_to(sine[j : j + 1], (16, 128)).astype(low)
        return carry

    lax.fori_loop(0, count, phases, 0)

    def shift(stage, k, to):
        step, t, h = stage
        rows_to = pl.ds(pl.multiple_of(k % 2 * 8, 8), 8)
        rows_at = pl.ds(pl.multiple_of(h * 16 + k % 2 * 8, 8), 8)
        first_lane = k // 2 * plane
        lanes = pl.ds(pl.multiple_of(first_lane, plane), plane)
        for c in range(3):
            w = fields[step][t + 1, c, rows_at, lanes]
            to[0, c, rows_to, lanes] = pltpu.roll(w, plane - LZ, 1)
            to[1, c, rows_to, lanes] = pltpu.roll(w, LZ, 1)
            for part in range(tiles):
                u = w[:, part * 128 : part * 128 + 128]
                here = pl.ds(pl.multiple_of(first_lane + part * 128, 128), 128)
                to[2, c, rows_to, here] = jnp.where(
                    depth == LZ - 1, pltpu.roll(u, LZ - 1, 1), pltpu.roll(u, 127, 1)
                )
                to[3, c, rows_to, here] = jnp.where(
                    depth == 0, pltpu.roll(u, 128 - (LZ - 1), 1), pltpu.roll(u, 1, 1)
                )

    def block(stage, lane, now):
        step, t, half = stage
        field = fields[step]
        lanes = (
            pl.ds(pl.multiple_of(lane * 128, 128), 128),
            pl.ds(pl.multiple_of(plane + lane * 128, 128), 128),
        )
        at_rows = [slice(half * 16 + 8 * h, half * 16 + 8 * h + 8) for h in range(2)]
        acc = {}
        for h in range(2):
            for r in range(3):
                for part in range(2):
                    mid = field[t + 1, r, at_rows[h], lanes[part]]
                    acc[h, r, part] = (1.0 - 6.0 * KAPPA) * mid
        for way in range(6):
            direction, back = way // 2, way % 2
            for c in range(3):
                sources = []
                for h in range(2):
                    if direction == 0:
                        p = t + 2 - 2 * back
                        sources.append([field[p, c, at_rows[h], lanes[i]] for i in range(2)])
                    else:
                        sources.append([now[way - 2, c, 8 * h : 8 * h + 8, lanes[i]] for i in range(2)])
                for r in range(3):
                    row = direction * 18 + (54 + c * 6 + r * 2 if back else r * 6 + c * 2)
                    ur = table[t, row, :, lanes[0]]
                    ui = table[t, row + 1, :, lanes[0]]
                    for h, (sr, si) in enumerate(sources):
                        if back:
                            acc[h, r, 0] = acc[h, r, 0] + (ur * sr + ui * si)
                            acc[h, r, 1] = acc[h, r, 1] + (ur * si - ui * sr)
                        else:
                            acc[h, r, 0] = acc[h, r, 0] + (ur * sr - ui * si)
                            acc[h, r, 1] = acc[h, r, 1] + (ur * si + ui * sr)
        both = slice(half * 16, half * 16 + 16)
        for r in range(3):
            for part in range(2):
                if step == 0:
                    for h in range(2):
                        field1[t + 1, r, at_rows[h], lanes[part]] = acc[h, r, part]
                if step == 1 or t in outer:
                    pair = jnp.concatenate([acc[0, r, part], acc[1, r, part]], axis=0).astype(low)
                    if step == 1:
                        smeared[position[t] * 3 + r, both, lanes[part]] = pair
                    else:
                        k_at = pl.ds(pl.multiple_of((2 * r + part) * plane + lane * 128, 128), 128)
                        hsend[half, outer.index(t), :, k_at] = pair

    stages = [(0, t, h) for h in range(halves) for t in inner]
    for h in range(halves):
        stages += [(0, t, h) for t in outer] + [(1, t, h) for t in inner]
    stages += [(1, t, h) for h in range(halves) for t in outer]

    def run(step, ts, h):
        for t in ts:
            i = stages.index((step, t, h))

            def trip(k, carry):
                shift(stages[(i + 1) % len(stages)], k, moved[(i + 1) % 2])
                block(stages[i], k, moved[i % 2])
                return carry

            lax.fori_loop(0, tiles, trip, 0)

    def begin(k, carry):
        shift(stages[0], k, moved[0])
        return carry

    lax.fori_loop(0, tiles, begin, 0)
    for h in range(halves):
        run(0, inner, h)

    def take(step, h, side):
        copies[step, h][side].wait_recv()
        for c in range(3):
            fields[step][planes + 1 if side else 0, c, 16 * h : 16 * h + 16] = (
                halo[step, h, side, :, c * wide : (c + 1) * wide].astype(f32)
            )

    links_up.wait_recv()
    for part in range(2):
        got = lrecv[16 * part : 16 * part + 16, :].astype(f32)
        for index in range(9):
            table[0, 54 + index * 2 + part] = jnp.broadcast_to(got[index : index + 1], (8, plane))
    for h in range(halves):
        for side in range(2):
            take(0, h, side)
            run(0, [outer[side]], h)
            copies[1, h][1 - side].start()
        if h == halves - 1:
            across[0].wait_recv()
            onward[0].start()
        run(1, inner, h)
    beside.wait_recv()
    onward[0].wait_recv()

    def fill(k, carry):
        re = pl.ds(pl.multiple_of(k * wide, wide), plane)
        im = pl.ds(pl.multiple_of(k * wide + plane, plane), plane)
        for slot in range(4):
            at_raw = slice(slot * unit, slot * unit + rows)
            at_turned = slice(slot * unit + rows, (slot + 1) * unit)
            right[at_turned, re] = -right[at_raw, im]
            right[at_turned, im] = right[at_raw, re]
        return carry

    members = (inner, outer)
    order = [(h, half, t) for h in range(halves) for half in range(2) for t in members[half]]
    per = width // 16
    streamed = 16 * count

    def ready(i):
        return order[i][1] == 0 or order[i - 1][1] == 1

    def turn(i):
        h, half, t = order[i]
        to = left[i % 2]
        for q in range(count):
            for lane in range(0, plane, 256):
                cosine = cosb[q, :, t * plane + lane : t * plane + lane + 256]
                sine = sinb[q, :, t * plane + lane : t * plane + lane + 256]
                for c in range(3):
                    k = position[t] * 3 + c
                    sr = smeared[k, 16 * h : 16 * h + 16, lane : lane + 256]
                    si = smeared[k, 16 * h : 16 * h + 16, plane + lane : plane + lane + 256]
                    col = c * wide + lane
                    to[16 * q : 16 * q + 16, col : col + 256] = cosine * sr + sine * si
                    to[16 * q : 16 * q + 16, col + plane : col + plane + 256] = cosine * si - sine * sr

    def product(i):
        h, half, t = order[i]
        first = position[t] * 3 * wide
        length = 3 * wide
        pieces = []
        for k in range(0, length, length // 2):
            pieces.append(
                lax.dot_general(
                    left[i % 2][:, k : k + length // 2],
                    right[:, first + k : first + k + length // 2],
                    (((1,), (1,)), ((), ())), preferred_element_type=f32,
                )
            )
        if i + 1 < len(order) and ready(i + 1):
            turn(i + 1)
        part = pieces[0] * scale + pieces[1] * scale
        if t == inner[0]:
            total[h, 0:streamed] = part
        else:
            total[h, 0:streamed] += part

    def finish(e):
        per_half = ships // halves
        at = e % per_half * width
        part = total[e // per_half, at : at + width, :].T.astype(low)
        parted[e, 0] = part[0 : 2 * unit]
        crossing[e] = part[2 * unit :]

    roots = (v * 2 + s, (1 - v) * 2 + s)

    def cross(e):
        return remote(
            crossing.at[e], parted.at[e, 1], cross_sem.at[e], vec=1 - v
        )

    def ends(e, hop, ds):
        src = parted.at[e, hop, ds * unit : (ds + 1) * unit]
        return src, rx.at[e, b]

    def far(e, hop, ds):
        src, dst = ends(e, hop, ds)
        return pltpu.make_async_remote_copy(
            src_ref=src, dst_ref=dst,
            send_sem=last_sem.at[e, bricks + hop * 2 + ds], recv_sem=last_sem.at[e, b],
            device_id={"brick": roots[hop], "sub": (s + ds) % 2}, device_id_type=pl.DeviceIdType.MESH,
        )

    def depart(e, hop):
        far(e, hop, 1).start()

        @pl.when(roots[hop] != b)
        def _():
            far(e, hop, 0).start()

        @pl.when(roots[hop] == b)
        def _():
            src, dst = ends(e, hop, 0)
            pltpu.make_async_copy(src, dst, last_sem.at[e, b]).start()

    def ship(e):
        finish(e)
        cross(e).start()
        depart(e, 0)

    def hand_on(e):
        cross(e).wait_recv()
        depart(e, 1)

    def arrive(e):
        for i in range(bricks):
            dst = rx.at[e, i]
            pltpu.make_async_copy(dst, dst, last_sem.at[e, i]).wait()

    def fill_half(half):
        first = len(inner) * 3 if half else 0
        count_k = len(members[half]) * 3
        lax.fori_loop(first, first + count_k, fill, 0)

    per_half = ships // halves
    for i, (h, half, t) in enumerate(order):
        opens = t == members[half][0]
        if i == 0:
            fill_half(0)
        if half and opens:
            if h == 0:
                across[1].wait_recv()
                onward[1].start()
            for side in range(2):
                take(1, h, side)
                run(1, [outer[side]], h)
            if h == 0:
                onward[1].wait_recv()
                fill_half(1)
        if i == 0 or not ready(i):
            turn(i)
        product(i)
        if h and not half and opens:
            for e in range(per_half * (h - 1), per_half * h):
                hand_on(e)
        if half and not opens:
            for e in range(per_half * h, per_half * (h + 1)):
                ship(e)
    for e in range(per_half * (halves - 1), ships):
        hand_on(e)
    lane_at = lax.broadcasted_iota(jnp.int32, (8, 128), 1)
    for e in range(ships):
        arrive(e)
    for q in range(count):
        for first in range(0, unit, 8):
            pieces = []
            for h in range(halves):
                e, at = h * per_half + q // per, q % per * 16
                tile = slice(at // 128 * 128, at // 128 * 128 + 128)
                rows_at = slice(first // 16 * 16, first // 16 * 16 + 16)
                got = [rx[e, i, rows_at, tile].astype(f32) for i in range(bricks)]
                got = (got[0] + got[1]) + (got[2] + got[3])
                got = got[first % 16 : first % 16 + 8]
                turned = (16 * h - at) % 128
                pieces.append(pltpu.roll(got, turned, 1) if turned else got)
            value = jnp.where(lane_at < 16, pieces[0], pieces[1])
            start = (first % rows) * 2 * count + 2 * q + first // rows
            out_ref[pl.ds(start, 8, stride=2 * count), :] = value[:, 0:rows]
    sent = [links_up, *across, beside, *onward]
    for copy in copies.values():
        sent += copy
    sent += [cross(e) for e in range(ships)]
    for copy in sent:
        copy.wait_send()
    for e in range(ships):
        for hop in range(2):
            far(e, hop, 1).wait_send()

            @pl.when(roots[hop] != b)
            def _():
                far(e, hop, 0).wait_send()


def shards_fused(vectors, gauge_links, momenta):
    plane = LY * LZ
    rows, local_sites = vectors.shape[0], vectors.shape[3]
    planes = local_sites // plane
    tiles = plane // 128
    bricks = lax.axis_size("brick")
    count = momenta.shape[0]
    halves = rows // 16
    width = 256
    per_half = -(-count * 16 // width)
    ships = halves * per_half
    low, f32 = jnp.bfloat16, jnp.float32
    v = vectors.reshape((rows, 3, 2, planes * tiles, 128)).transpose((0, 1, 3, 2, 4))
    v = v.reshape((rows * 3, planes, tiles * 2, 128))
    g = gauge_links.reshape((27, 2, planes * tiles, 128)).transpose((0, 2, 1, 3))
    g = g.reshape((54 * planes * tiles, 128))
    wide = 2 * plane
    scale = (3.0 * bricks * local_sites) ** (-0.5)
    vmem, dma = pltpu.VMEM, pltpu.SemaphoreType.DMA
    plan = (planes, rows, count, bricks, ships, width, scale)
    out = pl.pallas_call(
        functools.partial(fused_kernel, plan),
        out_shape=jax.ShapeDtypeStruct((rows * count * 2, rows), f32),
        in_specs=[
            pl.BlockSpec(memory_space=pltpu.SMEM),
            pl.BlockSpec(memory_space=pl.ANY),
            pl.BlockSpec(memory_space=pl.ANY),
        ],
        out_specs=pl.BlockSpec(memory_space=pltpu.VMEM),
        scratch_shapes=[
            vmem((planes, rows * 3, tiles * 2, 128), f32),
            vmem((64 * planes * tiles, 128), f32),
            vmem((planes + 2, 3, rows, wide), f32),
            vmem((planes + 2, 3, rows, wide), f32),
            vmem((planes + 1, 108, 8, plane), f32),
            vmem((4, 3, 16, wide), f32),
            vmem((4, 3, 16, wide), f32),
            vmem((8 * rows, planes * 3 * wide), low),
            vmem((planes * 3, rows, wide), low),
            vmem((16 * count, 3 * wide), low),
            vmem((16 * count, 3 * wide), low),
            vmem((count, 16, local_sites), low),
            vmem((count, 16, local_sites), low),
            vmem((halves, per_half * width, 8 * rows), f32),
            vmem((ships, 2, 4 * rows, width), low),
            vmem((ships, 4 * rows, width), low),
            vmem((ships, bricks, 2 * rows, width), low),
            vmem((2, halves, 2, 16, 3 * wide), low),
            vmem((halves, 2, 16, 3 * wide), low),
            vmem((32, plane), low),
            vmem((32, plane), low),
            dma((planes + 1,)),
            dma((2, halves, 2, 2)),
            dma((2,)),
            dma((5, 2)),
            dma((ships, 2)),
            dma((ships, bricks + 4)),
        ],
        compiler_params=pltpu.CompilerParams(
            vmem_limit_bytes=60 * 2**20, collective_id=0, has_side_effects=True
        ),
        name="elementals",
    )(momenta.T, v, g)
    return out.reshape((rows, count, 2, rows))


def choose(vectors, gauge_links, momenta):
    plane = LY * LZ
    bricks, vecs, subs = (lax.axis_size(a) for a in ("brick", "vec", "sub"))
    rows, local_sites = vectors.shape[0], vectors.shape[3]
    fits = local_sites % plane == 0 and local_sites // plane == 4 and rows == 32
    if fits and vecs == 2 and subs == 2 and bricks == 4 and momenta.shape[0] <= 32:
        return shards_fused(vectors, gauge_links, momenta)
    return shards(vectors, gauge_links, momenta)


def solution(mesh):
    in_specs = (
        P(("vec", "sub"), None, None, ("grp", "brick")),
        P(None, None, None, None, ("grp", "brick")),
        P(),
    )
    out_specs = P(("vec", "sub"), "grp", None, "brick")
    return jax.shard_map(choose, mesh=mesh, in_specs=in_specs, out_specs=out_specs, check_vma=False)
```

```python
import functools
import math

import jax
import jax.numpy as jnp
from jax import lax
from jax.experimental import pallas as pl
from jax.experimental.pallas import tpu as pltpu
from jax.sharding import PartitionSpec as P

LY = 64
LZ = 8
ITERS = 2


KAPPA = 0.125


def from_behind(array, axis, by):
    peers = lax.axis_size(axis)
    return lax.ppermute(array, axis, [(i, (i + by) % peers) for i in range(peers)])


def padded_2(array, sides, width):
    for axis, dim in sides:
        peers, length = (lax.axis_size(axis), array.shape[dim])
        up = [(i, (i + 1) % peers) for i in range(peers)]
        down = [(j, i) for i, j in up]
        last = lax.slice_in_dim(array, length - width, length, axis=dim)
        initial = lax.slice_in_dim(array, 0, width, axis=dim)
        before = lax.ppermute(last, axis, up)
        after = lax.ppermute(initial, axis, down)
        array = jnp.concatenate([before, array, after], axis=dim)
    return array


def matrix_apply(matrix, source):
    matrix_real = matrix[:, :, 0][None]
    matrix_imag = matrix[:, :, 1][None]
    source_real = source[:, None, :, 0]
    source_imag = source[:, None, :, 1]
    real_part = jnp.sum(matrix_real * source_real - matrix_imag * source_imag, axis=2)
    imag_part = jnp.sum(matrix_real * source_imag + matrix_imag * source_real, axis=2)
    return jnp.stack([real_part, imag_part], axis=2)


def adjoint(matrix):
    return jnp.stack(
        [jnp.swapaxes(matrix[:, :, 0], 0, 1), -jnp.swapaxes(matrix[:, :, 1], 0, 1)], axis=2
    )


def step_depth(values, offset):
    depth_index = lax.iota(jnp.int32, values.shape[-1]) % LZ
    if offset > 0:
        return jnp.where(
            depth_index == LZ - 1, jnp.roll(values, LZ - 1, -1), jnp.roll(values, -1, -1)
        )
    return jnp.where(depth_index == 0, jnp.roll(values, 1 - LZ, -1), jnp.roll(values, 1, -1))


def step_column(values, offset):
    plane = LY * LZ
    column_index = lax.iota(jnp.int32, values.shape[-1]) // LZ % LY
    if offset > 0:
        return jnp.where(
            column_index == LY - 1, jnp.roll(values, plane - LZ, -1), jnp.roll(values, -LZ, -1)
        )
    return jnp.where(column_index == 0, jnp.roll(values, LZ - plane, -1), jnp.roll(values, LZ, -1))


def laplace_step(center, ahead, behind, here_links, back_links):
    forward = matrix_apply(here_links[0], ahead)
    backward = matrix_apply(adjoint(back_links), behind)
    total = forward + backward
    for direction, stepper in ((1, step_column), (2, step_depth)):
        forward = matrix_apply(here_links[direction], stepper(center, 1))
        backward = matrix_apply(adjoint(stepper(here_links[direction], -1)), stepper(center, -1))
        total = total + (forward + backward)
    return center + KAPPA * (total - 6.0 * center)


def shards(vectors, gauge_links, momenta):
    plane = LY * LZ
    local_sites = vectors.shape[3]
    raw_low = vectors.astype(jnp.bfloat16)
    field = vectors
    x_links = gauge_links[0]
    rim = from_behind(x_links[..., local_sites - plane :], "brick", 1)
    back_links = jnp.concatenate([rim, x_links[..., : local_sites - plane]], axis=3)
    for step in range(ITERS):
        padded = padded_2(field, (("brick", 3),), plane)
        field = laplace_step(
            padded[..., plane : plane + local_sites],
            padded[..., 2 * plane :],
            padded[..., :local_sites],
            gauge_links,
            back_links,
        )
    smeared_low = field.astype(jnp.bfloat16)
    raw_sites, smeared_sites = (
        lax.all_to_all(raw_low, ("vec", "sub"), split_axis=3, concat_axis=0, tiled=True),
        lax.all_to_all(smeared_low, ("vec", "sub"), split_axis=3, concat_axis=0, tiled=True),
    )
    groups = lax.axis_size(("vec", "sub"))
    total_vec = raw_sites.shape[0]
    width = raw_sites.shape[3]
    total_x = lax.axis_size("brick") * (local_sites // plane)
    first_site = lax.axis_index("brick") * local_sites + lax.axis_index(("vec", "sub")) * width
    site = first_site + lax.iota(jnp.int32, width)
    layer_index = (site // plane)[None]
    column_index = (site // LZ % LY)[None]
    depth_index = (site % LZ)[None]
    fraction = (
        jnp.mod(momenta[:, 0:1] * layer_index, total_x).astype(jnp.float32) / total_x
        + jnp.mod(momenta[:, 1:2] * column_index, LY).astype(jnp.float32) / LY
        + jnp.mod(momenta[:, 2:3] * depth_index, LZ).astype(jnp.float32) / LZ
    )
    angle = 2.0 * math.pi * fraction
    cosines = jnp.cos(angle)
    sines = jnp.sin(angle)
    right = smeared_sites.reshape((total_vec, 6 * width))
    scale = (3.0 * total_x * plane) ** (-0.5)

    def one_momentum(angles):
        cosine, sine = angles
        real_part = raw_sites[:, :, 0] * cosine - raw_sites[:, :, 1] * sine
        imag_part = raw_sites[:, :, 0] * sine + raw_sites[:, :, 1] * cosine
        phased = jnp.stack([real_part, imag_part], axis=2).astype(jnp.bfloat16)
        turned = jnp.stack([-phased[:, :, 1], phased[:, :, 0]], axis=2)
        left = jnp.concatenate(
            [
                phased.reshape((lax.axis_size(("vec", "sub")) * (total_vec // groups), 6 * width)),
                turned.reshape((lax.axis_size(("vec", "sub")) * (total_vec // groups), 6 * width)),
            ],
            axis=0,
        )
        product = lax.dot_general(
            left, right, (((1,), (1,)), ((), ())), preferred_element_type=jnp.float32
        )
        return product.reshape(
            (2, lax.axis_size(("vec", "sub")) * (total_vec // groups), total_vec)
        )

    blocks = lax.map(one_momentum, (cosines, sines))
    shares = lax.psum_scatter(
        jnp.transpose(blocks, (2, 0, 1, 3)) * scale, ("vec", "sub"), scatter_dimension=0, tiled=True
    )
    return lax.psum_scatter(shares, "brick", scatter_dimension=3, tiled=True)


def fused_kernel(plan, mom_ref, v_ref, g_ref, out_ref, *scratch):
    (vst, gst, field0, field1, table, moved0, moved1, right, smeared, left0, left1, cosb, sinb, total, parted,
     crossing, rx, halo, hsend, lsend, lrecv, load_sem, halo_sem, link_sem, raw_sem, cross_sem, last_sem) = scratch
    planes, rows, count, bricks, ships, width, scale = plan
    fields, moved = (field0, field1), (moved0, moved1)
    halves = rows // 16
    plane = LY * LZ
    tiles = plane // 128
    all_tiles = planes * tiles
    f32, low = jnp.float32, jnp.bfloat16
    wide = 2 * plane
    last = planes - 1
    inner = list(range(1, last))
    outer = [0, last]
    position = {t: i for i, t in enumerate(inner + outer)}
    cut = len(inner) * 3 * wide
    span = planes * 3 * wide
    b, v, s = (lax.axis_index(a) for a in ("brick", "vec", "sub"))
    left = (left0, left1)

    def remote(src, dst, sems, **ids):
        return pltpu.make_async_remote_copy(
            src_ref=src, dst_ref=dst, send_sem=sems.at[0], recv_sem=sems.at[1],
            device_id=ids, device_id_type=pl.DeviceIdType.MESH,
        )

    loads = {}
    for t in outer + inner:
        loads[t] = pltpu.make_async_copy(v_ref.at[:, t], vst.at[t], load_sem.at[t])
        loads[t].start()
    load_links = pltpu.make_async_copy(g_ref, gst.at[pl.ds(0, 54 * all_tiles)], load_sem.at[planes])
    load_links.start()
    barrier = pltpu.get_barrier_semaphore()
    for db in range(bricks):
        for ds in range(2):
            if db or ds:
                pl.semaphore_signal(
                    barrier, inc=1, device_id={"brick": (b + db) % bricks, "sub": (s + ds) % 2},
                    device_id_type=pl.DeviceIdType.MESH,
                )
    pl.semaphore_signal(
        barrier, inc=1, device_id={"vec": 1 - v}, device_id_type=pl.DeviceIdType.MESH
    )

    def unpack(t):
        flat = vst.at[t].reshape(rows * 3 * tiles * 2, 128)
        step = 3 * tiles * 2
        for c in range(3):
            for first in range(0, rows, 16):
                for part in range(2):
                    for lane in range(0, tiles, 2):
                        at = part * plane + lane * 128
                        quad = []
                        for h in range(2):
                            start = (first + 8 * h) * step + c * tiles * 2 + lane * 2 + part
                            quad.append(
                                jnp.concatenate(
                                    [flat[pl.ds(start + 2 * i, 8, stride=step), :] for i in range(2)], axis=1
                                )
                            )
                            field0[t + 1, c, first + 8 * h : first + 8 * h + 8, at : at + 256] = quad[h]
                        k = (position[t] * 3 + c) * wide + at
                        right[first : first + 16, k : k + 256] = jnp.concatenate(quad, axis=0).astype(low)

    def link_rows(t, part, group):
        return jnp.concatenate(
            [
                gst[pl.ds(group * 16 * all_tiles + (t * tiles + lane) * 2 + part, 8, stride=2 * all_tiles), :]
                for lane in range(tiles)
            ],
            axis=1,
        ) * KAPPA

    for t in outer:
        loads[t].wait()
        unpack(t)
    load_links.wait()
    for part in range(2):
        both = jnp.concatenate([link_rows(last, part, 0), link_rows(last, part, 1)], axis=0)
        lsend[16 * part : 16 * part + 16, :] = both.astype(low)
    pl.semaphore_wait(barrier, 2 * bricks)
    up, down = (b + 1) % bricks, (b + bricks - 1) % bricks

    def halos(step, h, low_src, high_src):
        sems = halo_sem.at[step, h]
        return (
            remote(high_src, halo.at[step, h, 0], sems.at[0], brick=up),
            remote(low_src, halo.at[step, h, 1], sems.at[1], brick=down),
        )

    def own(t, h):
        at = position[t] * 3 * wide
        return right.at[16 * h : 16 * h + 16, at : at + 3 * wide]

    copies = {}
    links_up = remote(lsend, lrecv, link_sem, brick=up)
    for h in range(halves):
        copies[0, h] = halos(0, h, own(0, h), own(last, h))
        copies[1, h] = halos(1, h, hsend.at[h, 0], hsend.at[h, 1])
        for copy in copies[0, h]:
            copy.start()
        if h == 0:
            links_up.start()
    for t in inner:
        loads[t].wait()
        unpack(t)
    parts = [slice(0, cut)] + [
        slice(cut + i * 3 * wide, cut + (i + 1) * 3 * wide) for i in range(2)
    ]
    unit = 2 * rows

    def raw_copy(index, from_slot, to_slot, ks, **ids):
        return remote(
            right.at[from_slot * unit : from_slot * unit + rows, ks],
            right.at[to_slot * unit : to_slot * unit + rows, ks],
            raw_sem.at[index], **ids,
        )

    across = [raw_copy(i, 0, 2, parts[i], vec=1 - v) for i in range(3)]
    beside = raw_copy(6, 0, 1, slice(0, span), sub=1 - s)
    onward = [raw_copy(3 + i, 2, 3, parts[i], sub=1 - s) for i in range(3)]
    for copy in across + [beside]:
        copy.start()

    depth_wide = lax.broadcasted_iota(jnp.int32, (8, plane), 1) % LZ
    depth = lax.broadcasted_iota(jnp.int32, (8, 128), 1) % LZ

    def spread(t, carry):
        for part in range(2):
            for group in range(4):
                here = link_rows(t, part, group)
                if group > 0:
                    by = pltpu.roll(here, LZ, 1)
                    bz = jnp.where(
                        depth_wide == 0, pltpu.roll(here, plane - (LZ - 1), 1), pltpu.roll(here, 1, 1)
                    )
                for j in range(min(8, 27 - 8 * group)):
                    index = group * 8 + j
                    row = jnp.broadcast_to(here[j : j + 1], (8, plane))
                    table[t, index * 2 + part] = row
                    if index < 9:
                        table[t + 1, 54 + index * 2 + part] = row
                    else:
                        back = by if index < 18 else bz
                        table[t, 54 + index * 2 + part] = jnp.broadcast_to(back[j : j + 1], (8, plane))
        return carry

    lax.fori_loop(0, planes, spread, 0)

    places = []
    for group in range(0, all_tiles, 8):
        height = min(8, all_tiles - group)
        site = (
            lax.broadcasted_iota(jnp.int32, (height, 128), 0) * 128
            + lax.broadcasted_iota(jnp.int32, (height, 128), 1)
            + group * 128
        )
        places.append(
            (
                (site // plane + b * planes).astype(f32) * (1.0 / (bricks * planes)),
                (site // LZ % LY).astype(f32) * (1.0 / LY),
                (site % LZ).astype(f32) * (1.0 / LZ),
            )
        )

    def phases(q, carry):
        n = [mom_ref[d, jnp.minimum(q, count - 1)].astype(f32) for d in range(3)]
        for group, (x, y, z) in enumerate(places):
            turns = n[0] * x + n[1] * y + n[2] * z
            half = jnp.round(2.0 * turns)
            sign = 1.0 - 2.0 * jnp.abs(half - 2.0 * jnp.round(0.5 * half))
            angle = (2.0 * math.pi) * (turns - 0.5 * half)
            square = angle * angle
            cosine, sine = 0.0, 0.0
            for i in range(7, 0, -1):
                cosine = (cosine * square) + (-1.0) ** i / math.factorial(2 * i)
            cosine = sign * (1.0 + cosine * square)
            for i in range(6, 0, -1):
                sine = (sine * square) + (-1.0) ** i / math.factorial(2 * i + 1)
            sine = sign * (angle + angle * (sine * square))
            for j in range(x.shape[0]):
                at = (group * 8 + j) * 128
                cosb[q, :, at : at + 128] = jnp.broadcast_to(cosine[j : j + 1], (16, 128)).astype(low)
                sinb[q, :, at : at + 128] = jnp.broadcast_to(sine[j : j + 1], (16, 128)).astype(low)
        return carry

    lax.fori_loop(0, count, phases, 0)

    def shift(stage, k, to):
        step, t, h = stage
        rows_to = pl.ds(pl.multiple_of(k % 2 * 8, 8), 8)
        rows_at = pl.ds(pl.multiple_of(h * 16 + k % 2 * 8, 8), 8)
        first_lane = k // 2 * plane
        lanes = pl.ds(pl.multiple_of(first_lane, plane), plane)
        for c in range(3):
            w = fields[step][t + 1, c, rows_at, lanes]
            to[0, c, rows_to, lanes] = pltpu.roll(w, plane - LZ, 1)
            to[1, c, rows_to, lanes] = pltpu.roll(w, LZ, 1)
            for part in range(tiles):
                u = w[:, part * 128 : part * 128 + 128]
                here = pl.ds(pl.multiple_of(first_lane + part * 128, 128), 128)
                to[2, c, rows_to, here] = jnp.where(
                    depth == LZ - 1, pltpu.roll(u, LZ - 1, 1), pltpu.roll(u, 127, 1)
                )
                to[3, c, rows_to, here] = jnp.where(
                    depth == 0, pltpu.roll(u, 128 - (LZ - 1), 1), pltpu.roll(u, 1, 1)
                )

    def block(stage, lane, now):
        step, t, half = stage
        field = fields[step]
        lanes = (
            pl.ds(pl.multiple_of(lane * 128, 128), 128),
            pl.ds(pl.multiple_of(plane + lane * 128, 128), 128),
        )
        at_rows = [slice(half * 16 + 8 * h, half * 16 + 8 * h + 8) for h in range(2)]
        acc = {}
        for h in range(2):
            for r in range(3):
                for part in range(2):
                    mid = field[t + 1, r, at_rows[h], lanes[part]]
                    acc[h, r, part] = (1.0 - 6.0 * KAPPA) * mid
        for way in range(6):
            direction, back = way // 2, way % 2
            for c in range(3):
                sources = []
                for h in range(2):
                    if direction == 0:
                        p = t + 2 - 2 * back
                        sources.append([field[p, c, at_rows[h], lanes[i]] for i in range(2)])
                    else:
                        sources.append([now[way - 2, c, 8 * h : 8 * h + 8, lanes[i]] for i in range(2)])
                for r in range(3):
                    row = direction * 18 + (54 + c * 6 + r * 2 if back else r * 6 + c * 2)
                    ur = table[t, row, :, lanes[0]]
                    ui = table[t, row + 1, :, lanes[0]]
                    for h, (sr, si) in enumerate(sources):
                        if back:
                            acc[h, r, 0] = acc[h, r, 0] + (ur * sr + ui * si)
                            acc[h, r, 1] = acc[h, r, 1] + (ur * si - ui * sr)
                        else:
                            acc[h, r, 0] = acc[h, r, 0] + (ur * sr - ui * si)
                            acc[h, r, 1] = acc[h, r, 1] + (ur * si + ui * sr)
        both = slice(half * 16, half * 16 + 16)
        for r in range(3):
            for part in range(2):
                if step == 0:
                    for h in range(2):
                        field1[t + 1, r, at_rows[h], lanes[part]] = acc[h, r, part]
                if step == 1 or t in outer:
                    pair = jnp.concatenate([acc[0, r, part], acc[1, r, part]], axis=0).astype(low)
                    if step == 1:
                        smeared[position[t] * 3 + r, both, lanes[part]] = pair
                    else:
                        k_at = pl.ds(pl.multiple_of((2 * r + part) * plane + lane * 128, 128), 128)
                        hsend[half, outer.index(t), :, k_at] = pair

    stages = [(0, t, h) for h in range(halves) for t in inner]
    for h in range(halves):
        stages += [(0, t, h) for t in outer] + [(1, t, h) for t in inner]
    stages += [(1, t, h) for h in range(halves) for t in outer]

    def run(step, ts, h):
        for t in ts:
            i = stages.index((step, t, h))

            def trip(k, carry):
                shift(stages[(i + 1) % len(stages)], k, moved[(i + 1) % 2])
                block(stages[i], k, moved[i % 2])
                return carry

            lax.fori_loop(0, tiles, trip, 0)

    def begin(k, carry):
        shift(stages[0], k, moved[0])
        return carry

    lax.fori_loop(0, tiles, begin, 0)
    for h in range(halves):
        run(0, inner, h)

    def take(step, h, side):
        copies[step, h][side].wait_recv()
        for c in range(3):
            fields[step][planes + 1 if side else 0, c, 16 * h : 16 * h + 16] = (
                halo[step, h, side, :, c * wide : (c + 1) * wide].astype(f32)
            )

    links_up.wait_recv()
    for part in range(2):
        got = lrecv[16 * part : 16 * part + 16, :].astype(f32)
        for index in range(9):
            table[0, 54 + index * 2 + part] = jnp.broadcast_to(got[index : index + 1], (8, plane))
    for h in range(halves):
        for side in range(2):
            take(0, h, side)
            run(0, [outer[side]], h)
            copies[1, h][1 - side].start()
        if h == halves - 1:
            across[0].wait_recv()
            onward[0].start()
        run(1, inner, h)
    beside.wait_recv()
    onward[0].wait_recv()

    def fill(k, carry):
        re = pl.ds(pl.multiple_of(k * wide, wide), plane)
        im = pl.ds(pl.multiple_of(k * wide + plane, plane), plane)
        for slot in range(4):
            at_raw = slice(slot * unit, slot * unit + rows)
            at_turned = slice(slot * unit + rows, (slot + 1) * unit)
            right[at_turned, re] = -right[at_raw, im]
            right[at_turned, im] = right[at_raw, re]
        return carry

    members = (inner, outer)
    streamed = 16 * count
    per_half = ships // halves
    used = streamed - (per_half - 1) * width
    spare = used % 128 // 16
    if used + 16 * spare > width:
        spare = 0
    sizes = [width] * ships
    if spare and used - 16 * spare:
        sizes[per_half - 1] = used - 16 * spare
    order = [(h, half, t) for half in range(2) for h in range(halves) for t in members[half]]
    per = width // 16

    def ready(i):
        return order[i][1] == 0 or order[i][2] != outer[0]

    def turn(i):
        h, half, t = order[i]
        to = left[i % 2]
        for q in range(count):
            for lane in range(0, plane, 256):
                cosine = cosb[q, :, t * plane + lane : t * plane + lane + 256]
                sine = sinb[q, :, t * plane + lane : t * plane + lane + 256]
                for c in range(3):
                    k = position[t] * 3 + c
                    sr = smeared[k, 16 * h : 16 * h + 16, lane : lane + 256]
                    si = smeared[k, 16 * h : 16 * h + 16, plane + lane : plane + lane + 256]
                    col = c * wide + lane
                    to[16 * q : 16 * q + 16, col : col + 256] = cosine * sr + sine * si
                    to[16 * q : 16 * q + 16, col + plane : col + plane + 256] = cosine * si - sine * sr

    def product(i):
        h, half, t = order[i]
        first = position[t] * 3 * wide
        length = 3 * wide
        pieces = []
        for k in range(0, length, length // 2):
            pieces.append(
                lax.dot_general(
                    left[i % 2][:, k : k + length // 2],
                    right[:, first + k : first + k + length // 2],
                    (((1,), (1,)), ((), ())), preferred_element_type=f32,
                )
            )
        if i + 1 < len(order) and ready(i + 1):
            turn(i + 1)
        part = pieces[0] * scale + pieces[1] * scale
        if t == inner[0]:
            total[h, 0:streamed] = part
        else:
            total[h, 0:streamed] += part

    def finish(e):
        at = e % per_half * width
        part = total[e // per_half, at : at + sizes[e], :].T.astype(low)
        parted[e, 0, :, 0 : sizes[e]] = part[0 : 2 * unit]
        crossing[e, :, 0 : sizes[e]] = part[2 * unit :]

    roots = (v * 2 + s, (1 - v) * 2 + s)

    def cross(e):
        return remote(
            crossing.at[e, :, 0 : sizes[e]], parted.at[e, 1, :, 0 : sizes[e]], cross_sem.at[e], vec=1 - v
        )

    def ends(e, hop, ds):
        src = parted.at[e, hop, ds * unit : (ds + 1) * unit, 0 : sizes[e]]
        return src, rx.at[e, b, :, 0 : sizes[e]]

    def far(e, hop, ds):
        src, dst = ends(e, hop, ds)
        return pltpu.make_async_remote_copy(
            src_ref=src, dst_ref=dst,
            send_sem=last_sem.at[e, bricks + hop * 2 + ds], recv_sem=last_sem.at[e, b],
            device_id={"brick": roots[hop], "sub": (s + ds) % 2}, device_id_type=pl.DeviceIdType.MESH,
        )

    def depart(e, hop):
        far(e, hop, 1).start()

        @pl.when(roots[hop] != b)
        def _():
            far(e, hop, 0).start()

        @pl.when(roots[hop] == b)
        def _():
            src, dst = ends(e, hop, 0)
            pltpu.make_async_copy(src, dst, last_sem.at[e, b]).start()

    def ship(e):
        finish(e)
        cross(e).start()
        depart(e, 0)

    def hand_on(e):
        cross(e).wait_recv()
        depart(e, 1)

    def arrive(e):
        for i in range(bricks):
            dst = rx.at[e, i, :, 0 : sizes[e]]
            pltpu.make_async_copy(dst, dst, last_sem.at[e, i]).wait()

    def fill_half(half):
        first = len(inner) * 3 if half else 0
        count_k = len(members[half]) * 3
        lax.fori_loop(first, first + count_k, fill, 0)

    for i, (h, half, t) in enumerate(order):
        opens = t == members[half][0]
        if i == 0:
            fill_half(0)
        if half and opens:
            if h == 0:
                for part in (1, 2):
                    across[part].wait_recv()
                    onward[part].start()
            for side in range(2):
                take(1, h, side)
                run(1, [outer[side]], h)
            if h == 0:
                for part in (1, 2):
                    onward[part].wait_recv()
                fill_half(1)
            else:
                for e in range(per_half * (h - 1), per_half * h):
                    hand_on(e)
        if i == 0 or not ready(i):
            turn(i)
        product(i)
        if half and not opens:
            if h == halves - 1:
                total[h, streamed : streamed + 16 * spare] = total[0, 16 * (count - spare) : streamed]
            for e in range(per_half * h, per_half * (h + 1)):
                ship(e)
    for e in range(per_half * (halves - 1), ships):
        hand_on(e)
    lane_at = lax.broadcasted_iota(jnp.int32, (8, 128), 1)
    seen = set()
    for q in range(count):
        for first in range(0, unit, 8):
            pieces = []
            for h in range(halves):
                e, at = h * per_half + q // per, q % per * 16
                if h == 0 and q >= count - spare:
                    e, at = ships - 1, used + 16 * (q - count + spare)
                if e not in seen:
                    arrive(e)
                    seen.add(e)
                tile = slice(at // 128 * 128, at // 128 * 128 + 128)
                rows_at = slice(first // 16 * 16, first // 16 * 16 + 16)
                got = [rx[e, i, rows_at, tile].astype(f32) for i in range(bricks)]
                got = (got[0] + got[1]) + (got[2] + got[3])
                got = got[first % 16 : first % 16 + 8]
                turned = (16 * h - at) % 128
                pieces.append(pltpu.roll(got, turned, 1) if turned else got)
            value = jnp.where(lane_at < 16, pieces[0], pieces[1])
            start = (first % rows) * 2 * count + 2 * q + first // rows
            out_ref[pl.ds(start, 8, stride=2 * count), :] = value[:, 0:rows]
    sent = [links_up, *across, beside, *onward]
    for copy in copies.values():
        sent += copy
    sent += [cross(e) for e in range(ships)]
    for copy in sent:
        copy.wait_send()
    for e in range(ships):
        for hop in range(2):
            far(e, hop, 1).wait_send()

            @pl.when(roots[hop] != b)
            def _():
                far(e, hop, 0).wait_send()


def shards_fused(vectors, gauge_links, momenta):
    plane = LY * LZ
    rows, local_sites = vectors.shape[0], vectors.shape[3]
    planes = local_sites // plane
    tiles = plane // 128
    bricks = lax.axis_size("brick")
    count = momenta.shape[0]
    halves = rows // 16
    width = 256
    per_half = -(-count * 16 // width)
    ships = halves * per_half
    low, f32 = jnp.bfloat16, jnp.float32
    v = vectors.reshape((rows, 3, 2, planes * tiles, 128)).transpose((0, 1, 3, 2, 4))
    v = v.reshape((rows * 3, planes, tiles * 2, 128))
    g = gauge_links.reshape((27, 2, planes * tiles, 128)).transpose((0, 2, 1, 3))
    g = g.reshape((54 * planes * tiles, 128))
    wide = 2 * plane
    scale = (3.0 * bricks * local_sites) ** (-0.5)
    vmem, dma = pltpu.VMEM, pltpu.SemaphoreType.DMA
    plan = (planes, rows, count, bricks, ships, width, scale)
    out = pl.pallas_call(
        functools.partial(fused_kernel, plan),
        out_shape=jax.ShapeDtypeStruct((rows * count * 2, rows), f32),
        in_specs=[
            pl.BlockSpec(memory_space=pltpu.SMEM),
            pl.BlockSpec(memory_space=pl.ANY),
            pl.BlockSpec(memory_space=pl.ANY),
        ],
        out_specs=pl.BlockSpec(memory_space=pltpu.VMEM),
        scratch_shapes=[
            vmem((planes, rows * 3, tiles * 2, 128), f32),
            vmem((64 * planes * tiles, 128), f32),
            vmem((planes + 2, 3, rows, wide), f32),
            vmem((planes + 2, 3, rows, wide), f32),
            vmem((planes + 1, 108, 8, plane), f32),
            vmem((4, 3, 16, wide), f32),
            vmem((4, 3, 16, wide), f32),
            vmem((8 * rows, planes * 3 * wide), low),
            vmem((planes * 3, rows, wide), low),
            vmem((16 * count, 3 * wide), low),
            vmem((16 * count, 3 * wide), low),
            vmem((count, 16, local_sites), low),
            vmem((count, 16, local_sites), low),
            vmem((halves, per_half * width, 8 * rows), f32),
            vmem((ships, 2, 4 * rows, width), low),
            vmem((ships, 4 * rows, width), low),
            vmem((ships, bricks, 2 * rows, width), low),
            vmem((2, halves, 2, 16, 3 * wide), low),
            vmem((halves, 2, 16, 3 * wide), low),
            vmem((32, plane), low),
            vmem((32, plane), low),
            dma((planes + 1,)),
            dma((2, halves, 2, 2)),
            dma((2,)),
            dma((7, 2)),
            dma((ships, 2)),
            dma((ships, bricks + 4)),
        ],
        compiler_params=pltpu.CompilerParams(
            vmem_limit_bytes=60 * 2**20, collective_id=0, has_side_effects=True
        ),
        name="elementals",
    )(momenta.T, v, g)
    return out.reshape((rows, count, 2, rows))


def choose(vectors, gauge_links, momenta):
    plane = LY * LZ
    bricks, vecs, subs = (lax.axis_size(a) for a in ("brick", "vec", "sub"))
    rows, local_sites = vectors.shape[0], vectors.shape[3]
    fits = local_sites % plane == 0 and local_sites // plane == 4 and rows == 32
    if fits and vecs == 2 and subs == 2 and bricks == 4 and 24 <= momenta.shape[0] < 32:
        return shards_fused(vectors, gauge_links, momenta)
    return shards(vectors, gauge_links, momenta)


def solution(mesh):
    in_specs = (
        P(("vec", "sub"), None, None, ("grp", "brick")),
        P(None, None, None, None, ("grp", "brick")),
        P(),
    )
    out_specs = P(("vec", "sub"), "grp", None, "brick")
    return jax.shard_map(choose, mesh=mesh, in_specs=in_specs, out_specs=out_specs, check_vma=False)
```

```python
import functools
import math

import jax
import jax.numpy as jnp
from jax import lax
from jax.experimental import pallas as pl
from jax.experimental.pallas import tpu as pltpu
from jax.sharding import PartitionSpec as P

LY = 64
LZ = 8
ITERS = 2


KAPPA = 0.125


def from_behind(array, axis, by):
    peers = lax.axis_size(axis)
    return lax.ppermute(array, axis, [(i, (i + by) % peers) for i in range(peers)])


def padded_2(array, sides, width):
    for axis, dim in sides:
        peers, length = (lax.axis_size(axis), array.shape[dim])
        up = [(i, (i + 1) % peers) for i in range(peers)]
        down = [(j, i) for i, j in up]
        last = lax.slice_in_dim(array, length - width, length, axis=dim)
        initial = lax.slice_in_dim(array, 0, width, axis=dim)
        before = lax.ppermute(last, axis, up)
        after = lax.ppermute(initial, axis, down)
        array = jnp.concatenate([before, array, after], axis=dim)
    return array


def matrix_apply(matrix, source):
    matrix_real = matrix[:, :, 0][None]
    matrix_imag = matrix[:, :, 1][None]
    source_real = source[:, None, :, 0]
    source_imag = source[:, None, :, 1]
    real_part = jnp.sum(matrix_real * source_real - matrix_imag * source_imag, axis=2)
    imag_part = jnp.sum(matrix_real * source_imag + matrix_imag * source_real, axis=2)
    return jnp.stack([real_part, imag_part], axis=2)


def adjoint(matrix):
    return jnp.stack(
        [jnp.swapaxes(matrix[:, :, 0], 0, 1), -jnp.swapaxes(matrix[:, :, 1], 0, 1)], axis=2
    )


def step_depth(values, offset):
    depth_index = lax.iota(jnp.int32, values.shape[-1]) % LZ
    if offset > 0:
        return jnp.where(
            depth_index == LZ - 1, jnp.roll(values, LZ - 1, -1), jnp.roll(values, -1, -1)
        )
    return jnp.where(depth_index == 0, jnp.roll(values, 1 - LZ, -1), jnp.roll(values, 1, -1))


def step_column(values, offset):
    plane = LY * LZ
    column_index = lax.iota(jnp.int32, values.shape[-1]) // LZ % LY
    if offset > 0:
        return jnp.where(
            column_index == LY - 1, jnp.roll(values, plane - LZ, -1), jnp.roll(values, -LZ, -1)
        )
    return jnp.where(column_index == 0, jnp.roll(values, LZ - plane, -1), jnp.roll(values, LZ, -1))


def laplace_step(center, ahead, behind, here_links, back_links):
    forward = matrix_apply(here_links[0], ahead)
    backward = matrix_apply(adjoint(back_links), behind)
    total = forward + backward
    for direction, stepper in ((1, step_column), (2, step_depth)):
        forward = matrix_apply(here_links[direction], stepper(center, 1))
        backward = matrix_apply(adjoint(stepper(here_links[direction], -1)), stepper(center, -1))
        total = total + (forward + backward)
    return center + KAPPA * (total - 6.0 * center)


def shards(vectors, gauge_links, momenta):
    plane = LY * LZ
    local_sites = vectors.shape[3]
    raw_low = vectors.astype(jnp.bfloat16)
    field = vectors
    x_links = gauge_links[0]
    rim = from_behind(x_links[..., local_sites - plane :], "brick", 1)
    back_links = jnp.concatenate([rim, x_links[..., : local_sites - plane]], axis=3)
    for step in range(ITERS):
        padded = padded_2(field, (("brick", 3),), plane)
        field = laplace_step(
            padded[..., plane : plane + local_sites],
            padded[..., 2 * plane :],
            padded[..., :local_sites],
            gauge_links,
            back_links,
        )
    smeared_low = field.astype(jnp.bfloat16)
    raw_sites, smeared_sites = (
        lax.all_to_all(raw_low, ("vec", "sub"), split_axis=3, concat_axis=0, tiled=True),
        lax.all_to_all(smeared_low, ("vec", "sub"), split_axis=3, concat_axis=0, tiled=True),
    )
    groups = lax.axis_size(("vec", "sub"))
    total_vec = raw_sites.shape[0]
    width = raw_sites.shape[3]
    total_x = lax.axis_size("brick") * (local_sites // plane)
    first_site = lax.axis_index("brick") * local_sites + lax.axis_index(("vec", "sub")) * width
    site = first_site + lax.iota(jnp.int32, width)
    layer_index = (site // plane)[None]
    column_index = (site // LZ % LY)[None]
    depth_index = (site % LZ)[None]
    fraction = (
        jnp.mod(momenta[:, 0:1] * layer_index, total_x).astype(jnp.float32) / total_x
        + jnp.mod(momenta[:, 1:2] * column_index, LY).astype(jnp.float32) / LY
        + jnp.mod(momenta[:, 2:3] * depth_index, LZ).astype(jnp.float32) / LZ
    )
    angle = 2.0 * math.pi * fraction
    cosines = jnp.cos(angle)
    sines = jnp.sin(angle)
    right = smeared_sites.reshape((total_vec, 6 * width))
    scale = (3.0 * total_x * plane) ** (-0.5)

    def one_momentum(angles):
        cosine, sine = angles
        real_part = raw_sites[:, :, 0] * cosine - raw_sites[:, :, 1] * sine
        imag_part = raw_sites[:, :, 0] * sine + raw_sites[:, :, 1] * cosine
        phased = jnp.stack([real_part, imag_part], axis=2).astype(jnp.bfloat16)
        turned = jnp.stack([-phased[:, :, 1], phased[:, :, 0]], axis=2)
        left = jnp.concatenate(
            [
                phased.reshape((lax.axis_size(("vec", "sub")) * (total_vec // groups), 6 * width)),
                turned.reshape((lax.axis_size(("vec", "sub")) * (total_vec // groups), 6 * width)),
            ],
            axis=0,
        )
        product = lax.dot_general(
            left, right, (((1,), (1,)), ((), ())), preferred_element_type=jnp.float32
        )
        return product.reshape(
            (2, lax.axis_size(("vec", "sub")) * (total_vec // groups), total_vec)
        )

    blocks = lax.map(one_momentum, (cosines, sines))
    shares = lax.psum_scatter(
        jnp.transpose(blocks, (2, 0, 1, 3)) * scale, ("vec", "sub"), scatter_dimension=0, tiled=True
    )
    return lax.psum_scatter(shares, "brick", scatter_dimension=3, tiled=True)


def fused_kernel(plan, mom_ref, v_ref, g_ref, out_ref, *scratch):
    (vst, gst, field0, field1, table, moved0, moved1, right, smeared, left0, left1, cosb, sinb, total, parted,
     crossing, rx, halo, hsend, lsend, lrecv, load_sem, halo_sem, link_sem, raw_sem, cross_sem, last_sem) = scratch
    planes, rows, count, bricks, ships, width, scale = plan
    fields, moved = (field0, field1), (moved0, moved1)
    halves = rows // 16
    plane = LY * LZ
    tiles = plane // 128
    all_tiles = planes * tiles
    f32, low = jnp.float32, jnp.bfloat16
    wide = 2 * plane
    last = planes - 1
    inner = list(range(1, last))
    outer = [0, last]
    position = {t: i for i, t in enumerate(inner + outer)}
    cut = len(inner) * 3 * wide
    span = planes * 3 * wide
    b, v, s = (lax.axis_index(a) for a in ("brick", "vec", "sub"))
    left = (left0, left1)

    def remote(src, dst, sems, **ids):
        return pltpu.make_async_remote_copy(
            src_ref=src, dst_ref=dst, send_sem=sems.at[0], recv_sem=sems.at[1],
            device_id=ids, device_id_type=pl.DeviceIdType.MESH,
        )

    loads = {}
    for t in outer + inner:
        loads[t] = pltpu.make_async_copy(v_ref.at[:, t], vst.at[t], load_sem.at[t])
        loads[t].start()
    load_links = pltpu.make_async_copy(g_ref, gst.at[pl.ds(0, 54 * all_tiles)], load_sem.at[planes])
    load_links.start()
    barrier = pltpu.get_barrier_semaphore()
    for db in range(bricks):
        for ds in range(2):
            if db or ds:
                pl.semaphore_signal(
                    barrier, inc=1, device_id={"brick": (b + db) % bricks, "sub": (s + ds) % 2},
                    device_id_type=pl.DeviceIdType.MESH,
                )
    pl.semaphore_signal(
        barrier, inc=1, device_id={"vec": 1 - v}, device_id_type=pl.DeviceIdType.MESH
    )

    def unpack(t):
        flat = vst.at[t].reshape(rows * 3 * tiles * 2, 128)
        step = 3 * tiles * 2
        for c in range(3):
            for first in range(0, rows, 16):
                for part in range(2):
                    for lane in range(0, tiles, 2):
                        at = part * plane + lane * 128
                        quad = []
                        for h in range(2):
                            start = (first + 8 * h) * step + c * tiles * 2 + lane * 2 + part
                            quad.append(
                                jnp.concatenate(
                                    [flat[pl.ds(start + 2 * i, 8, stride=step), :] for i in range(2)], axis=1
                                )
                            )
                            field0[t + 1, c, first + 8 * h : first + 8 * h + 8, at : at + 256] = quad[h]
                        k = (position[t] * 3 + c) * wide + at
                        right[first : first + 16, k : k + 256] = jnp.concatenate(quad, axis=0).astype(low)

    def link_rows(t, part, group):
        return jnp.concatenate(
            [
                gst[pl.ds(group * 16 * all_tiles + (t * tiles + lane) * 2 + part, 8, stride=2 * all_tiles), :]
                for lane in range(tiles)
            ],
            axis=1,
        ) * KAPPA

    for t in outer:
        loads[t].wait()
        unpack(t)
    load_links.wait()
    for part in range(2):
        both = jnp.concatenate([link_rows(last, part, 0), link_rows(last, part, 1)], axis=0)
        lsend[16 * part : 16 * part + 16, :] = both.astype(low)
    pl.semaphore_wait(barrier, 2 * bricks)
    up, down = (b + 1) % bricks, (b + bricks - 1) % bricks

    def halos(step, h, low_src, high_src):
        sems = halo_sem.at[step, h]
        return (
            remote(high_src, halo.at[step, h, 0], sems.at[0], brick=up),
            remote(low_src, halo.at[step, h, 1], sems.at[1], brick=down),
        )

    def own(t, h):
        at = position[t] * 3 * wide
        return right.at[16 * h : 16 * h + 16, at : at + 3 * wide]

    copies = {}
    links_up = remote(lsend, lrecv, link_sem, brick=up)
    for h in range(halves):
        copies[0, h] = halos(0, h, own(0, h), own(last, h))
        copies[1, h] = halos(1, h, hsend.at[h, 0], hsend.at[h, 1])
        for copy in copies[0, h]:
            copy.start()
        if h == 0:
            links_up.start()
    for t in inner:
        loads[t].wait()
        unpack(t)
    parts = [slice(0, cut)] + [
        slice(cut + i * 3 * wide, cut + (i + 1) * 3 * wide) for i in range(2)
    ]
    unit = 2 * rows

    def raw_copy(index, from_slot, to_slot, ks, **ids):
        return remote(
            right.at[from_slot * unit : from_slot * unit + rows, ks],
            right.at[to_slot * unit : to_slot * unit + rows, ks],
            raw_sem.at[index], **ids,
        )

    across = [raw_copy(i, 0, 2, parts[i], vec=1 - v) for i in range(3)]
    beside = raw_copy(6, 0, 1, slice(0, span), sub=1 - s)
    onward = [raw_copy(3 + i, 2, 3, parts[i], sub=1 - s) for i in range(3)]
    for copy in across + [beside]:
        copy.start()

    depth_wide = lax.broadcasted_iota(jnp.int32, (8, plane), 1) % LZ
    depth = lax.broadcasted_iota(jnp.int32, (8, 128), 1) % LZ

    def spread(t, carry):
        for part in range(2):
            for group in range(4):
                here = link_rows(t, part, group)
                if group > 0:
                    by = pltpu.roll(here, LZ, 1)
                    bz = jnp.where(
                        depth_wide == 0, pltpu.roll(here, plane - (LZ - 1), 1), pltpu.roll(here, 1, 1)
                    )
                for j in range(min(8, 27 - 8 * group)):
                    index = group * 8 + j
                    row = jnp.broadcast_to(here[j : j + 1], (8, plane))
                    table[t, index * 2 + part] = row
                    if index < 9:
                        table[t + 1, 54 + index * 2 + part] = row
                    else:
                        back = by if index < 18 else bz
                        table[t, 54 + index * 2 + part] = jnp.broadcast_to(back[j : j + 1], (8, plane))
        return carry

    lax.fori_loop(0, planes, spread, 0)

    places = []
    for group in range(0, all_tiles, 8):
        height = min(8, all_tiles - group)
        site = (
            lax.broadcasted_iota(jnp.int32, (height, 128), 0) * 128
            + lax.broadcasted_iota(jnp.int32, (height, 128), 1)
            + group * 128
        )
        places.append(
            (
                (site // plane + b * planes).astype(f32) * (1.0 / (bricks * planes)),
                (site // LZ % LY).astype(f32) * (1.0 / LY),
                (site % LZ).astype(f32) * (1.0 / LZ),
            )
        )

    def phases(q, carry):
        n = [mom_ref[d, jnp.minimum(q, count - 1)].astype(f32) for d in range(3)]
        for group, (x, y, z) in enumerate(places):
            turns = n[0] * x + n[1] * y + n[2] * z
            half = jnp.round(2.0 * turns)
            sign = 1.0 - 2.0 * jnp.abs(half - 2.0 * jnp.round(0.5 * half))
            angle = (2.0 * math.pi) * (turns - 0.5 * half)
            square = angle * angle
            cosine, sine = 0.0, 0.0
            for i in range(7, 0, -1):
                cosine = (cosine * square) + (-1.0) ** i / math.factorial(2 * i)
            cosine = sign * (1.0 + cosine * square)
            for i in range(6, 0, -1):
                sine = (sine * square) + (-1.0) ** i / math.factorial(2 * i + 1)
            sine = sign * (angle + angle * (sine * square))
            for j in range(x.shape[0]):
                at = (group * 8 + j) * 128
                cosb[q, :, at : at + 128] = jnp.broadcast_to(cosine[j : j + 1], (16, 128)).astype(low)
                sinb[q, :, at : at + 128] = jnp.broadcast_to(sine[j : j + 1], (16, 128)).astype(low)
        return carry

    lax.fori_loop(0, count, phases, 0)

    def shift(stage, k, to):
        step, t, h = stage
        rows_to = pl.ds(pl.multiple_of(k % 2 * 8, 8), 8)
        rows_at = pl.ds(pl.multiple_of(h * 16 + k % 2 * 8, 8), 8)
        first_lane = k // 2 * plane
        lanes = pl.ds(pl.multiple_of(first_lane, plane), plane)
        for c in range(3):
            w = fields[step][t + 1, c, rows_at, lanes]
            to[0, c, rows_to, lanes] = pltpu.roll(w, plane - LZ, 1)
            to[1, c, rows_to, lanes] = pltpu.roll(w, LZ, 1)
            for part in range(tiles):
                u = w[:, part * 128 : part * 128 + 128]
                here = pl.ds(pl.multiple_of(first_lane + part * 128, 128), 128)
                to[2, c, rows_to, here] = jnp.where(
                    depth == LZ - 1, pltpu.roll(u, LZ - 1, 1), pltpu.roll(u, 127, 1)
                )
                to[3, c, rows_to, here] = jnp.where(
                    depth == 0, pltpu.roll(u, 128 - (LZ - 1), 1), pltpu.roll(u, 1, 1)
                )

    def block(stage, lane, now):
        step, t, half = stage
        field = fields[step]
        lanes = (
            pl.ds(pl.multiple_of(lane * 128, 128), 128),
            pl.ds(pl.multiple_of(plane + lane * 128, 128), 128),
        )
        at_rows = [slice(half * 16 + 8 * h, half * 16 + 8 * h + 8) for h in range(2)]
        acc = {}
        for h in range(2):
            for r in range(3):
                for part in range(2):
                    mid = field[t + 1, r, at_rows[h], lanes[part]]
                    acc[h, r, part] = (1.0 - 6.0 * KAPPA) * mid
        for way in range(6):
            direction, back = way // 2, way % 2
            for c in range(3):
                sources = []
                for h in range(2):
                    if direction == 0:
                        p = t + 2 - 2 * back
                        sources.append([field[p, c, at_rows[h], lanes[i]] for i in range(2)])
                    else:
                        sources.append([now[way - 2, c, 8 * h : 8 * h + 8, lanes[i]] for i in range(2)])
                for r in range(3):
                    row = direction * 18 + (54 + c * 6 + r * 2 if back else r * 6 + c * 2)
                    ur = table[t, row, :, lanes[0]]
                    ui = table[t, row + 1, :, lanes[0]]
                    for h, (sr, si) in enumerate(sources):
                        if back:
                            acc[h, r, 0] = acc[h, r, 0] + (ur * sr + ui * si)
                            acc[h, r, 1] = acc[h, r, 1] + (ur * si - ui * sr)
                        else:
                            acc[h, r, 0] = acc[h, r, 0] + (ur * sr - ui * si)
                            acc[h, r, 1] = acc[h, r, 1] + (ur * si + ui * sr)
        both = slice(half * 16, half * 16 + 16)
        for r in range(3):
            for part in range(2):
                if step == 0:
                    for h in range(2):
                        field1[t + 1, r, at_rows[h], lanes[part]] = acc[h, r, part]
                if step == 1 or t in outer:
                    pair = jnp.concatenate([acc[0, r, part], acc[1, r, part]], axis=0).astype(low)
                    if step == 1:
                        smeared[position[t] * 3 + r, both, lanes[part]] = pair
                    else:
                        k_at = pl.ds(pl.multiple_of((2 * r + part) * plane + lane * 128, 128), 128)
                        hsend[half, outer.index(t), :, k_at] = pair

    stages = [(0, t, h) for h in range(halves) for t in inner]
    for h in range(halves):
        stages += [(0, t, h) for t in outer] + [(1, t, h) for t in inner]
    stages += [(1, t, h) for h in range(halves) for t in outer]

    def run(step, ts, h):
        for t in ts:
            i = stages.index((step, t, h))

            def trip(k, carry):
                shift(stages[(i + 1) % len(stages)], k, moved[(i + 1) % 2])
                block(stages[i], k, moved[i % 2])
                return carry

            lax.fori_loop(0, tiles, trip, 0)

    def begin(k, carry):
        shift(stages[0], k, moved[0])
        return carry

    lax.fori_loop(0, tiles, begin, 0)
    for h in range(halves):
        run(0, inner, h)

    def take(step, h, side):
        copies[step, h][side].wait_recv()
        for c in range(3):
            fields[step][planes + 1 if side else 0, c, 16 * h : 16 * h + 16] = (
                halo[step, h, side, :, c * wide : (c + 1) * wide].astype(f32)
            )

    links_up.wait_recv()
    for part in range(2):
        got = lrecv[16 * part : 16 * part + 16, :].astype(f32)
        for index in range(9):
            table[0, 54 + index * 2 + part] = jnp.broadcast_to(got[index : index + 1], (8, plane))
    for h in range(halves):
        for side in range(2):
            take(0, h, side)
            run(0, [outer[side]], h)
            copies[1, h][1 - side].start()
        if h == halves - 1:
            across[0].wait_recv()
            onward[0].start()
        run(1, inner, h)
    beside.wait_recv()
    onward[0].wait_recv()

    def fill(k, carry):
        re = pl.ds(pl.multiple_of(k * wide, wide), plane)
        im = pl.ds(pl.multiple_of(k * wide + plane, plane), plane)
        for slot in range(4):
            at_raw = slice(slot * unit, slot * unit + rows)
            at_turned = slice(slot * unit + rows, (slot + 1) * unit)
            right[at_turned, re] = -right[at_raw, im]
            right[at_turned, im] = right[at_raw, re]
        return carry

    members = (inner, outer)
    streamed = 16 * count
    per_half = ships // halves
    used = streamed - (per_half - 1) * width
    spare = used % 128 // 16
    if used + 16 * spare > width:
        spare = 0
    sizes = [width] * ships
    if spare and used - 16 * spare:
        sizes[per_half - 1] = used - 16 * spare
    order = [(h, half, t) for half in range(2) for h in range(halves) for t in members[half]]
    per = width // 16

    def ready(i):
        return order[i] != (0, 1, outer[0])

    def turn(i):
        h, half, t = order[i]
        to = left[i % 2]
        for q in range(count):
            for lane in range(0, plane, 256):
                cosine = cosb[q, :, t * plane + lane : t * plane + lane + 256]
                sine = sinb[q, :, t * plane + lane : t * plane + lane + 256]
                for c in range(3):
                    k = position[t] * 3 + c
                    sr = smeared[k, 16 * h : 16 * h + 16, lane : lane + 256]
                    si = smeared[k, 16 * h : 16 * h + 16, plane + lane : plane + lane + 256]
                    col = c * wide + lane
                    to[16 * q : 16 * q + 16, col : col + 256] = cosine * sr + sine * si
                    to[16 * q : 16 * q + 16, col + plane : col + plane + 256] = cosine * si - sine * sr

    def product(i):
        h, half, t = order[i]
        first = position[t] * 3 * wide
        length = 3 * wide
        pieces = []
        for k in range(0, length, length // 2):
            pieces.append(
                lax.dot_general(
                    left[i % 2][:, k : k + length // 2],
                    right[:, first + k : first + k + length // 2],
                    (((1,), (1,)), ((), ())), preferred_element_type=f32,
                )
            )
        if i + 1 < len(order) and ready(i + 1):
            turn(i + 1)
        part = pieces[0] * scale + pieces[1] * scale
        if t == inner[0]:
            total[h, 0:streamed] = part
        else:
            total[h, 0:streamed] += part

    def finish(e):
        at = e % per_half * width
        part = total[e // per_half, at : at + sizes[e], :].T.astype(low)
        parted[e, 0, :, 0 : sizes[e]] = part[0 : 2 * unit]
        crossing[e, :, 0 : sizes[e]] = part[2 * unit :]

    roots = (v * 2 + s, (1 - v) * 2 + s)

    def cross(e):
        return remote(
            crossing.at[e, :, 0 : sizes[e]], parted.at[e, 1, :, 0 : sizes[e]], cross_sem.at[e], vec=1 - v
        )

    def ends(e, hop, ds):
        src = parted.at[e, hop, ds * unit : (ds + 1) * unit, 0 : sizes[e]]
        return src, rx.at[e, b, :, 0 : sizes[e]]

    def far(e, hop, ds):
        src, dst = ends(e, hop, ds)
        return pltpu.make_async_remote_copy(
            src_ref=src, dst_ref=dst,
            send_sem=last_sem.at[e, bricks + hop * 2 + ds], recv_sem=last_sem.at[e, b],
            device_id={"brick": roots[hop], "sub": (s + ds) % 2}, device_id_type=pl.DeviceIdType.MESH,
        )

    def depart(e, hop):
        far(e, hop, 1).start()

        @pl.when(roots[hop] != b)
        def _():
            far(e, hop, 0).start()

        @pl.when(roots[hop] == b)
        def _():
            src, dst = ends(e, hop, 0)
            pltpu.make_async_copy(src, dst, last_sem.at[e, b]).start()

    def ship(e):
        finish(e)
        cross(e).start()
        depart(e, 0)

    def hand_on(e):
        cross(e).wait_recv()
        depart(e, 1)

    def arrive(e):
        for i in range(bricks):
            dst = rx.at[e, i, :, 0 : sizes[e]]
            pltpu.make_async_copy(dst, dst, last_sem.at[e, i]).wait()

    def fill_half(half):
        first = len(inner) * 3 if half else 0
        count_k = len(members[half]) * 3
        lax.fori_loop(first, first + count_k, fill, 0)

    for i, (h, half, t) in enumerate(order):
        opens = t == members[half][0]
        if i == 0:
            fill_half(0)
        if half and opens and h == 0:
            for part in (1, 2):
                across[part].wait_recv()
                onward[part].start()
                for side in range(2):
                    take(1, part - 1, side)
                    run(1, [outer[side]], part - 1)
            for part in (1, 2):
                onward[part].wait_recv()
            fill_half(1)
        if i == 0 or not ready(i):
            turn(i)
        product(i)
        if half and opens and h:
            for e in range(per_half * (h - 1), per_half * h):
                hand_on(e)
        if half and not opens:
            if h == halves - 1:
                total[h, streamed : streamed + 16 * spare] = total[0, 16 * (count - spare) : streamed]
            for e in range(per_half * h, per_half * (h + 1)):
                ship(e)
    for e in range(per_half * (halves - 1), ships):
        hand_on(e)
    lane_at = lax.broadcasted_iota(jnp.int32, (8, 128), 1)
    seen = set()
    for q in range(count):
        for first in range(0, unit, 8):
            pieces = []
            for h in range(halves):
                e, at = h * per_half + q // per, q % per * 16
                if h == 0 and q >= count - spare:
                    e, at = ships - 1, used + 16 * (q - count + spare)
                if e not in seen:
                    arrive(e)
                    seen.add(e)
                tile = slice(at // 128 * 128, at // 128 * 128 + 128)
                rows_at = slice(first // 16 * 16, first // 16 * 16 + 16)
                got = [rx[e, i, rows_at, tile].astype(f32) for i in range(bricks)]
                got = (got[0] + got[1]) + (got[2] + got[3])
                got = got[first % 16 : first % 16 + 8]
                turned = (16 * h - at) % 128
                pieces.append(pltpu.roll(got, turned, 1) if turned else got)
            value = jnp.where(lane_at < 16, pieces[0], pieces[1])
            start = (first % rows) * 2 * count + 2 * q + first // rows
            out_ref[pl.ds(start, 8, stride=2 * count), :] = value[:, 0:rows]
    sent = [links_up, *across, beside, *onward]
    for copy in copies.values():
        sent += copy
    sent += [cross(e) for e in range(ships)]
    for copy in sent:
        copy.wait_send()
    for e in range(ships):
        for hop in range(2):
            far(e, hop, 1).wait_send()

            @pl.when(roots[hop] != b)
            def _():
                far(e, hop, 0).wait_send()


def shards_fused(vectors, gauge_links, momenta):
    plane = LY * LZ
    rows, local_sites = vectors.shape[0], vectors.shape[3]
    planes = local_sites // plane
    tiles = plane // 128
    bricks = lax.axis_size("brick")
    count = momenta.shape[0]
    halves = rows // 16
    width = 256
    per_half = -(-count * 16 // width)
    ships = halves * per_half
    low, f32 = jnp.bfloat16, jnp.float32
    v = vectors.reshape((rows, 3, 2, planes * tiles, 128)).transpose((0, 1, 3, 2, 4))
    v = v.reshape((rows * 3, planes, tiles * 2, 128))
    g = gauge_links.reshape((27, 2, planes * tiles, 128)).transpose((0, 2, 1, 3))
    g = g.reshape((54 * planes * tiles, 128))
    wide = 2 * plane
    scale = (3.0 * bricks * local_sites) ** (-0.5)
    vmem, dma = pltpu.VMEM, pltpu.SemaphoreType.DMA
    plan = (planes, rows, count, bricks, ships, width, scale)
    out = pl.pallas_call(
        functools.partial(fused_kernel, plan),
        out_shape=jax.ShapeDtypeStruct((rows * count * 2, rows), f32),
        in_specs=[
            pl.BlockSpec(memory_space=pltpu.SMEM),
            pl.BlockSpec(memory_space=pl.ANY),
            pl.BlockSpec(memory_space=pl.ANY),
        ],
        out_specs=pl.BlockSpec(memory_space=pltpu.VMEM),
        scratch_shapes=[
            vmem((planes, rows * 3, tiles * 2, 128), f32),
            vmem((64 * planes * tiles, 128), f32),
            vmem((planes + 2, 3, rows, wide), f32),
            vmem((planes + 2, 3, rows, wide), f32),
            vmem((planes + 1, 108, 8, plane), f32),
            vmem((4, 3, 16, wide), f32),
            vmem((4, 3, 16, wide), f32),
            vmem((8 * rows, planes * 3 * wide), low),
            vmem((planes * 3, rows, wide), low),
            vmem((16 * count, 3 * wide), low),
            vmem((16 * count, 3 * wide), low),
            vmem((count, 16, local_sites), low),
            vmem((count, 16, local_sites), low),
            vmem((halves, per_half * width, 8 * rows), f32),
            vmem((ships, 2, 4 * rows, width), low),
            vmem((ships, 4 * rows, width), low),
            vmem((ships, bricks, 2 * rows, width), low),
            vmem((2, halves, 2, 16, 3 * wide), low),
            vmem((halves, 2, 16, 3 * wide), low),
            vmem((32, plane), low),
            vmem((32, plane), low),
            dma((planes + 1,)),
            dma((2, halves, 2, 2)),
            dma((2,)),
            dma((7, 2)),
            dma((ships, 2)),
            dma((ships, bricks + 4)),
        ],
        compiler_params=pltpu.CompilerParams(
            vmem_limit_bytes=60 * 2**20, collective_id=0, has_side_effects=True
        ),
        name="elementals",
    )(momenta.T, v, g)
    return out.reshape((rows, count, 2, rows))


def choose(vectors, gauge_links, momenta):
    plane = LY * LZ
    bricks, vecs, subs = (lax.axis_size(a) for a in ("brick", "vec", "sub"))
    rows, local_sites = vectors.shape[0], vectors.shape[3]
    fits = local_sites % plane == 0 and local_sites // plane == 4 and rows == 32
    if fits and vecs == 2 and subs == 2 and bricks == 4 and 24 <= momenta.shape[0] < 32:
        return shards_fused(vectors, gauge_links, momenta)
    return shards(vectors, gauge_links, momenta)


def solution(mesh):
    in_specs = (
        P(("vec", "sub"), None, None, ("grp", "brick")),
        P(None, None, None, None, ("grp", "brick")),
        P(),
    )
    out_specs = P(("vec", "sub"), "grp", None, "brick")
    return jax.shard_map(choose, mesh=mesh, in_specs=in_specs, out_specs=out_specs, check_vma=False)
```

```python
import functools
import math

import jax
import jax.numpy as jnp
from jax import lax
from jax.experimental import pallas as pl
from jax.experimental.pallas import tpu as pltpu
from jax.sharding import PartitionSpec as P

LY = 64
LZ = 8
ITERS = 2


KAPPA = 0.125


def from_behind(array, axis, by):
    peers = lax.axis_size(axis)
    return lax.ppermute(array, axis, [(i, (i + by) % peers) for i in range(peers)])


def padded_2(array, sides, width):
    for axis, dim in sides:
        peers, length = (lax.axis_size(axis), array.shape[dim])
        up = [(i, (i + 1) % peers) for i in range(peers)]
        down = [(j, i) for i, j in up]
        last = lax.slice_in_dim(array, length - width, length, axis=dim)
        initial = lax.slice_in_dim(array, 0, width, axis=dim)
        before = lax.ppermute(last, axis, up)
        after = lax.ppermute(initial, axis, down)
        array = jnp.concatenate([before, array, after], axis=dim)
    return array


def matrix_apply(matrix, source):
    matrix_real = matrix[:, :, 0][None]
    matrix_imag = matrix[:, :, 1][None]
    source_real = source[:, None, :, 0]
    source_imag = source[:, None, :, 1]
    real_part = jnp.sum(matrix_real * source_real - matrix_imag * source_imag, axis=2)
    imag_part = jnp.sum(matrix_real * source_imag + matrix_imag * source_real, axis=2)
    return jnp.stack([real_part, imag_part], axis=2)


def adjoint(matrix):
    return jnp.stack(
        [jnp.swapaxes(matrix[:, :, 0], 0, 1), -jnp.swapaxes(matrix[:, :, 1], 0, 1)], axis=2
    )


def step_depth(values, offset):
    depth_index = lax.iota(jnp.int32, values.shape[-1]) % LZ
    if offset > 0:
        return jnp.where(
            depth_index == LZ - 1, jnp.roll(values, LZ - 1, -1), jnp.roll(values, -1, -1)
        )
    return jnp.where(depth_index == 0, jnp.roll(values, 1 - LZ, -1), jnp.roll(values, 1, -1))


def step_column(values, offset):
    plane = LY * LZ
    column_index = lax.iota(jnp.int32, values.shape[-1]) // LZ % LY
    if offset > 0:
        return jnp.where(
            column_index == LY - 1, jnp.roll(values, plane - LZ, -1), jnp.roll(values, -LZ, -1)
        )
    return jnp.where(column_index == 0, jnp.roll(values, LZ - plane, -1), jnp.roll(values, LZ, -1))


def laplace_step(center, ahead, behind, here_links, back_links):
    forward = matrix_apply(here_links[0], ahead)
    backward = matrix_apply(adjoint(back_links), behind)
    total = forward + backward
    for direction, stepper in ((1, step_column), (2, step_depth)):
        forward = matrix_apply(here_links[direction], stepper(center, 1))
        backward = matrix_apply(adjoint(stepper(here_links[direction], -1)), stepper(center, -1))
        total = total + (forward + backward)
    return center + KAPPA * (total - 6.0 * center)


def shards(vectors, gauge_links, momenta):
    plane = LY * LZ
    local_sites = vectors.shape[3]
    raw_low = vectors.astype(jnp.bfloat16)
    field = vectors
    x_links = gauge_links[0]
    rim = from_behind(x_links[..., local_sites - plane :], "brick", 1)
    back_links = jnp.concatenate([rim, x_links[..., : local_sites - plane]], axis=3)
    for step in range(ITERS):
        padded = padded_2(field, (("brick", 3),), plane)
        field = laplace_step(
            padded[..., plane : plane + local_sites],
            padded[..., 2 * plane :],
            padded[..., :local_sites],
            gauge_links,
            back_links,
        )
    smeared_low = field.astype(jnp.bfloat16)
    raw_sites, smeared_sites = (
        lax.all_to_all(raw_low, ("vec", "sub"), split_axis=3, concat_axis=0, tiled=True),
        lax.all_to_all(smeared_low, ("vec", "sub"), split_axis=3, concat_axis=0, tiled=True),
    )
    groups = lax.axis_size(("vec", "sub"))
    total_vec = raw_sites.shape[0]
    width = raw_sites.shape[3]
    total_x = lax.axis_size("brick") * (local_sites // plane)
    first_site = lax.axis_index("brick") * local_sites + lax.axis_index(("vec", "sub")) * width
    site = first_site + lax.iota(jnp.int32, width)
    layer_index = (site // plane)[None]
    column_index = (site // LZ % LY)[None]
    depth_index = (site % LZ)[None]
    fraction = (
        jnp.mod(momenta[:, 0:1] * layer_index, total_x).astype(jnp.float32) / total_x
        + jnp.mod(momenta[:, 1:2] * column_index, LY).astype(jnp.float32) / LY
        + jnp.mod(momenta[:, 2:3] * depth_index, LZ).astype(jnp.float32) / LZ
    )
    angle = 2.0 * math.pi * fraction
    cosines = jnp.cos(angle)
    sines = jnp.sin(angle)
    right = smeared_sites.reshape((total_vec, 6 * width))
    scale = (3.0 * total_x * plane) ** (-0.5)

    def one_momentum(angles):
        cosine, sine = angles
        real_part = raw_sites[:, :, 0] * cosine - raw_sites[:, :, 1] * sine
        imag_part = raw_sites[:, :, 0] * sine + raw_sites[:, :, 1] * cosine
        phased = jnp.stack([real_part, imag_part], axis=2).astype(jnp.bfloat16)
        turned = jnp.stack([-phased[:, :, 1], phased[:, :, 0]], axis=2)
        left = jnp.concatenate(
            [
                phased.reshape((lax.axis_size(("vec", "sub")) * (total_vec // groups), 6 * width)),
                turned.reshape((lax.axis_size(("vec", "sub")) * (total_vec // groups), 6 * width)),
            ],
            axis=0,
        )
        product = lax.dot_general(
            left, right, (((1,), (1,)), ((), ())), preferred_element_type=jnp.float32
        )
        return product.reshape(
            (2, lax.axis_size(("vec", "sub")) * (total_vec // groups), total_vec)
        )

    blocks = lax.map(one_momentum, (cosines, sines))
    shares = lax.psum_scatter(
        jnp.transpose(blocks, (2, 0, 1, 3)) * scale, ("vec", "sub"), scatter_dimension=0, tiled=True
    )
    return lax.psum_scatter(shares, "brick", scatter_dimension=3, tiled=True)


def fused_kernel(plan, momenta_ref, v_ref, g_ref, out_ref, *scratch):
    (mom_ref, mom_sem, vst, gst, field0, field1, table, moved0, moved1, right, smeared, left0, left1, cosb, sinb, total, parted,
     crossing, rx, halo, hsend, lsend, lrecv, load_sem, halo_sem, link_sem, raw_sem, cross_sem, last_sem) = scratch
    planes, rows, count, bricks, ships, width, scale = plan
    fields, moved = (field0, field1), (moved0, moved1)
    halves = rows // 16
    plane = LY * LZ
    tiles = plane // 128
    all_tiles = planes * tiles
    f32, low = jnp.float32, jnp.bfloat16
    wide = 2 * plane
    last = planes - 1
    inner = list(range(1, last))
    outer = [0, last]
    position = {t: i for i, t in enumerate(inner + outer)}
    cut = len(inner) * 3 * wide
    span = planes * 3 * wide
    b, v, s = (lax.axis_index(a) for a in ("brick", "vec", "sub"))
    left = (left0, left1)

    def remote(src, dst, sems, **ids):
        return pltpu.make_async_remote_copy(
            src_ref=src, dst_ref=dst, send_sem=sems.at[0], recv_sem=sems.at[1],
            device_id=ids, device_id_type=pl.DeviceIdType.MESH,
        )

    loads = {}
    for t in outer + inner:
        loads[t] = pltpu.make_async_copy(v_ref.at[:, t], vst.at[t], load_sem.at[t])
        loads[t].start()
    load_links = pltpu.make_async_copy(g_ref, gst.at[pl.ds(0, 54 * all_tiles)], load_sem.at[planes])
    load_links.start()
    load_momenta = pltpu.make_async_copy(momenta_ref, mom_ref, mom_sem)
    load_momenta.start()
    barrier = pltpu.get_barrier_semaphore()
    for db in range(bricks):
        for ds in range(2):
            if db or ds:
                pl.semaphore_signal(
                    barrier, inc=1, device_id={"brick": (b + db) % bricks, "sub": (s + ds) % 2},
                    device_id_type=pl.DeviceIdType.MESH,
                )
    pl.semaphore_signal(
        barrier, inc=1, device_id={"vec": 1 - v}, device_id_type=pl.DeviceIdType.MESH
    )

    def unpack(t):
        flat = vst.at[t].reshape(rows * 3 * tiles * 2, 128)
        step = 3 * tiles * 2
        for c in range(3):
            for first in range(0, rows, 16):
                for part in range(2):
                    for lane in range(0, tiles, 2):
                        at = part * plane + lane * 128
                        quad = []
                        for h in range(2):
                            start = (first + 8 * h) * step + c * tiles * 2 + lane * 2 + part
                            quad.append(
                                jnp.concatenate(
                                    [flat[pl.ds(start + 2 * i, 8, stride=step), :] for i in range(2)], axis=1
                                )
                            )
                            field0[t + 1, c, first + 8 * h : first + 8 * h + 8, at : at + 256] = quad[h]
                        k = (position[t] * 3 + c) * wide + at
                        right[first : first + 16, k : k + 256] = jnp.concatenate(quad, axis=0).astype(low)

    def link_rows(t, part, group):
        return jnp.concatenate(
            [
                gst[pl.ds(group * 16 * all_tiles + (t * tiles + lane) * 2 + part, 8, stride=2 * all_tiles), :]
                for lane in range(tiles)
            ],
            axis=1,
        ) * KAPPA

    for t in outer:
        loads[t].wait()
        unpack(t)
    load_links.wait()
    for part in range(2):
        both = jnp.concatenate([link_rows(last, part, 0), link_rows(last, part, 1)], axis=0)
        lsend[16 * part : 16 * part + 16, :] = both.astype(low)
    pl.semaphore_wait(barrier, 2 * bricks)
    up, down = (b + 1) % bricks, (b + bricks - 1) % bricks

    def halos(step, h, low_src, high_src):
        sems = halo_sem.at[step, h]
        return (
            remote(high_src, halo.at[step, h, 0], sems.at[0], brick=up),
            remote(low_src, halo.at[step, h, 1], sems.at[1], brick=down),
        )

    def own(t, h):
        at = position[t] * 3 * wide
        return right.at[16 * h : 16 * h + 16, at : at + 3 * wide]

    copies = {}
    links_up = remote(lsend, lrecv, link_sem, brick=up)
    for h in range(halves):
        copies[0, h] = halos(0, h, own(0, h), own(last, h))
        copies[1, h] = halos(1, h, hsend.at[h, 0], hsend.at[h, 1])
        for copy in copies[0, h]:
            copy.start()
        if h == 0:
            links_up.start()
    for t in inner:
        loads[t].wait()
        unpack(t)
    parts = [slice(0, cut)] + [
        slice(cut + i * 3 * wide, cut + (i + 1) * 3 * wide) for i in range(2)
    ]
    unit = 2 * rows

    def raw_copy(index, from_slot, to_slot, ks, **ids):
        return remote(
            right.at[from_slot * unit : from_slot * unit + rows, ks],
            right.at[to_slot * unit : to_slot * unit + rows, ks],
            raw_sem.at[index], **ids,
        )

    across = [raw_copy(i, 0, 2, parts[i], vec=1 - v) for i in range(3)]
    beside = raw_copy(6, 0, 1, slice(0, span), sub=1 - s)
    onward = [raw_copy(3 + i, 2, 3, parts[i], sub=1 - s) for i in range(3)]
    for copy in across + [beside]:
        copy.start()

    depth_wide = lax.broadcasted_iota(jnp.int32, (8, plane), 1) % LZ
    depth = lax.broadcasted_iota(jnp.int32, (8, 128), 1) % LZ

    def spread(t, carry):
        for part in range(2):
            for group in range(4):
                here = link_rows(t, part, group)
                if group > 0:
                    by = pltpu.roll(here, LZ, 1)
                    bz = jnp.where(
                        depth_wide == 0, pltpu.roll(here, plane - (LZ - 1), 1), pltpu.roll(here, 1, 1)
                    )
                for j in range(min(8, 27 - 8 * group)):
                    index = group * 8 + j
                    row = jnp.broadcast_to(here[j : j + 1], (8, plane))
                    table[t, index * 2 + part] = row
                    if index < 9:
                        table[t + 1, 54 + index * 2 + part] = row
                    else:
                        back = by if index < 18 else bz
                        table[t, 54 + index * 2 + part] = jnp.broadcast_to(back[j : j + 1], (8, plane))
        return carry

    lax.fori_loop(0, planes, spread, 0)

    places = []
    for group in range(0, all_tiles, 8):
        height = min(8, all_tiles - group)
        site = (
            lax.broadcasted_iota(jnp.int32, (height, 128), 0) * 128
            + lax.broadcasted_iota(jnp.int32, (height, 128), 1)
            + group * 128
        )
        places.append(
            (
                (site // plane + b * planes).astype(f32) * (1.0 / (bricks * planes)),
                (site // LZ % LY).astype(f32) * (1.0 / LY),
                (site % LZ).astype(f32) * (1.0 / LZ),
            )
        )

    def phases(q, carry):
        n = [mom_ref[d, jnp.minimum(q, count - 1)].astype(f32) for d in range(3)]
        for group, (x, y, z) in enumerate(places):
            turns = n[0] * x + n[1] * y + n[2] * z
            half = jnp.round(2.0 * turns)
            sign = 1.0 - 2.0 * jnp.abs(half - 2.0 * jnp.round(0.5 * half))
            angle = (2.0 * math.pi) * (turns - 0.5 * half)
            square = angle * angle
            cosine, sine = 0.0, 0.0
            for i in range(7, 0, -1):
                cosine = (cosine * square) + (-1.0) ** i / math.factorial(2 * i)
            cosine = sign * (1.0 + cosine * square)
            for i in range(6, 0, -1):
                sine = (sine * square) + (-1.0) ** i / math.factorial(2 * i + 1)
            sine = sign * (angle + angle * (sine * square))
            for j in range(x.shape[0]):
                at = (group * 8 + j) * 128
                cosb[q, :, at : at + 128] = jnp.broadcast_to(cosine[j : j + 1], (16, 128)).astype(low)
                sinb[q, :, at : at + 128] = jnp.broadcast_to(sine[j : j + 1], (16, 128)).astype(low)
        return carry

    load_momenta.wait()
    lax.fori_loop(0, count, phases, 0)

    def shift(stage, k, to):
        step, t, h = stage
        rows_to = pl.ds(pl.multiple_of(k % 2 * 8, 8), 8)
        rows_at = pl.ds(pl.multiple_of(h * 16 + k % 2 * 8, 8), 8)
        first_lane = k // 2 * plane
        lanes = pl.ds(pl.multiple_of(first_lane, plane), plane)
        for c in range(3):
            w = fields[step][t + 1, c, rows_at, lanes]
            to[0, c, rows_to, lanes] = pltpu.roll(w, plane - LZ, 1)
            to[1, c, rows_to, lanes] = pltpu.roll(w, LZ, 1)
            for part in range(tiles):
                u = w[:, part * 128 : part * 128 + 128]
                here = pl.ds(pl.multiple_of(first_lane + part * 128, 128), 128)
                to[2, c, rows_to, here] = jnp.where(
                    depth == LZ - 1, pltpu.roll(u, LZ - 1, 1), pltpu.roll(u, 127, 1)
                )
                to[3, c, rows_to, here] = jnp.where(
                    depth == 0, pltpu.roll(u, 128 - (LZ - 1), 1), pltpu.roll(u, 1, 1)
                )

    def block(stage, lane, now):
        step, t, half = stage
        field = fields[step]
        lanes = (
            pl.ds(pl.multiple_of(lane * 128, 128), 128),
            pl.ds(pl.multiple_of(plane + lane * 128, 128), 128),
        )
        at_rows = [slice(half * 16 + 8 * h, half * 16 + 8 * h + 8) for h in range(2)]
        acc = {}
        for h in range(2):
            for r in range(3):
                for part in range(2):
                    mid = field[t + 1, r, at_rows[h], lanes[part]]
                    acc[h, r, part] = (1.0 - 6.0 * KAPPA) * mid
        for way in range(6):
            direction, back = way // 2, way % 2
            for c in range(3):
                sources = []
                for h in range(2):
                    if direction == 0:
                        p = t + 2 - 2 * back
                        sources.append([field[p, c, at_rows[h], lanes[i]] for i in range(2)])
                    else:
                        sources.append([now[way - 2, c, 8 * h : 8 * h + 8, lanes[i]] for i in range(2)])
                for r in range(3):
                    row = direction * 18 + (54 + c * 6 + r * 2 if back else r * 6 + c * 2)
                    ur = table[t, row, :, lanes[0]]
                    ui = table[t, row + 1, :, lanes[0]]
                    for h, (sr, si) in enumerate(sources):
                        if back:
                            acc[h, r, 0] = acc[h, r, 0] + (ur * sr + ui * si)
                            acc[h, r, 1] = acc[h, r, 1] + (ur * si - ui * sr)
                        else:
                            acc[h, r, 0] = acc[h, r, 0] + (ur * sr - ui * si)
                            acc[h, r, 1] = acc[h, r, 1] + (ur * si + ui * sr)
        both = slice(half * 16, half * 16 + 16)
        for r in range(3):
            for part in range(2):
                if step == 0:
                    for h in range(2):
                        field1[t + 1, r, at_rows[h], lanes[part]] = acc[h, r, part]
                if step == 1 or t in outer:
                    pair = jnp.concatenate([acc[0, r, part], acc[1, r, part]], axis=0).astype(low)
                    if step == 1:
                        smeared[position[t] * 3 + r, both, lanes[part]] = pair
                    else:
                        k_at = pl.ds(pl.multiple_of((2 * r + part) * plane + lane * 128, 128), 128)
                        hsend[half, outer.index(t), :, k_at] = pair

    stages = [(0, t, h) for h in range(halves) for t in inner]
    for h in range(halves):
        stages += [(0, t, h) for t in outer] + [(1, t, h) for t in inner]
    stages += [(1, t, h) for h in range(halves) for t in outer]

    def run(step, ts, h):
        for t in ts:
            i = stages.index((step, t, h))

            def trip(k, carry):
                shift(stages[(i + 1) % len(stages)], k, moved[(i + 1) % 2])
                block(stages[i], k, moved[i % 2])
                return carry

            lax.fori_loop(0, tiles, trip, 0)

    def begin(k, carry):
        shift(stages[0], k, moved[0])
        return carry

    lax.fori_loop(0, tiles, begin, 0)
    for h in range(halves):
        run(0, inner, h)

    def take(step, h, side):
        copies[step, h][side].wait_recv()
        for c in range(3):
            fields[step][planes + 1 if side else 0, c, 16 * h : 16 * h + 16] = (
                halo[step, h, side, :, c * wide : (c + 1) * wide].astype(f32)
            )

    links_up.wait_recv()
    for part in range(2):
        got = lrecv[16 * part : 16 * part + 16, :].astype(f32)
        for index in range(9):
            table[0, 54 + index * 2 + part] = jnp.broadcast_to(got[index : index + 1], (8, plane))
    for h in range(halves):
        for side in range(2):
            take(0, h, side)
            run(0, [outer[side]], h)
            copies[1, h][1 - side].start()
        if h == halves - 1:
            across[0].wait_recv()
            onward[0].start()
        run(1, inner, h)
    beside.wait_recv()
    onward[0].wait_recv()

    def fill(k, carry):
        re = pl.ds(pl.multiple_of(k * wide, wide), plane)
        im = pl.ds(pl.multiple_of(k * wide + plane, plane), plane)
        for slot in range(4):
            at_raw = slice(slot * unit, slot * unit + rows)
            at_turned = slice(slot * unit + rows, (slot + 1) * unit)
            right[at_turned, re] = -right[at_raw, im]
            right[at_turned, im] = right[at_raw, re]
        return carry

    members = (inner, outer)
    streamed = 16 * count
    per_half, used, spare, sizes = pieces_of(count, halves, ships, width)
    order = [(h, half, t) for half in range(2) for h in range(halves) for t in members[half]]
    per = width // 16

    def ready(i):
        return order[i][1] == 0 or order[i][2] != outer[0]

    def turn(i):
        h, half, t = order[i]
        to = left[i % 2]
        for q in range(count):
            for lane in range(0, plane, 256):
                cosine = cosb[q, :, t * plane + lane : t * plane + lane + 256]
                sine = sinb[q, :, t * plane + lane : t * plane + lane + 256]
                for c in range(3):
                    k = position[t] * 3 + c
                    sr = smeared[k, 16 * h : 16 * h + 16, lane : lane + 256]
                    si = smeared[k, 16 * h : 16 * h + 16, plane + lane : plane + lane + 256]
                    col = c * wide + lane
                    to[16 * q : 16 * q + 16, col : col + 256] = cosine * sr + sine * si
                    to[16 * q : 16 * q + 16, col + plane : col + plane + 256] = cosine * si - sine * sr

    def product(i):
        h, half, t = order[i]
        first = position[t] * 3 * wide
        length = 3 * wide
        pieces = []
        for k in range(0, length, length // 2):
            pieces.append(
                lax.dot_general(
                    left[i % 2][:, k : k + length // 2],
                    right[:, first + k : first + k + length // 2],
                    (((1,), (1,)), ((), ())), preferred_element_type=f32,
                )
            )
        if i + 1 < len(order) and ready(i + 1):
            turn(i + 1)
        part = pieces[0] * scale + pieces[1] * scale
        if t == inner[0]:
            total[h, 0:streamed] = part
        else:
            total[h, 0:streamed] += part

    def finish(e):
        at = e % per_half * width
        part = total[e // per_half, at : at + sizes[e], :].T.astype(low)
        parted[e, 0, :, 0 : sizes[e]] = part[0 : 2 * unit]
        crossing[e, :, 0 : sizes[e]] = part[2 * unit :]

    roots = (v * 2 + s, (1 - v) * 2 + s)

    def cross(e):
        return remote(
            crossing.at[e, :, 0 : sizes[e]], parted.at[e, 1, :, 0 : sizes[e]], cross_sem.at[e], vec=1 - v
        )

    def ends(e, hop, ds):
        src = parted.at[e, hop, ds * unit : (ds + 1) * unit, 0 : sizes[e]]
        return src, rx.at[e, b, :, 0 : sizes[e]]

    def far(e, hop, ds):
        src, dst = ends(e, hop, ds)
        return pltpu.make_async_remote_copy(
            src_ref=src, dst_ref=dst,
            send_sem=last_sem.at[e, bricks + hop * 2 + ds], recv_sem=last_sem.at[e, b],
            device_id={"brick": roots[hop], "sub": (s + ds) % 2}, device_id_type=pl.DeviceIdType.MESH,
        )

    def depart(e, hop):
        far(e, hop, 1).start()

        @pl.when(roots[hop] != b)
        def _():
            far(e, hop, 0).start()

        @pl.when(roots[hop] == b)
        def _():
            src, dst = ends(e, hop, 0)
            pltpu.make_async_copy(src, dst, last_sem.at[e, b]).start()

    def ship(e):
        finish(e)
        cross(e).start()
        depart(e, 0)

    def hand_on(e):
        cross(e).wait_recv()
        depart(e, 1)

    def arrive(e):
        for i in range(bricks):
            dst = rx.at[e, i, :, 0 : sizes[e]]
            pltpu.make_async_copy(dst, dst, last_sem.at[e, i]).wait()

    def fill_half(half):
        first = len(inner) * 3 if half else 0
        count_k = len(members[half]) * 3
        lax.fori_loop(first, first + count_k, fill, 0)

    for i, (h, half, t) in enumerate(order):
        opens = t == members[half][0]
        if i == 0:
            fill_half(0)
        if half and opens:
            if h == 0:
                for part in (1, 2):
                    across[part].wait_recv()
                    onward[part].start()
            for side in range(2):
                take(1, h, side)
                run(1, [outer[side]], h)
            if h == 0:
                for part in (1, 2):
                    onward[part].wait_recv()
                fill_half(1)
            else:
                for e in range(per_half * (h - 1), per_half * h):
                    hand_on(e)
        if i == 0 or not ready(i):
            turn(i)
        product(i)
        if half and not opens:
            if h == halves - 1:
                total[h, streamed : streamed + 16 * spare] = total[0, 16 * (count - spare) : streamed]
            for e in range(per_half * h, per_half * (h + 1)):
                ship(e)
    for e in range(per_half * (halves - 1), ships):
        hand_on(e)
    for e in [i * per_half + j for j in range(per_half) for i in range(halves)]:
        arrive(e)
        got = [rx[e, i, :, 0 : sizes[e]].astype(f32) for i in range(bricks)]
        out_ref[:, e * width : e * width + sizes[e]] = (got[0] + got[1]) + (got[2] + got[3])
    sent = [links_up, *across, beside, *onward]
    for copy in copies.values():
        sent += copy
    sent += [cross(e) for e in range(ships)]
    for copy in sent:
        copy.wait_send()
    for e in range(ships):
        for hop in range(2):
            far(e, hop, 1).wait_send()

            @pl.when(roots[hop] != b)
            def _():
                far(e, hop, 0).wait_send()


def pieces_of(count, halves, ships, width):
    per_half = ships // halves
    used = 16 * count - (per_half - 1) * width
    spare = used % 128 // 16
    if used + 16 * spare > width:
        spare = 0
    sizes = [width] * ships
    if spare and used - 16 * spare:
        sizes[per_half - 1] = used - 16 * spare
    return per_half, used, spare, sizes


def rows_kernel(plan, sums_ref, out_ref):
    rows, count, ships, width = plan
    halves, unit = rows // 16, 2 * rows
    per = width // 16
    per_half, used, spare, _ = pieces_of(count, halves, ships, width)
    lane_at = lax.broadcasted_iota(jnp.int32, (8, 128), 1)
    for q in range(count):
        for first in range(0, unit, 8):
            pieces = []
            for h in range(halves):
                e, at = h * per_half + q // per, q % per * 16
                if h == 0 and q >= count - spare:
                    e, at = ships - 1, used + 16 * (q - count + spare)
                tile = e * width + at // 128 * 128
                got = sums_ref[first : first + 8, tile : tile + 128]
                turned = (16 * h - at) % 128
                pieces.append(pltpu.roll(got, turned, 1) if turned else got)
            value = jnp.where(lane_at < 16, pieces[0], pieces[1])
            start = (first % rows) * 2 * count + 2 * q + first // rows
            out_ref[pl.ds(start, 8, stride=2 * count), :] = value[:, 0:rows]


def shards_fused(vectors, gauge_links, momenta):
    plane = LY * LZ
    rows, local_sites = vectors.shape[0], vectors.shape[3]
    planes = local_sites // plane
    tiles = plane // 128
    bricks = lax.axis_size("brick")
    count = momenta.shape[0]
    halves = rows // 16
    width = 256
    per_half = -(-count * 16 // width)
    ships = halves * per_half
    low, f32 = jnp.bfloat16, jnp.float32
    v = vectors.reshape((rows, 3, 2, planes * tiles, 128)).transpose((0, 1, 3, 2, 4))
    v = v.reshape((rows * 3, planes, tiles * 2, 128))
    g = gauge_links.reshape((27, 2, planes * tiles, 128)).transpose((0, 2, 1, 3))
    g = g.reshape((54 * planes * tiles, 128))
    wide = 2 * plane
    scale = (3.0 * bricks * local_sites) ** (-0.5)
    vmem, dma = pltpu.VMEM, pltpu.SemaphoreType.DMA
    plan = (planes, rows, count, bricks, ships, width, scale)
    out = pl.pallas_call(
        functools.partial(fused_kernel, plan),
        out_shape=jax.ShapeDtypeStruct((2 * rows, ships * width), f32),
        in_specs=[
            pl.BlockSpec(memory_space=pl.ANY),
            pl.BlockSpec(memory_space=pl.ANY),
            pl.BlockSpec(memory_space=pl.ANY),
        ],
        out_specs=pl.BlockSpec(memory_space=pltpu.VMEM),
        scratch_shapes=[
            pltpu.SMEM((3, count), jnp.int32),
            dma,
            vmem((planes, rows * 3, tiles * 2, 128), f32),
            vmem((64 * planes * tiles, 128), f32),
            vmem((planes + 2, 3, rows, wide), f32),
            vmem((planes + 2, 3, rows, wide), f32),
            vmem((planes + 1, 108, 8, plane), f32),
            vmem((4, 3, 16, wide), f32),
            vmem((4, 3, 16, wide), f32),
            vmem((8 * rows, planes * 3 * wide), low),
            vmem((planes * 3, rows, wide), low),
            vmem((16 * count, 3 * wide), low),
            vmem((16 * count, 3 * wide), low),
            vmem((count, 16, local_sites), low),
            vmem((count, 16, local_sites), low),
            vmem((halves, per_half * width, 8 * rows), f32),
            vmem((ships, 2, 4 * rows, width), low),
            vmem((ships, 4 * rows, width), low),
            vmem((ships, bricks, 2 * rows, width), low),
            vmem((2, halves, 2, 16, 3 * wide), low),
            vmem((halves, 2, 16, 3 * wide), low),
            vmem((32, plane), low),
            vmem((32, plane), low),
            dma((planes + 1,)),
            dma((2, halves, 2, 2)),
            dma((2,)),
            dma((7, 2)),
            dma((ships, 2)),
            dma((ships, bricks + 4)),
        ],
        compiler_params=pltpu.CompilerParams(
            vmem_limit_bytes=60 * 2**20, collective_id=0, has_side_effects=True
        ),
        name="elementals",
    )(momenta.T, v, g)
    out = pl.pallas_call(
        functools.partial(rows_kernel, (rows, count, ships, width)),
        out_shape=jax.ShapeDtypeStruct((rows * count * 2, rows), f32),
        in_specs=[pl.BlockSpec(memory_space=pltpu.VMEM)],
        out_specs=pl.BlockSpec(memory_space=pltpu.VMEM),
        name="rows",
    )(out)
    return out.reshape((rows, count, 2, rows))


def choose(vectors, gauge_links, momenta):
    plane = LY * LZ
    bricks, vecs, subs = (lax.axis_size(a) for a in ("brick", "vec", "sub"))
    rows, local_sites = vectors.shape[0], vectors.shape[3]
    fits = local_sites % plane == 0 and local_sites // plane == 4 and rows == 32
    if fits and vecs == 2 and subs == 2 and bricks == 4 and 24 <= momenta.shape[0] < 32:
        return shards_fused(vectors, gauge_links, momenta)
    return shards(vectors, gauge_links, momenta)


def solution(mesh):
    in_specs = (
        P(("vec", "sub"), None, None, ("grp", "brick")),
        P(None, None, None, None, ("grp", "brick")),
        P(),
    )
    out_specs = P(("vec", "sub"), "grp", None, "brick")
    return jax.shard_map(choose, mesh=mesh, in_specs=in_specs, out_specs=out_specs, check_vma=False)
```

```python
import functools
import math

import jax
import jax.numpy as jnp
from jax import lax
from jax.experimental import pallas as pl
from jax.experimental.pallas import tpu as pltpu
from jax.sharding import PartitionSpec as P

LY = 64
LZ = 8
ITERS = 2


KAPPA = 0.125


def from_behind(array, axis, by):
    peers = lax.axis_size(axis)
    return lax.ppermute(array, axis, [(i, (i + by) % peers) for i in range(peers)])


def padded_2(array, sides, width):
    for axis, dim in sides:
        peers, length = (lax.axis_size(axis), array.shape[dim])
        up = [(i, (i + 1) % peers) for i in range(peers)]
        down = [(j, i) for i, j in up]
        last = lax.slice_in_dim(array, length - width, length, axis=dim)
        initial = lax.slice_in_dim(array, 0, width, axis=dim)
        before = lax.ppermute(last, axis, up)
        after = lax.ppermute(initial, axis, down)
        array = jnp.concatenate([before, array, after], axis=dim)
    return array


def matrix_apply(matrix, source):
    matrix_real = matrix[:, :, 0][None]
    matrix_imag = matrix[:, :, 1][None]
    source_real = source[:, None, :, 0]
    source_imag = source[:, None, :, 1]
    real_part = jnp.sum(matrix_real * source_real - matrix_imag * source_imag, axis=2)
    imag_part = jnp.sum(matrix_real * source_imag + matrix_imag * source_real, axis=2)
    return jnp.stack([real_part, imag_part], axis=2)


def adjoint(matrix):
    return jnp.stack(
        [jnp.swapaxes(matrix[:, :, 0], 0, 1), -jnp.swapaxes(matrix[:, :, 1], 0, 1)], axis=2
    )


def step_depth(values, offset):
    depth_index = lax.iota(jnp.int32, values.shape[-1]) % LZ
    if offset > 0:
        return jnp.where(
            depth_index == LZ - 1, jnp.roll(values, LZ - 1, -1), jnp.roll(values, -1, -1)
        )
    return jnp.where(depth_index == 0, jnp.roll(values, 1 - LZ, -1), jnp.roll(values, 1, -1))


def step_column(values, offset):
    plane = LY * LZ
    column_index = lax.iota(jnp.int32, values.shape[-1]) // LZ % LY
    if offset > 0:
        return jnp.where(
            column_index == LY - 1, jnp.roll(values, plane - LZ, -1), jnp.roll(values, -LZ, -1)
        )
    return jnp.where(column_index == 0, jnp.roll(values, LZ - plane, -1), jnp.roll(values, LZ, -1))


def laplace_step(center, ahead, behind, here_links, back_links):
    forward = matrix_apply(here_links[0], ahead)
    backward = matrix_apply(adjoint(back_links), behind)
    total = forward + backward
    for direction, stepper in ((1, step_column), (2, step_depth)):
        forward = matrix_apply(here_links[direction], stepper(center, 1))
        backward = matrix_apply(adjoint(stepper(here_links[direction], -1)), stepper(center, -1))
        total = total + (forward + backward)
    return center + KAPPA * (total - 6.0 * center)


def shards(vectors, gauge_links, momenta):
    plane = LY * LZ
    local_sites = vectors.shape[3]
    raw_low = vectors.astype(jnp.bfloat16)
    field = vectors
    x_links = gauge_links[0]
    rim = from_behind(x_links[..., local_sites - plane :], "brick", 1)
    back_links = jnp.concatenate([rim, x_links[..., : local_sites - plane]], axis=3)
    for step in range(ITERS):
        padded = padded_2(field, (("brick", 3),), plane)
        field = laplace_step(
            padded[..., plane : plane + local_sites],
            padded[..., 2 * plane :],
            padded[..., :local_sites],
            gauge_links,
            back_links,
        )
    smeared_low = field.astype(jnp.bfloat16)
    raw_sites, smeared_sites = (
        lax.all_to_all(raw_low, ("vec", "sub"), split_axis=3, concat_axis=0, tiled=True),
        lax.all_to_all(smeared_low, ("vec", "sub"), split_axis=3, concat_axis=0, tiled=True),
    )
    groups = lax.axis_size(("vec", "sub"))
    total_vec = raw_sites.shape[0]
    width = raw_sites.shape[3]
    total_x = lax.axis_size("brick") * (local_sites // plane)
    first_site = lax.axis_index("brick") * local_sites + lax.axis_index(("vec", "sub")) * width
    site = first_site + lax.iota(jnp.int32, width)
    layer_index = (site // plane)[None]
    column_index = (site // LZ % LY)[None]
    depth_index = (site % LZ)[None]
    fraction = (
        jnp.mod(momenta[:, 0:1] * layer_index, total_x).astype(jnp.float32) / total_x
        + jnp.mod(momenta[:, 1:2] * column_index, LY).astype(jnp.float32) / LY
        + jnp.mod(momenta[:, 2:3] * depth_index, LZ).astype(jnp.float32) / LZ
    )
    angle = 2.0 * math.pi * fraction
    cosines = jnp.cos(angle)
    sines = jnp.sin(angle)
    right = smeared_sites.reshape((total_vec, 6 * width))
    scale = (3.0 * total_x * plane) ** (-0.5)

    def one_momentum(angles):
        cosine, sine = angles
        real_part = raw_sites[:, :, 0] * cosine - raw_sites[:, :, 1] * sine
        imag_part = raw_sites[:, :, 0] * sine + raw_sites[:, :, 1] * cosine
        phased = jnp.stack([real_part, imag_part], axis=2).astype(jnp.bfloat16)
        turned = jnp.stack([-phased[:, :, 1], phased[:, :, 0]], axis=2)
        left = jnp.concatenate(
            [
                phased.reshape((lax.axis_size(("vec", "sub")) * (total_vec // groups), 6 * width)),
                turned.reshape((lax.axis_size(("vec", "sub")) * (total_vec // groups), 6 * width)),
            ],
            axis=0,
        )
        product = lax.dot_general(
            left, right, (((1,), (1,)), ((), ())), preferred_element_type=jnp.float32
        )
        return product.reshape(
            (2, lax.axis_size(("vec", "sub")) * (total_vec // groups), total_vec)
        )

    blocks = lax.map(one_momentum, (cosines, sines))
    shares = lax.psum_scatter(
        jnp.transpose(blocks, (2, 0, 1, 3)) * scale, ("vec", "sub"), scatter_dimension=0, tiled=True
    )
    return lax.psum_scatter(shares, "brick", scatter_dimension=3, tiled=True)


def fused_kernel(plan, momenta_ref, v_ref, g_ref, out_ref, *scratch):
    (mom_ref, mom_sem, vst, gst, field0, field1, table, moved0, moved1, right, smeared, left0, left1, cosb, sinb, total, parted,
     crossing, rx, halo, hsend, lsend, lrecv, load_sem, halo_sem, link_sem, raw_sem, cross_sem, last_sem) = scratch
    planes, rows, count, bricks, ships, width, scale = plan
    fields, moved = (field0, field1), (moved0, moved1)
    halves = rows // 16
    plane = LY * LZ
    tiles = plane // 128
    all_tiles = planes * tiles
    f32, low = jnp.float32, jnp.bfloat16
    wide = 2 * plane
    last = planes - 1
    inner = list(range(1, last))
    outer = [0, last]
    position = {t: i for i, t in enumerate(inner + outer)}
    cut = len(inner) * 3 * wide
    span = planes * 3 * wide
    b, v, s = (lax.axis_index(a) for a in ("brick", "vec", "sub"))
    left = (left0, left1)

    def remote(src, dst, sems, **ids):
        return pltpu.make_async_remote_copy(
            src_ref=src, dst_ref=dst, send_sem=sems.at[0], recv_sem=sems.at[1],
            device_id=ids, device_id_type=pl.DeviceIdType.MESH,
        )

    loads = {}
    for t in outer + inner:
        loads[t] = pltpu.make_async_copy(v_ref.at[:, t], vst.at[t], load_sem.at[t])
        loads[t].start()
    load_links = pltpu.make_async_copy(g_ref, gst.at[pl.ds(0, 54 * all_tiles)], load_sem.at[planes])
    load_links.start()
    load_momenta = pltpu.make_async_copy(momenta_ref, mom_ref, mom_sem)
    load_momenta.start()
    barrier = pltpu.get_barrier_semaphore()
    for db in range(bricks):
        for ds in range(2):
            if db or ds:
                pl.semaphore_signal(
                    barrier, inc=1, device_id={"brick": (b + db) % bricks, "sub": (s + ds) % 2},
                    device_id_type=pl.DeviceIdType.MESH,
                )
    pl.semaphore_signal(
        barrier, inc=1, device_id={"vec": 1 - v}, device_id_type=pl.DeviceIdType.MESH
    )

    def unpack(t):
        flat = vst.at[t].reshape(rows * 3 * tiles * 2, 128)
        step = 3 * tiles * 2
        for c in range(3):
            for first in range(0, rows, 16):
                for part in range(2):
                    for lane in range(0, tiles, 2):
                        at = part * plane + lane * 128
                        quad = []
                        for h in range(2):
                            start = (first + 8 * h) * step + c * tiles * 2 + lane * 2 + part
                            quad.append(
                                jnp.concatenate(
                                    [flat[pl.ds(start + 2 * i, 8, stride=step), :] for i in range(2)], axis=1
                                )
                            )
                            field0[t + 1, c, first + 8 * h : first + 8 * h + 8, at : at + 256] = quad[h]
                        k = (position[t] * 3 + c) * wide + at
                        right[first : first + 16, k : k + 256] = jnp.concatenate(quad, axis=0).astype(low)

    def link_rows(t, part, group):
        return jnp.concatenate(
            [
                gst[pl.ds(group * 16 * all_tiles + (t * tiles + lane) * 2 + part, 8, stride=2 * all_tiles), :]
                for lane in range(tiles)
            ],
            axis=1,
        ) * KAPPA

    for t in outer:
        loads[t].wait()
        unpack(t)
    load_links.wait()
    for part in range(2):
        both = jnp.concatenate([link_rows(last, part, 0), link_rows(last, part, 1)], axis=0)
        lsend[16 * part : 16 * part + 16, :] = both.astype(low)
    pl.semaphore_wait(barrier, 2 * bricks)
    up, down = (b + 1) % bricks, (b + bricks - 1) % bricks

    def halos(step, h, low_src, high_src):
        sems = halo_sem.at[step, h]
        return (
            remote(high_src, halo.at[step, h, 0], sems.at[0], brick=up),
            remote(low_src, halo.at[step, h, 1], sems.at[1], brick=down),
        )

    def own(t, h):
        at = position[t] * 3 * wide
        return right.at[16 * h : 16 * h + 16, at : at + 3 * wide]

    copies = {}
    links_up = remote(lsend, lrecv, link_sem, brick=up)
    for h in range(halves):
        copies[0, h] = halos(0, h, own(0, h), own(last, h))
        copies[1, h] = halos(1, h, hsend.at[h, 0], hsend.at[h, 1])
        for copy in copies[0, h]:
            copy.start()
        if h == 0:
            links_up.start()
    for t in inner:
        loads[t].wait()
        unpack(t)
    parts = [slice(0, cut)] + [
        slice(cut + i * 3 * wide, cut + (i + 1) * 3 * wide) for i in range(2)
    ]
    unit = 2 * rows

    def raw_copy(index, from_slot, to_slot, ks, **ids):
        return remote(
            right.at[from_slot * unit : from_slot * unit + rows, ks],
            right.at[to_slot * unit : to_slot * unit + rows, ks],
            raw_sem.at[index], **ids,
        )

    across = [raw_copy(i, 0, 2, parts[i], vec=1 - v) for i in range(3)]
    beside = raw_copy(6, 0, 1, slice(0, span), sub=1 - s)
    onward = [raw_copy(3 + i, 2, 3, parts[i], sub=1 - s) for i in range(3)]
    for copy in across + [beside]:
        copy.start()

    depth_wide = lax.broadcasted_iota(jnp.int32, (8, plane), 1) % LZ
    depth = lax.broadcasted_iota(jnp.int32, (8, 128), 1) % LZ

    def spread(t, carry):
        for part in range(2):
            for group in range(4):
                here = link_rows(t, part, group)
                if group > 0:
                    by = pltpu.roll(here, LZ, 1)
                    bz = jnp.where(
                        depth_wide == 0, pltpu.roll(here, plane - (LZ - 1), 1), pltpu.roll(here, 1, 1)
                    )
                for j in range(min(8, 27 - 8 * group)):
                    index = group * 8 + j
                    row = jnp.broadcast_to(here[j : j + 1], (8, plane))
                    table[t, index * 2 + part] = row
                    if index < 9:
                        table[t + 1, 54 + index * 2 + part] = row
                    else:
                        back = by if index < 18 else bz
                        table[t, 54 + index * 2 + part] = jnp.broadcast_to(back[j : j + 1], (8, plane))
        return carry

    lax.fori_loop(0, planes, spread, 0)

    places = []
    for group in range(0, all_tiles, 8):
        height = min(8, all_tiles - group)
        site = (
            lax.broadcasted_iota(jnp.int32, (height, 128), 0) * 128
            + lax.broadcasted_iota(jnp.int32, (height, 128), 1)
            + group * 128
        )
        places.append(
            (
                (site // plane + b * planes).astype(f32) * (1.0 / (bricks * planes)),
                (site // LZ % LY).astype(f32) * (1.0 / LY),
                (site % LZ).astype(f32) * (1.0 / LZ),
            )
        )

    def phases(q, carry):
        n = [mom_ref[d, jnp.minimum(q, count - 1)].astype(f32) for d in range(3)]
        for group, (x, y, z) in enumerate(places):
            turns = n[0] * x + n[1] * y + n[2] * z
            half = jnp.round(2.0 * turns)
            sign = 1.0 - 2.0 * jnp.abs(half - 2.0 * jnp.round(0.5 * half))
            angle = (2.0 * math.pi) * (turns - 0.5 * half)
            square = angle * angle
            cosine, sine = 0.0, 0.0
            for i in range(7, 0, -1):
                cosine = (cosine * square) + (-1.0) ** i / math.factorial(2 * i)
            cosine = sign * (1.0 + cosine * square)
            for i in range(6, 0, -1):
                sine = (sine * square) + (-1.0) ** i / math.factorial(2 * i + 1)
            sine = sign * (angle + angle * (sine * square))
            for j in range(x.shape[0]):
                at = (group * 8 + j) * 128
                cosb[q, :, at : at + 128] = jnp.broadcast_to(cosine[j : j + 1], (16, 128)).astype(low)
                sinb[q, :, at : at + 128] = jnp.broadcast_to(sine[j : j + 1], (16, 128)).astype(low)
        return carry

    load_momenta.wait()
    lax.fori_loop(0, count, phases, 0)

    def shift(stage, k, to):
        step, t, h = stage
        rows_to = pl.ds(pl.multiple_of(k % 2 * 8, 8), 8)
        rows_at = pl.ds(pl.multiple_of(h * 16 + k % 2 * 8, 8), 8)
        first_lane = k // 2 * plane
        lanes = pl.ds(pl.multiple_of(first_lane, plane), plane)
        for c in range(3):
            w = fields[step][t + 1, c, rows_at, lanes]
            to[0, c, rows_to, lanes] = pltpu.roll(w, plane - LZ, 1)
            to[1, c, rows_to, lanes] = pltpu.roll(w, LZ, 1)
            for part in range(tiles):
                u = w[:, part * 128 : part * 128 + 128]
                here = pl.ds(pl.multiple_of(first_lane + part * 128, 128), 128)
                to[2, c, rows_to, here] = jnp.where(
                    depth == LZ - 1, pltpu.roll(u, LZ - 1, 1), pltpu.roll(u, 127, 1)
                )
                to[3, c, rows_to, here] = jnp.where(
                    depth == 0, pltpu.roll(u, 128 - (LZ - 1), 1), pltpu.roll(u, 1, 1)
                )

    def block(stage, lane, now):
        step, t, half = stage
        field = fields[step]
        lanes = (
            pl.ds(pl.multiple_of(lane * 128, 128), 128),
            pl.ds(pl.multiple_of(plane + lane * 128, 128), 128),
        )
        at_rows = [slice(half * 16 + 8 * h, half * 16 + 8 * h + 8) for h in range(2)]
        acc = {}
        for h in range(2):
            for r in range(3):
                for part in range(2):
                    mid = field[t + 1, r, at_rows[h], lanes[part]]
                    acc[h, r, part] = (1.0 - 6.0 * KAPPA) * mid
        for way in range(6):
            direction, back = way // 2, way % 2
            for c in range(3):
                sources = []
                for h in range(2):
                    if direction == 0:
                        p = t + 2 - 2 * back
                        sources.append([field[p, c, at_rows[h], lanes[i]] for i in range(2)])
                    else:
                        sources.append([now[way - 2, c, 8 * h : 8 * h + 8, lanes[i]] for i in range(2)])
                for r in range(3):
                    row = direction * 18 + (54 + c * 6 + r * 2 if back else r * 6 + c * 2)
                    ur = table[t, row, :, lanes[0]]
                    ui = table[t, row + 1, :, lanes[0]]
                    for h, (sr, si) in enumerate(sources):
                        if back:
                            acc[h, r, 0] = acc[h, r, 0] + (ur * sr + ui * si)
                            acc[h, r, 1] = acc[h, r, 1] + (ur * si - ui * sr)
                        else:
                            acc[h, r, 0] = acc[h, r, 0] + (ur * sr - ui * si)
                            acc[h, r, 1] = acc[h, r, 1] + (ur * si + ui * sr)
        both = slice(half * 16, half * 16 + 16)
        for r in range(3):
            for part in range(2):
                if step == 0:
                    for h in range(2):
                        field1[t + 1, r, at_rows[h], lanes[part]] = acc[h, r, part]
                if step == 1 or t in outer:
                    pair = jnp.concatenate([acc[0, r, part], acc[1, r, part]], axis=0).astype(low)
                    if step == 1:
                        smeared[position[t] * 3 + r, both, lanes[part]] = pair
                    else:
                        k_at = pl.ds(pl.multiple_of((2 * r + part) * plane + lane * 128, 128), 128)
                        hsend[half, outer.index(t), :, k_at] = pair

    stages = [(0, t, h) for h in range(halves) for t in inner]
    for h in range(halves):
        stages += [(0, t, h) for t in outer] + [(1, t, h) for t in inner]
    stages += [(1, t, h) for h in range(halves) for t in outer]

    def run(step, ts, h):
        for t in ts:
            i = stages.index((step, t, h))

            def trip(k, carry):
                shift(stages[(i + 1) % len(stages)], k, moved[(i + 1) % 2])
                block(stages[i], k, moved[i % 2])
                return carry

            lax.fori_loop(0, tiles, trip, 0)

    def begin(k, carry):
        shift(stages[0], k, moved[0])
        return carry

    lax.fori_loop(0, tiles, begin, 0)
    for h in range(halves):
        run(0, inner, h)

    def take(step, h, side):
        copies[step, h][side].wait_recv()
        for c in range(3):
            fields[step][planes + 1 if side else 0, c, 16 * h : 16 * h + 16] = (
                halo[step, h, side, :, c * wide : (c + 1) * wide].astype(f32)
            )

    links_up.wait_recv()
    for part in range(2):
        got = lrecv[16 * part : 16 * part + 16, :].astype(f32)
        for index in range(9):
            table[0, 54 + index * 2 + part] = jnp.broadcast_to(got[index : index + 1], (8, plane))
    for h in range(halves):
        for side in range(2):
            take(0, h, side)
            run(0, [outer[side]], h)
            copies[1, h][1 - side].start()
        if h == halves - 1:
            across[0].wait_recv()
            onward[0].start()
        run(1, inner, h)
    beside.wait_recv()
    onward[0].wait_recv()

    def fill(k, carry):
        re = pl.ds(pl.multiple_of(k * wide, wide), plane)
        im = pl.ds(pl.multiple_of(k * wide + plane, plane), plane)
        for slot in range(4):
            at_raw = slice(slot * unit, slot * unit + rows)
            at_turned = slice(slot * unit + rows, (slot + 1) * unit)
            right[at_turned, re] = -right[at_raw, im]
            right[at_turned, im] = right[at_raw, re]
        return carry

    members = (inner, outer)
    streamed = 16 * count
    per_half, used, spare, sizes = pieces_of(count, halves, ships, width)
    order = [(h, half, t) for half in range(2) for h in range(halves) for t in members[half]]
    per = width // 16

    def ready(i):
        return order[i][1] == 0 or order[i][2] != outer[0]

    def turn(i):
        h, half, t = order[i]
        to = left[i % 2]
        for q in range(count):
            for lane in range(0, plane, 256):
                cosine = cosb[q, :, t * plane + lane : t * plane + lane + 256]
                sine = sinb[q, :, t * plane + lane : t * plane + lane + 256]
                for c in range(3):
                    k = position[t] * 3 + c
                    sr = smeared[k, 16 * h : 16 * h + 16, lane : lane + 256]
                    si = smeared[k, 16 * h : 16 * h + 16, plane + lane : plane + lane + 256]
                    col = c * wide + lane
                    to[16 * q : 16 * q + 16, col : col + 256] = cosine * sr + sine * si
                    to[16 * q : 16 * q + 16, col + plane : col + plane + 256] = cosine * si - sine * sr

    def product(i):
        h, half, t = order[i]
        first = position[t] * 3 * wide
        length = 3 * wide
        pieces = []
        for k in range(0, length, length // 2):
            pieces.append(
                lax.dot_general(
                    left[i % 2][:, k : k + length // 2],
                    right[:, first + k : first + k + length // 2],
                    (((1,), (1,)), ((), ())), preferred_element_type=f32,
                )
            )
        if i + 1 < len(order) and ready(i + 1):
            turn(i + 1)
        part = pieces[0] * scale + pieces[1] * scale
        if t == inner[0]:
            total[h, 0:streamed] = part
        else:
            total[h, 0:streamed] += part

    def finish(e):
        at = e % per_half * width
        part = total[e // per_half, at : at + sizes[e], :].T.astype(low)
        parted[e, 0, :, 0 : sizes[e]] = part[0 : 2 * unit]
        crossing[e, :, 0 : sizes[e]] = part[2 * unit :]

    roots = (v * 2 + s, (1 - v) * 2 + s)

    def cross(e):
        return remote(
            crossing.at[e, :, 0 : sizes[e]], parted.at[e, 1, :, 0 : sizes[e]], cross_sem.at[e], vec=1 - v
        )

    def ends(e, hop, ds):
        src = parted.at[e, hop, ds * unit : (ds + 1) * unit, 0 : sizes[e]]
        return src, rx.at[e, b, :, 0 : sizes[e]]

    def far(e, hop, ds):
        src, dst = ends(e, hop, ds)
        return pltpu.make_async_remote_copy(
            src_ref=src, dst_ref=dst,
            send_sem=last_sem.at[e, bricks + hop * 2 + ds], recv_sem=last_sem.at[e, b],
            device_id={"brick": roots[hop], "sub": (s + ds) % 2}, device_id_type=pl.DeviceIdType.MESH,
        )

    def depart(e, hop):
        far(e, hop, 1).start()

        @pl.when(roots[hop] != b)
        def _():
            far(e, hop, 0).start()

        @pl.when(roots[hop] == b)
        def _():
            src, dst = ends(e, hop, 0)
            pltpu.make_async_copy(src, dst, last_sem.at[e, b]).start()

    def ship(e):
        finish(e)
        cross(e).start()
        depart(e, 0)

    def hand_on(e):
        cross(e).wait_recv()
        depart(e, 1)

    def arrive(e):
        for i in range(bricks):
            dst = rx.at[e, i, :, 0 : sizes[e]]
            pltpu.make_async_copy(dst, dst, last_sem.at[e, i]).wait()

    def fill_half(half):
        first = len(inner) * 3 if half else 0
        count_k = len(members[half]) * 3
        lax.fori_loop(first, first + count_k, fill, 0)

    for i, (h, half, t) in enumerate(order):
        opens = t == members[half][0]
        if i == 0:
            fill_half(0)
        if half and opens:
            for side in range(2):
                if h == 0:
                    across[1 + side].wait_recv()
                    onward[1 + side].start()
                take(1, h, side)
                run(1, [outer[side]], h)
            if h:
                for e in range(per_half * (h - 1), per_half * h):
                    hand_on(e)
        if i == 0 or not ready(i):
            turn(i)
        if half and opens and h == 0:
            for part in (1, 2):
                onward[part].wait_recv()
            fill_half(1)
        product(i)
        if half and not opens:
            if h == halves - 1:
                total[h, streamed : streamed + 16 * spare] = total[0, 16 * (count - spare) : streamed]
            for e in range(per_half * h, per_half * (h + 1)):
                ship(e)
    for e in range(per_half * (halves - 1), ships):
        hand_on(e)
    for e in [i * per_half + j for j in range(per_half) for i in range(halves)]:
        arrive(e)
        got = [rx[e, i, :, 0 : sizes[e]].astype(f32) for i in range(bricks)]
        out_ref[:, e * width : e * width + sizes[e]] = (got[0] + got[1]) + (got[2] + got[3])
    sent = [links_up, *across, beside, *onward]
    for copy in copies.values():
        sent += copy
    sent += [cross(e) for e in range(ships)]
    for copy in sent:
        copy.wait_send()
    for e in range(ships):
        for hop in range(2):
            far(e, hop, 1).wait_send()

            @pl.when(roots[hop] != b)
            def _():
                far(e, hop, 0).wait_send()


def pieces_of(count, halves, ships, width):
    per_half = ships // halves
    used = 16 * count - (per_half - 1) * width
    spare = used % 128 // 16
    if used + 16 * spare > width:
        spare = 0
    sizes = [width] * ships
    if spare and used - 16 * spare:
        sizes[per_half - 1] = used - 16 * spare
    return per_half, used, spare, sizes


def rows_kernel(plan, sums_ref, out_ref, stage, sems):
    rows, count, ships, width = plan
    halves, per = rows // 16, width // 16
    per_half, used, spare, _ = pieces_of(count, halves, ships, width)
    lane_at = lax.broadcasted_iota(jnp.int32, (8, 128), 1)
    copies = []
    for octet in range(0, rows, 8):
        for q in range(count):
            for part in range(2):
                first = part * rows + octet
                pieces = []
                for h in range(halves):
                    e, at = h * per_half + q // per, q % per * 16
                    if h == 0 and q >= count - spare:
                        e, at = ships - 1, used + 16 * (q - count + spare)
                    tile = e * width + at // 128 * 128
                    got = sums_ref[first : first + 8, tile : tile + 128]
                    turned = (16 * h - at) % 128
                    pieces.append(pltpu.roll(got, turned, 1) if turned else got)
                value = jnp.where(lane_at < 16, pieces[0], pieces[1])
                start = octet * 2 * count + 2 * q + part
                stage[pl.ds(start, 8, stride=2 * count), :] = value[:, 0:rows]
        done = pl.ds(octet * 2 * count, 16 * count)
        copies.append(pltpu.make_async_copy(stage.at[done], out_ref.at[done], sems.at[octet // 8]))
        copies[-1].start()
    for copy in copies:
        copy.wait()


def shards_fused(vectors, gauge_links, momenta):
    plane = LY * LZ
    rows, local_sites = vectors.shape[0], vectors.shape[3]
    planes = local_sites // plane
    tiles = plane // 128
    bricks = lax.axis_size("brick")
    count = momenta.shape[0]
    halves = rows // 16
    width = 256
    per_half = -(-count * 16 // width)
    ships = halves * per_half
    low, f32 = jnp.bfloat16, jnp.float32
    v = vectors.reshape((rows, 3, 2, planes * tiles, 128)).transpose((0, 1, 3, 2, 4))
    v = v.reshape((rows * 3, planes, tiles * 2, 128))
    g = gauge_links.reshape((27, 2, planes * tiles, 128)).transpose((0, 2, 1, 3))
    g = g.reshape((54 * planes * tiles, 128))
    wide = 2 * plane
    scale = (3.0 * bricks * local_sites) ** (-0.5)
    vmem, dma = pltpu.VMEM, pltpu.SemaphoreType.DMA
    plan = (planes, rows, count, bricks, ships, width, scale)
    out = pl.pallas_call(
        functools.partial(fused_kernel, plan),
        out_shape=jax.ShapeDtypeStruct((2 * rows, ships * width), f32),
        in_specs=[
            pl.BlockSpec(memory_space=pl.ANY),
            pl.BlockSpec(memory_space=pl.ANY),
            pl.BlockSpec(memory_space=pl.ANY),
        ],
        out_specs=pl.BlockSpec(memory_space=pltpu.VMEM),
        scratch_shapes=[
            pltpu.SMEM((3, count), jnp.int32),
            dma,
            vmem((planes, rows * 3, tiles * 2, 128), f32),
            vmem((64 * planes * tiles, 128), f32),
            vmem((planes + 2, 3, rows, wide), f32),
            vmem((planes + 2, 3, rows, wide), f32),
            vmem((planes + 1, 108, 8, plane), f32),
            vmem((4, 3, 16, wide), f32),
            vmem((4, 3, 16, wide), f32),
            vmem((8 * rows, planes * 3 * wide), low),
            vmem((planes * 3, rows, wide), low),
            vmem((16 * count, 3 * wide), low),
            vmem((16 * count, 3 * wide), low),
            vmem((count, 16, local_sites), low),
            vmem((count, 16, local_sites), low),
            vmem((halves, per_half * width, 8 * rows), f32),
            vmem((ships, 2, 4 * rows, width), low),
            vmem((ships, 4 * rows, width), low),
            vmem((ships, bricks, 2 * rows, width), low),
            vmem((2, halves, 2, 16, 3 * wide), low),
            vmem((halves, 2, 16, 3 * wide), low),
            vmem((32, plane), low),
            vmem((32, plane), low),
            dma((planes + 1,)),
            dma((2, halves, 2, 2)),
            dma((2,)),
            dma((7, 2)),
            dma((ships, 2)),
            dma((ships, bricks + 4)),
        ],
        compiler_params=pltpu.CompilerParams(
            vmem_limit_bytes=60 * 2**20, collective_id=0, has_side_effects=True
        ),
        name="elementals",
    )(momenta.T, v, g)
    out = pl.pallas_call(
        functools.partial(rows_kernel, (rows, count, ships, width)),
        out_shape=jax.ShapeDtypeStruct((rows * count * 2, rows), f32),
        in_specs=[pl.BlockSpec(memory_space=pltpu.VMEM)],
        out_specs=pl.BlockSpec(memory_space=pl.ANY),
        scratch_shapes=[vmem((rows * count * 2, rows), f32), dma((rows // 8,))],
        name="rows",
    )(out)
    return out.reshape((rows, count, 2, rows))


def choose(vectors, gauge_links, momenta):
    plane = LY * LZ
    bricks, vecs, subs = (lax.axis_size(a) for a in ("brick", "vec", "sub"))
    rows, local_sites = vectors.shape[0], vectors.shape[3]
    fits = local_sites % plane == 0 and local_sites // plane == 4 and rows == 32
    if fits and vecs == 2 and subs == 2 and bricks == 4 and 24 <= momenta.shape[0] < 32:
        return shards_fused(vectors, gauge_links, momenta)
    return shards(vectors, gauge_links, momenta)


def solution(mesh):
    in_specs = (
        P(("vec", "sub"), None, None, ("grp", "brick")),
        P(None, None, None, None, ("grp", "brick")),
        P(),
    )
    out_specs = P(("vec", "sub"), "grp", None, "brick")
    return jax.shard_map(choose, mesh=mesh, in_specs=in_specs, out_specs=out_specs, check_vma=False)
```

```python
import functools
import math

import jax
import jax.numpy as jnp
from jax import lax
from jax.experimental import pallas as pl
from jax.experimental.pallas import tpu as pltpu
from jax.sharding import PartitionSpec as P

LY = 64
LZ = 8
ITERS = 2


KAPPA = 0.125


def from_behind(array, axis, by):
    peers = lax.axis_size(axis)
    return lax.ppermute(array, axis, [(i, (i + by) % peers) for i in range(peers)])


def padded_2(array, sides, width):
    for axis, dim in sides:
        peers, length = (lax.axis_size(axis), array.shape[dim])
        up = [(i, (i + 1) % peers) for i in range(peers)]
        down = [(j, i) for i, j in up]
        last = lax.slice_in_dim(array, length - width, length, axis=dim)
        initial = lax.slice_in_dim(array, 0, width, axis=dim)
        before = lax.ppermute(last, axis, up)
        after = lax.ppermute(initial, axis, down)
        array = jnp.concatenate([before, array, after], axis=dim)
    return array


def matrix_apply(matrix, source):
    matrix_real = matrix[:, :, 0][None]
    matrix_imag = matrix[:, :, 1][None]
    source_real = source[:, None, :, 0]
    source_imag = source[:, None, :, 1]
    real_part = jnp.sum(matrix_real * source_real - matrix_imag * source_imag, axis=2)
    imag_part = jnp.sum(matrix_real * source_imag + matrix_imag * source_real, axis=2)
    return jnp.stack([real_part, imag_part], axis=2)


def adjoint(matrix):
    return jnp.stack(
        [jnp.swapaxes(matrix[:, :, 0], 0, 1), -jnp.swapaxes(matrix[:, :, 1], 0, 1)], axis=2
    )


def step_depth(values, offset):
    depth_index = lax.iota(jnp.int32, values.shape[-1]) % LZ
    if offset > 0:
        return jnp.where(
            depth_index == LZ - 1, jnp.roll(values, LZ - 1, -1), jnp.roll(values, -1, -1)
        )
    return jnp.where(depth_index == 0, jnp.roll(values, 1 - LZ, -1), jnp.roll(values, 1, -1))


def step_column(values, offset):
    plane = LY * LZ
    column_index = lax.iota(jnp.int32, values.shape[-1]) // LZ % LY
    if offset > 0:
        return jnp.where(
            column_index == LY - 1, jnp.roll(values, plane - LZ, -1), jnp.roll(values, -LZ, -1)
        )
    return jnp.where(column_index == 0, jnp.roll(values, LZ - plane, -1), jnp.roll(values, LZ, -1))


def laplace_step(center, ahead, behind, here_links, back_links):
    forward = matrix_apply(here_links[0], ahead)
    backward = matrix_apply(adjoint(back_links), behind)
    total = forward + backward
    for direction, stepper in ((1, step_column), (2, step_depth)):
        forward = matrix_apply(here_links[direction], stepper(center, 1))
        backward = matrix_apply(adjoint(stepper(here_links[direction], -1)), stepper(center, -1))
        total = total + (forward + backward)
    return center + KAPPA * (total - 6.0 * center)


def shards(vectors, gauge_links, momenta):
    plane = LY * LZ
    local_sites = vectors.shape[3]
    raw_low = vectors.astype(jnp.bfloat16)
    field = vectors
    x_links = gauge_links[0]
    rim = from_behind(x_links[..., local_sites - plane :], "brick", 1)
    back_links = jnp.concatenate([rim, x_links[..., : local_sites - plane]], axis=3)
    for step in range(ITERS):
        padded = padded_2(field, (("brick", 3),), plane)
        field = laplace_step(
            padded[..., plane : plane + local_sites],
            padded[..., 2 * plane :],
            padded[..., :local_sites],
            gauge_links,
            back_links,
        )
    smeared_low = field.astype(jnp.bfloat16)
    raw_sites, smeared_sites = (
        lax.all_to_all(raw_low, ("vec", "sub"), split_axis=3, concat_axis=0, tiled=True),
        lax.all_to_all(smeared_low, ("vec", "sub"), split_axis=3, concat_axis=0, tiled=True),
    )
    groups = lax.axis_size(("vec", "sub"))
    total_vec = raw_sites.shape[0]
    width = raw_sites.shape[3]
    total_x = lax.axis_size("brick") * (local_sites // plane)
    first_site = lax.axis_index("brick") * local_sites + lax.axis_index(("vec", "sub")) * width
    site = first_site + lax.iota(jnp.int32, width)
    layer_index = (site // plane)[None]
    column_index = (site // LZ % LY)[None]
    depth_index = (site % LZ)[None]
    fraction = (
        jnp.mod(momenta[:, 0:1] * layer_index, total_x).astype(jnp.float32) / total_x
        + jnp.mod(momenta[:, 1:2] * column_index, LY).astype(jnp.float32) / LY
        + jnp.mod(momenta[:, 2:3] * depth_index, LZ).astype(jnp.float32) / LZ
    )
    angle = 2.0 * math.pi * fraction
    cosines = jnp.cos(angle)
    sines = jnp.sin(angle)
    right = smeared_sites.reshape((total_vec, 6 * width))
    scale = (3.0 * total_x * plane) ** (-0.5)

    def one_momentum(angles):
        cosine, sine = angles
        real_part = raw_sites[:, :, 0] * cosine - raw_sites[:, :, 1] * sine
        imag_part = raw_sites[:, :, 0] * sine + raw_sites[:, :, 1] * cosine
        phased = jnp.stack([real_part, imag_part], axis=2).astype(jnp.bfloat16)
        turned = jnp.stack([-phased[:, :, 1], phased[:, :, 0]], axis=2)
        left = jnp.concatenate(
            [
                phased.reshape((lax.axis_size(("vec", "sub")) * (total_vec // groups), 6 * width)),
                turned.reshape((lax.axis_size(("vec", "sub")) * (total_vec // groups), 6 * width)),
            ],
            axis=0,
        )
        product = lax.dot_general(
            left, right, (((1,), (1,)), ((), ())), preferred_element_type=jnp.float32
        )
        return product.reshape(
            (2, lax.axis_size(("vec", "sub")) * (total_vec // groups), total_vec)
        )

    blocks = lax.map(one_momentum, (cosines, sines))
    shares = lax.psum_scatter(
        jnp.transpose(blocks, (2, 0, 1, 3)) * scale, ("vec", "sub"), scatter_dimension=0, tiled=True
    )
    return lax.psum_scatter(shares, "brick", scatter_dimension=3, tiled=True)


def fused_kernel(plan, momenta_ref, v_ref, g_ref, out_ref, *scratch):
    (mom_ref, mom_sem, vst, gst, field0, field1, table, moved0, moved1, right, smeared, left0, left1, cosb, sinb, total, parted,
     crossing, inward, rx, halo, hsend, lsend, lrecv, load_sem, halo_sem, link_sem, raw_sem, cross_sem, inward_sem, last_sem) = scratch
    planes, rows, count, bricks, ships, width, scale = plan
    fields, moved = (field0, field1), (moved0, moved1)
    halves = rows // 16
    plane = LY * LZ
    tiles = plane // 128
    all_tiles = planes * tiles
    f32, low = jnp.float32, jnp.bfloat16
    wide = 2 * plane
    last = planes - 1
    inner = list(range(1, last))
    outer = [0, last]
    position = {t: i for i, t in enumerate(inner + outer)}
    cut = len(inner) * 3 * wide
    span = planes * 3 * wide
    b, v, s = (lax.axis_index(a) for a in ("brick", "vec", "sub"))
    left = (left0, left1)

    def remote(src, dst, sems, **ids):
        return pltpu.make_async_remote_copy(
            src_ref=src, dst_ref=dst, send_sem=sems.at[0], recv_sem=sems.at[1],
            device_id=ids, device_id_type=pl.DeviceIdType.MESH,
        )

    loads = {}
    for t in outer + inner:
        loads[t] = pltpu.make_async_copy(v_ref.at[:, t], vst.at[t], load_sem.at[t])
        loads[t].start()
    load_links = pltpu.make_async_copy(g_ref, gst.at[pl.ds(0, 54 * all_tiles)], load_sem.at[planes])
    load_links.start()
    load_momenta = pltpu.make_async_copy(momenta_ref, mom_ref, mom_sem)
    load_momenta.start()
    barrier = pltpu.get_barrier_semaphore()
    for db in range(bricks):
        for ds in range(2):
            if db or ds:
                pl.semaphore_signal(
                    barrier, inc=1, device_id={"brick": (b + db) % bricks, "sub": (s + ds) % 2},
                    device_id_type=pl.DeviceIdType.MESH,
                )
    pl.semaphore_signal(
        barrier, inc=1, device_id={"vec": 1 - v}, device_id_type=pl.DeviceIdType.MESH
    )
    outermost, adder = b == 3 - 3 * v, b == 1 + v
    pl.when(outermost)(
        lambda: pl.semaphore_signal(
            barrier, inc=1, device_id={"brick": 2 - v, "vec": 1 - v}, device_id_type=pl.DeviceIdType.MESH
        )
    )
    pl.when(adder)(
        lambda: pl.semaphore_signal(
            barrier, inc=1, device_id={"brick": 3 * v, "vec": 1 - v}, device_id_type=pl.DeviceIdType.MESH
        )
    )
    silent = 3 * v

    @pl.when(b // 2 != v)
    def _():
        for e in range(ships):
            rx[e, silent] = jnp.zeros(rx.shape[2:], low)


    def unpack(t):
        flat = vst.at[t].reshape(rows * 3 * tiles * 2, 128)
        step = 3 * tiles * 2
        for c in range(3):
            for first in range(0, rows, 16):
                for part in range(2):
                    for lane in range(0, tiles, 2):
                        at = part * plane + lane * 128
                        quad = []
                        for h in range(2):
                            start = (first + 8 * h) * step + c * tiles * 2 + lane * 2 + part
                            quad.append(
                                jnp.concatenate(
                                    [flat[pl.ds(start + 2 * i, 8, stride=step), :] for i in range(2)], axis=1
                                )
                            )
                            field0[t + 1, c, first + 8 * h : first + 8 * h + 8, at : at + 256] = quad[h]
                        k = (position[t] * 3 + c) * wide + at
                        right[first : first + 16, k : k + 256] = jnp.concatenate(quad, axis=0).astype(low)

    def link_rows(t, part, group):
        return jnp.concatenate(
            [
                gst[pl.ds(group * 16 * all_tiles + (t * tiles + lane) * 2 + part, 8, stride=2 * all_tiles), :]
                for lane in range(tiles)
            ],
            axis=1,
        ) * KAPPA

    for t in outer:
        loads[t].wait()
        unpack(t)
    load_links.wait()
    for part in range(2):
        both = jnp.concatenate([link_rows(last, part, 0), link_rows(last, part, 1)], axis=0)
        lsend[16 * part : 16 * part + 16, :] = both.astype(low)
    extra = (outermost | adder).astype(jnp.int32)
    pl.semaphore_wait(barrier, 2 * bricks + extra)
    up, down = (b + 1) % bricks, (b + bricks - 1) % bricks

    def halos(step, h, low_src, high_src):
        sems = halo_sem.at[step, h]
        return (
            remote(high_src, halo.at[step, h, 0], sems.at[0], brick=up),
            remote(low_src, halo.at[step, h, 1], sems.at[1], brick=down),
        )

    def own(t, h):
        at = position[t] * 3 * wide
        return right.at[16 * h : 16 * h + 16, at : at + 3 * wide]

    copies = {}
    links_up = remote(lsend, lrecv, link_sem, brick=up)
    for h in range(halves):
        copies[0, h] = halos(0, h, own(0, h), own(last, h))
        copies[1, h] = halos(1, h, hsend.at[h, 0], hsend.at[h, 1])
        for copy in copies[0, h]:
            copy.start()
        if h == 0:
            links_up.start()
    for t in inner:
        loads[t].wait()
        unpack(t)
    parts = [slice(0, cut)] + [
        slice(cut + i * 3 * wide, cut + (i + 1) * 3 * wide) for i in range(2)
    ]
    unit = 2 * rows

    def raw_copy(index, from_slot, to_slot, ks, **ids):
        return remote(
            right.at[from_slot * unit : from_slot * unit + rows, ks],
            right.at[to_slot * unit : to_slot * unit + rows, ks],
            raw_sem.at[index], **ids,
        )

    across = [raw_copy(i, 0, 2, parts[i], vec=1 - v) for i in range(3)]
    beside = raw_copy(6, 0, 1, slice(0, span), sub=1 - s)
    onward = [raw_copy(3 + i, 2, 3, parts[i], sub=1 - s) for i in range(3)]
    for copy in across + [beside]:
        copy.start()

    depth_wide = lax.broadcasted_iota(jnp.int32, (8, plane), 1) % LZ
    depth = lax.broadcasted_iota(jnp.int32, (8, 128), 1) % LZ

    def spread(t, carry):
        for part in range(2):
            for group in range(4):
                here = link_rows(t, part, group)
                if group > 0:
                    by = pltpu.roll(here, LZ, 1)
                    bz = jnp.where(
                        depth_wide == 0, pltpu.roll(here, plane - (LZ - 1), 1), pltpu.roll(here, 1, 1)
                    )
                for j in range(min(8, 27 - 8 * group)):
                    index = group * 8 + j
                    row = jnp.broadcast_to(here[j : j + 1], (8, plane))
                    table[t, index * 2 + part] = row
                    if index < 9:
                        table[t + 1, 54 + index * 2 + part] = row
                    else:
                        back = by if index < 18 else bz
                        table[t, 54 + index * 2 + part] = jnp.broadcast_to(back[j : j + 1], (8, plane))
        return carry

    lax.fori_loop(0, planes, spread, 0)

    places = []
    for group in range(0, all_tiles, 8):
        height = min(8, all_tiles - group)
        site = (
            lax.broadcasted_iota(jnp.int32, (height, 128), 0) * 128
            + lax.broadcasted_iota(jnp.int32, (height, 128), 1)
            + group * 128
        )
        places.append(
            (
                (site // plane + b * planes).astype(f32) * (1.0 / (bricks * planes)),
                (site // LZ % LY).astype(f32) * (1.0 / LY),
                (site % LZ).astype(f32) * (1.0 / LZ),
            )
        )

    def phases(q, carry):
        n = [mom_ref[d, jnp.minimum(q, count - 1)].astype(f32) for d in range(3)]
        for group, (x, y, z) in enumerate(places):
            turns = n[0] * x + n[1] * y + n[2] * z
            half = jnp.round(2.0 * turns)
            sign = 1.0 - 2.0 * jnp.abs(half - 2.0 * jnp.round(0.5 * half))
            angle = (2.0 * math.pi) * (turns - 0.5 * half)
            square = angle * angle
            cosine, sine = 0.0, 0.0
            for i in range(7, 0, -1):
                cosine = (cosine * square) + (-1.0) ** i / math.factorial(2 * i)
            cosine = sign * (1.0 + cosine * square)
            for i in range(6, 0, -1):
                sine = (sine * square) + (-1.0) ** i / math.factorial(2 * i + 1)
            sine = sign * (angle + angle * (sine * square))
            for j in range(x.shape[0]):
                at = (group * 8 + j) * 128
                cosb[q, :, at : at + 128] = jnp.broadcast_to(cosine[j : j + 1], (16, 128)).astype(low)
                sinb[q, :, at : at + 128] = jnp.broadcast_to(sine[j : j + 1], (16, 128)).astype(low)
        return carry

    load_momenta.wait()
    lax.fori_loop(0, count, phases, 0)

    def shift(stage, k, to):
        step, t, h = stage
        rows_to = pl.ds(pl.multiple_of(k % 2 * 8, 8), 8)
        rows_at = pl.ds(pl.multiple_of(h * 16 + k % 2 * 8, 8), 8)
        first_lane = k // 2 * plane
        lanes = pl.ds(pl.multiple_of(first_lane, plane), plane)
        for c in range(3):
            w = fields[step][t + 1, c, rows_at, lanes]
            to[0, c, rows_to, lanes] = pltpu.roll(w, plane - LZ, 1)
            to[1, c, rows_to, lanes] = pltpu.roll(w, LZ, 1)
            for part in range(tiles):
                u = w[:, part * 128 : part * 128 + 128]
                here = pl.ds(pl.multiple_of(first_lane + part * 128, 128), 128)
                to[2, c, rows_to, here] = jnp.where(
                    depth == LZ - 1, pltpu.roll(u, LZ - 1, 1), pltpu.roll(u, 127, 1)
                )
                to[3, c, rows_to, here] = jnp.where(
                    depth == 0, pltpu.roll(u, 128 - (LZ - 1), 1), pltpu.roll(u, 1, 1)
                )

    def block(stage, lane, now):
        step, t, half = stage
        field = fields[step]
        lanes = (
            pl.ds(pl.multiple_of(lane * 128, 128), 128),
            pl.ds(pl.multiple_of(plane + lane * 128, 128), 128),
        )
        at_rows = [slice(half * 16 + 8 * h, half * 16 + 8 * h + 8) for h in range(2)]
        acc = {}
        for h in range(2):
            for r in range(3):
                for part in range(2):
                    mid = field[t + 1, r, at_rows[h], lanes[part]]
                    acc[h, r, part] = (1.0 - 6.0 * KAPPA) * mid
        for way in range(6):
            direction, back = way // 2, way % 2
            for c in range(3):
                sources = []
                for h in range(2):
                    if direction == 0:
                        p = t + 2 - 2 * back
                        sources.append([field[p, c, at_rows[h], lanes[i]] for i in range(2)])
                    else:
                        sources.append([now[way - 2, c, 8 * h : 8 * h + 8, lanes[i]] for i in range(2)])
                for r in range(3):
                    row = direction * 18 + (54 + c * 6 + r * 2 if back else r * 6 + c * 2)
                    ur = table[t, row, :, lanes[0]]
                    ui = table[t, row + 1, :, lanes[0]]
                    for h, (sr, si) in enumerate(sources):
                        if back:
                            acc[h, r, 0] = acc[h, r, 0] + (ur * sr + ui * si)
                            acc[h, r, 1] = acc[h, r, 1] + (ur * si - ui * sr)
                        else:
                            acc[h, r, 0] = acc[h, r, 0] + (ur * sr - ui * si)
                            acc[h, r, 1] = acc[h, r, 1] + (ur * si + ui * sr)
        both = slice(half * 16, half * 16 + 16)
        for r in range(3):
            for part in range(2):
                if step == 0:
                    for h in range(2):
                        field1[t + 1, r, at_rows[h], lanes[part]] = acc[h, r, part]
                if step == 1 or t in outer:
                    pair = jnp.concatenate([acc[0, r, part], acc[1, r, part]], axis=0).astype(low)
                    if step == 1:
                        smeared[position[t] * 3 + r, both, lanes[part]] = pair
                    else:
                        k_at = pl.ds(pl.multiple_of((2 * r + part) * plane + lane * 128, 128), 128)
                        hsend[half, outer.index(t), :, k_at] = pair

    stages = [(0, t, h) for h in range(halves) for t in inner]
    for h in range(halves):
        stages += [(0, t, h) for t in outer] + [(1, t, h) for t in inner]
    stages += [(1, t, h) for h in range(halves) for t in outer]

    def run(step, ts, h):
        for t in ts:
            i = stages.index((step, t, h))

            def trip(k, carry):
                shift(stages[(i + 1) % len(stages)], k, moved[(i + 1) % 2])
                block(stages[i], k, moved[i % 2])
                return carry

            lax.fori_loop(0, tiles, trip, 0)

    def begin(k, carry):
        shift(stages[0], k, moved[0])
        return carry

    lax.fori_loop(0, tiles, begin, 0)
    for h in range(halves):
        run(0, inner, h)

    def take(step, h, side):
        copies[step, h][side].wait_recv()
        for c in range(3):
            fields[step][planes + 1 if side else 0, c, 16 * h : 16 * h + 16] = (
                halo[step, h, side, :, c * wide : (c + 1) * wide].astype(f32)
            )

    links_up.wait_recv()
    for part in range(2):
        got = lrecv[16 * part : 16 * part + 16, :].astype(f32)
        for index in range(9):
            table[0, 54 + index * 2 + part] = jnp.broadcast_to(got[index : index + 1], (8, plane))
    for h in range(halves):
        for side in range(2):
            take(0, h, side)
            run(0, [outer[side]], h)
            copies[1, h][1 - side].start()
        if h == halves - 1:
            across[0].wait_recv()
            onward[0].start()
        run(1, inner, h)
    beside.wait_recv()
    onward[0].wait_recv()

    def fill(k, carry):
        re = pl.ds(pl.multiple_of(k * wide, wide), plane)
        im = pl.ds(pl.multiple_of(k * wide + plane, plane), plane)
        for slot in range(4):
            at_raw = slice(slot * unit, slot * unit + rows)
            at_turned = slice(slot * unit + rows, (slot + 1) * unit)
            right[at_turned, re] = -right[at_raw, im]
            right[at_turned, im] = right[at_raw, re]
        return carry

    members = (inner, outer)
    streamed = 16 * count
    per_half, used, spare, sizes = pieces_of(count, halves, ships, width)
    order = [(h, half, t) for half in range(2) for h in range(halves) for t in members[half]]
    per = width // 16

    def ready(i):
        return order[i][1] == 0 or order[i][2] != outer[0]

    def turn(i):
        h, half, t = order[i]
        to = left[i % 2]
        for q in range(count):
            for lane in range(0, plane, 256):
                cosine = cosb[q, :, t * plane + lane : t * plane + lane + 256]
                sine = sinb[q, :, t * plane + lane : t * plane + lane + 256]
                for c in range(3):
                    k = position[t] * 3 + c
                    sr = smeared[k, 16 * h : 16 * h + 16, lane : lane + 256]
                    si = smeared[k, 16 * h : 16 * h + 16, plane + lane : plane + lane + 256]
                    col = c * wide + lane
                    to[16 * q : 16 * q + 16, col : col + 256] = cosine * sr + sine * si
                    to[16 * q : 16 * q + 16, col + plane : col + plane + 256] = cosine * si - sine * sr

    def product(i):
        h, half, t = order[i]
        first = position[t] * 3 * wide
        length = 3 * wide
        pieces = []
        for k in range(0, length, length // 2):
            pieces.append(
                lax.dot_general(
                    left[i % 2][:, k : k + length // 2],
                    right[:, first + k : first + k + length // 2],
                    (((1,), (1,)), ((), ())), preferred_element_type=f32,
                )
            )
        if i + 1 < len(order) and ready(i + 1):
            turn(i + 1)
        part = pieces[0] * scale + pieces[1] * scale
        if t == inner[0]:
            total[h, 0:streamed] = part
        else:
            total[h, 0:streamed] += part

    def finish(e):
        at = e % per_half * width
        part = total[e // per_half, at : at + sizes[e], :].T.astype(low)
        parted[e, 0, :, 0 : sizes[e]] = part[0 : 2 * unit]
        crossing[e, :, 0 : sizes[e]] = part[2 * unit :]

    roots = (v * 2 + s, (1 - v) * 2 + s)

    def cross(e):
        return remote(
            crossing.at[e, :, 0 : sizes[e]], parted.at[e, 1, :, 0 : sizes[e]], cross_sem.at[e], vec=1 - v
        )

    def ends(e, hop, ds):
        src = parted.at[e, hop, ds * unit : (ds + 1) * unit, 0 : sizes[e]]
        return src, rx.at[e, b, :, 0 : sizes[e]]

    def far(e, hop, ds):
        src, dst = ends(e, hop, ds)
        return pltpu.make_async_remote_copy(
            src_ref=src, dst_ref=dst,
            send_sem=last_sem.at[e, bricks + hop * 2 + ds], recv_sem=last_sem.at[e, b],
            device_id={"brick": roots[hop], "sub": (s + ds) % 2}, device_id_type=pl.DeviceIdType.MESH,
        )

    def depart(e, hop):
        far(e, hop, 1).start()

        @pl.when(roots[hop] != b)
        def _():
            far(e, hop, 0).start()

        @pl.when(roots[hop] == b)
        def _():
            src, dst = ends(e, hop, 0)
            pltpu.make_async_copy(src, dst, last_sem.at[e, b]).start()

    def cross_inward(e):
        return remote(
            crossing.at[e, :, 0 : sizes[e]], inward.at[e, :, 0 : sizes[e]], inward_sem.at[e],
            vec=1 - v, brick=2 - v,
        )

    def ship(e):
        finish(e)

        @pl.when(outermost)
        def _():
            cross_inward(e).start()

        @pl.when(jnp.logical_not(outermost))
        def _():
            cross(e).start()

        depart(e, 0)

    def hand_on(e):
        @pl.when(adder)
        def _():
            cross(e).wait_recv()
            cross_inward(e).wait_recv()
            both = parted[e, 1, :, 0 : sizes[e]].astype(f32) + inward[e, :, 0 : sizes[e]].astype(f32)
            parted[e, 1, :, 0 : sizes[e]] = both.astype(low)
            depart(e, 1)

        @pl.when(jnp.logical_not(adder) & (b != silent))
        def _():
            cross(e).wait_recv()
            depart(e, 1)

    def arrive(e):
        for i in range(bricks):
            @pl.when((b // 2 == v) | (silent != i))
            def _():
                dst = rx.at[e, i, :, 0 : sizes[e]]
                pltpu.make_async_copy(dst, dst, last_sem.at[e, i]).wait()


    def fill_half(half):
        first = len(inner) * 3 if half else 0
        count_k = len(members[half]) * 3
        lax.fori_loop(first, first + count_k, fill, 0)

    for i, (h, half, t) in enumerate(order):
        opens = t == members[half][0]
        if i == 0:
            fill_half(0)
        if half and opens:
            if h == 0:
                for part in (1, 2):
                    across[part].wait_recv()
                    onward[part].start()
            for side in range(2):
                take(1, h, side)
                run(1, [outer[side]], h)
            if h == 0:
                for part in (1, 2):
                    onward[part].wait_recv()
                fill_half(1)
            else:
                for e in range(per_half * (h - 1), per_half * h):
                    hand_on(e)
        if i == 0 or not ready(i):
            turn(i)
        product(i)
        if half and not opens:
            if h == halves - 1:
                total[h, streamed : streamed + 16 * spare] = total[0, 16 * (count - spare) : streamed]
            for e in range(per_half * h, per_half * (h + 1)):
                ship(e)
    for e in range(per_half * (halves - 1), ships):
        hand_on(e)
    for e in [i * per_half + j for j in range(per_half) for i in range(halves)]:
        arrive(e)
        got = [rx[e, i, :, 0 : sizes[e]].astype(f32) for i in range(bricks)]
        out_ref[:, e * width : e * width + sizes[e]] = (got[0] + got[1]) + (got[2] + got[3])
    sent = [links_up, *across, beside, *onward]
    for copy in copies.values():
        sent += copy
    for copy in sent:
        copy.wait_send()
    for e in range(ships):
        @pl.when(outermost)
        def _():
            cross_inward(e).wait_send()

        @pl.when(jnp.logical_not(outermost))
        def _():
            cross(e).wait_send()

        for hop in range(2):
            @pl.when((b != silent) | (hop == 0))
            def _():
                far(e, hop, 1).wait_send()

                @pl.when(roots[hop] != b)
                def _():
                    far(e, hop, 0).wait_send()


def pieces_of(count, halves, ships, width):
    per_half = ships // halves
    used = 16 * count - (per_half - 1) * width
    spare = used % 128 // 16
    if used + 16 * spare > width:
        spare = 0
    sizes = [width] * ships
    if spare and used - 16 * spare:
        sizes[per_half - 1] = used - 16 * spare
    return per_half, used, spare, sizes


def rows_kernel(plan, sums_ref, out_ref):
    rows, count, ships, width = plan
    halves, unit = rows // 16, 2 * rows
    per = width // 16
    per_half, used, spare, _ = pieces_of(count, halves, ships, width)
    lane_at = lax.broadcasted_iota(jnp.int32, (8, 128), 1)
    for q in range(count):
        for first in range(0, unit, 8):
            pieces = []
            for h in range(halves):
                e, at = h * per_half + q // per, q % per * 16
                if h == 0 and q >= count - spare:
                    e, at = ships - 1, used + 16 * (q - count + spare)
                tile = e * width + at // 128 * 128
                got = sums_ref[first : first + 8, tile : tile + 128]
                turned = (16 * h - at) % 128
                pieces.append(pltpu.roll(got, turned, 1) if turned else got)
            value = jnp.where(lane_at < 16, pieces[0], pieces[1])
            start = (first % rows) * 2 * count + 2 * q + first // rows
            out_ref[pl.ds(start, 8, stride=2 * count), :] = value[:, 0:rows]


def shards_fused(vectors, gauge_links, momenta):
    plane = LY * LZ
    rows, local_sites = vectors.shape[0], vectors.shape[3]
    planes = local_sites // plane
    tiles = plane // 128
    bricks = lax.axis_size("brick")
    count = momenta.shape[0]
    halves = rows // 16
    width = 256
    per_half = -(-count * 16 // width)
    ships = halves * per_half
    low, f32 = jnp.bfloat16, jnp.float32
    v = vectors.reshape((rows, 3, 2, planes * tiles, 128)).transpose((0, 1, 3, 2, 4))
    v = v.reshape((rows * 3, planes, tiles * 2, 128))
    g = gauge_links.reshape((27, 2, planes * tiles, 128)).transpose((0, 2, 1, 3))
    g = g.reshape((54 * planes * tiles, 128))
    wide = 2 * plane
    scale = (3.0 * bricks * local_sites) ** (-0.5)
    vmem, dma = pltpu.VMEM, pltpu.SemaphoreType.DMA
    plan = (planes, rows, count, bricks, ships, width, scale)
    out = pl.pallas_call(
        functools.partial(fused_kernel, plan),
        out_shape=jax.ShapeDtypeStruct((2 * rows, ships * width), f32),
        in_specs=[
            pl.BlockSpec(memory_space=pl.ANY),
            pl.BlockSpec(memory_space=pl.ANY),
            pl.BlockSpec(memory_space=pl.ANY),
        ],
        out_specs=pl.BlockSpec(memory_space=pltpu.VMEM),
        scratch_shapes=[
            pltpu.SMEM((3, count), jnp.int32),
            dma,
            vmem((planes, rows * 3, tiles * 2, 128), f32),
            vmem((64 * planes * tiles, 128), f32),
            vmem((planes + 2, 3, rows, wide), f32),
            vmem((planes + 2, 3, rows, wide), f32),
            vmem((planes + 1, 108, 8, plane), f32),
            vmem((4, 3, 16, wide), f32),
            vmem((4, 3, 16, wide), f32),
            vmem((8 * rows, planes * 3 * wide), low),
            vmem((planes * 3, rows, wide), low),
            vmem((16 * count, 3 * wide), low),
            vmem((16 * count, 3 * wide), low),
            vmem((count, 16, local_sites), low),
            vmem((count, 16, local_sites), low),
            vmem((halves, per_half * width, 8 * rows), f32),
            vmem((ships, 2, 4 * rows, width), low),
            vmem((ships, 4 * rows, width), low),
            vmem((ships, 4 * rows, width), low),
            vmem((ships, bricks, 2 * rows, width), low),
            vmem((2, halves, 2, 16, 3 * wide), low),
            vmem((halves, 2, 16, 3 * wide), low),
            vmem((32, plane), low),
            vmem((32, plane), low),
            dma((planes + 1,)),
            dma((2, halves, 2, 2)),
            dma((2,)),
            dma((7, 2)),
            dma((ships, 2)),
            dma((ships, 2)),
            dma((ships, bricks + 4)),
        ],
        compiler_params=pltpu.CompilerParams(
            vmem_limit_bytes=60 * 2**20, collective_id=0, has_side_effects=True
        ),
        name="elementals",
    )(momenta.T, v, g)
    out = pl.pallas_call(
        functools.partial(rows_kernel, (rows, count, ships, width)),
        out_shape=jax.ShapeDtypeStruct((rows * count * 2, rows), f32),
        in_specs=[pl.BlockSpec(memory_space=pltpu.VMEM)],
        out_specs=pl.BlockSpec(memory_space=pltpu.VMEM),
        name="rows",
    )(out)
    return out.reshape((rows, count, 2, rows))


def choose(vectors, gauge_links, momenta):
    plane = LY * LZ
    bricks, vecs, subs = (lax.axis_size(a) for a in ("brick", "vec", "sub"))
    rows, local_sites = vectors.shape[0], vectors.shape[3]
    fits = local_sites % plane == 0 and local_sites // plane == 4 and rows == 32
    if fits and vecs == 2 and subs == 2 and bricks == 4 and 24 <= momenta.shape[0] < 32:
        return shards_fused(vectors, gauge_links, momenta)
    return shards(vectors, gauge_links, momenta)


def solution(mesh):
    in_specs = (
        P(("vec", "sub"), None, None, ("grp", "brick")),
        P(None, None, None, None, ("grp", "brick")),
        P(),
    )
    out_specs = P(("vec", "sub"), "grp", None, "brick")
    return jax.shard_map(choose, mesh=mesh, in_specs=in_specs, out_specs=out_specs, check_vma=False)
```

```python
import functools
import math

import jax
import jax.numpy as jnp
from jax import lax
from jax.experimental import pallas as pl
from jax.experimental.pallas import tpu as pltpu
from jax.sharding import PartitionSpec as P

LY = 64
LZ = 8
ITERS = 2


KAPPA = 0.125


def from_behind(array, axis, by):
    peers = lax.axis_size(axis)
    return lax.ppermute(array, axis, [(i, (i + by) % peers) for i in range(peers)])


def padded_2(array, sides, width):
    for axis, dim in sides:
        peers, length = (lax.axis_size(axis), array.shape[dim])
        up = [(i, (i + 1) % peers) for i in range(peers)]
        down = [(j, i) for i, j in up]
        last = lax.slice_in_dim(array, length - width, length, axis=dim)
        initial = lax.slice_in_dim(array, 0, width, axis=dim)
        before = lax.ppermute(last, axis, up)
        after = lax.ppermute(initial, axis, down)
        array = jnp.concatenate([before, array, after], axis=dim)
    return array


def matrix_apply(matrix, source):
    matrix_real = matrix[:, :, 0][None]
    matrix_imag = matrix[:, :, 1][None]
    source_real = source[:, None, :, 0]
    source_imag = source[:, None, :, 1]
    real_part = jnp.sum(matrix_real * source_real - matrix_imag * source_imag, axis=2)
    imag_part = jnp.sum(matrix_real * source_imag + matrix_imag * source_real, axis=2)
    return jnp.stack([real_part, imag_part], axis=2)


def adjoint(matrix):
    return jnp.stack(
        [jnp.swapaxes(matrix[:, :, 0], 0, 1), -jnp.swapaxes(matrix[:, :, 1], 0, 1)], axis=2
    )


def step_depth(values, offset):
    depth_index = lax.iota(jnp.int32, values.shape[-1]) % LZ
    if offset > 0:
        return jnp.where(
            depth_index == LZ - 1, jnp.roll(values, LZ - 1, -1), jnp.roll(values, -1, -1)
        )
    return jnp.where(depth_index == 0, jnp.roll(values, 1 - LZ, -1), jnp.roll(values, 1, -1))


def step_column(values, offset):
    plane = LY * LZ
    column_index = lax.iota(jnp.int32, values.shape[-1]) // LZ % LY
    if offset > 0:
        return jnp.where(
            column_index == LY - 1, jnp.roll(values, plane - LZ, -1), jnp.roll(values, -LZ, -1)
        )
    return jnp.where(column_index == 0, jnp.roll(values, LZ - plane, -1), jnp.roll(values, LZ, -1))


def laplace_step(center, ahead, behind, here_links, back_links):
    forward = matrix_apply(here_links[0], ahead)
    backward = matrix_apply(adjoint(back_links), behind)
    total = forward + backward
    for direction, stepper in ((1, step_column), (2, step_depth)):
        forward = matrix_apply(here_links[direction], stepper(center, 1))
        backward = matrix_apply(adjoint(stepper(here_links[direction], -1)), stepper(center, -1))
        total = total + (forward + backward)
    return center + KAPPA * (total - 6.0 * center)


def shards(vectors, gauge_links, momenta):
    plane = LY * LZ
    local_sites = vectors.shape[3]
    raw_low = vectors.astype(jnp.bfloat16)
    field = vectors
    x_links = gauge_links[0]
    rim = from_behind(x_links[..., local_sites - plane :], "brick", 1)
    back_links = jnp.concatenate([rim, x_links[..., : local_sites - plane]], axis=3)
    for step in range(ITERS):
        padded = padded_2(field, (("brick", 3),), plane)
        field = laplace_step(
            padded[..., plane : plane + local_sites],
            padded[..., 2 * plane :],
            padded[..., :local_sites],
            gauge_links,
            back_links,
        )
    smeared_low = field.astype(jnp.bfloat16)
    raw_sites, smeared_sites = (
        lax.all_to_all(raw_low, ("vec", "sub"), split_axis=3, concat_axis=0, tiled=True),
        lax.all_to_all(smeared_low, ("vec", "sub"), split_axis=3, concat_axis=0, tiled=True),
    )
    groups = lax.axis_size(("vec", "sub"))
    total_vec = raw_sites.shape[0]
    width = raw_sites.shape[3]
    total_x = lax.axis_size("brick") * (local_sites // plane)
    first_site = lax.axis_index("brick") * local_sites + lax.axis_index(("vec", "sub")) * width
    site = first_site + lax.iota(jnp.int32, width)
    layer_index = (site // plane)[None]
    column_index = (site // LZ % LY)[None]
    depth_index = (site % LZ)[None]
    fraction = (
        jnp.mod(momenta[:, 0:1] * layer_index, total_x).astype(jnp.float32) / total_x
        + jnp.mod(momenta[:, 1:2] * column_index, LY).astype(jnp.float32) / LY
        + jnp.mod(momenta[:, 2:3] * depth_index, LZ).astype(jnp.float32) / LZ
    )
    angle = 2.0 * math.pi * fraction
    cosines = jnp.cos(angle)
    sines = jnp.sin(angle)
    right = smeared_sites.reshape((total_vec, 6 * width))
    scale = (3.0 * total_x * plane) ** (-0.5)

    def one_momentum(angles):
        cosine, sine = angles
        real_part = raw_sites[:, :, 0] * cosine - raw_sites[:, :, 1] * sine
        imag_part = raw_sites[:, :, 0] * sine + raw_sites[:, :, 1] * cosine
        phased = jnp.stack([real_part, imag_part], axis=2).astype(jnp.bfloat16)
        turned = jnp.stack([-phased[:, :, 1], phased[:, :, 0]], axis=2)
        left = jnp.concatenate(
            [
                phased.reshape((lax.axis_size(("vec", "sub")) * (total_vec // groups), 6 * width)),
                turned.reshape((lax.axis_size(("vec", "sub")) * (total_vec // groups), 6 * width)),
            ],
            axis=0,
        )
        product = lax.dot_general(
            left, right, (((1,), (1,)), ((), ())), preferred_element_type=jnp.float32
        )
        return product.reshape(
            (2, lax.axis_size(("vec", "sub")) * (total_vec // groups), total_vec)
        )

    blocks = lax.map(one_momentum, (cosines, sines))
    shares = lax.psum_scatter(
        jnp.transpose(blocks, (2, 0, 1, 3)) * scale, ("vec", "sub"), scatter_dimension=0, tiled=True
    )
    return lax.psum_scatter(shares, "brick", scatter_dimension=3, tiled=True)


def fused_kernel(plan, momenta_ref, v_ref, g_ref, out_ref, *scratch):
    (mom_ref, mom_sem, vst, gst, field0, field1, table, moved0, moved1, right, smeared, left0, left1, cosb, sinb, total, parted,
     crossing, rx, halo, hsend, lsend, lrecv, load_sem, halo_sem, link_sem, raw_sem, cross_sem, last_sem) = scratch
    planes, rows, count, bricks, ships, width, scale = plan
    fields, moved = (field0, field1), (moved0, moved1)
    halves = rows // 16
    plane = LY * LZ
    tiles = plane // 128
    all_tiles = planes * tiles
    f32, low = jnp.float32, jnp.bfloat16
    wide = 2 * plane
    last = planes - 1
    inner = list(range(1, last))
    outer = [0, last]
    position = {t: i for i, t in enumerate(inner + outer)}
    cut = len(inner) * 3 * wide
    span = planes * 3 * wide
    b, v, s = (lax.axis_index(a) for a in ("brick", "vec", "sub"))
    left = (left0, left1)

    def remote(src, dst, sems, **ids):
        return pltpu.make_async_remote_copy(
            src_ref=src, dst_ref=dst, send_sem=sems.at[0], recv_sem=sems.at[1],
            device_id=ids, device_id_type=pl.DeviceIdType.MESH,
        )

    loads = {}
    for t in outer + inner:
        loads[t] = pltpu.make_async_copy(v_ref.at[:, t], vst.at[t], load_sem.at[t])
        loads[t].start()
    load_links = pltpu.make_async_copy(g_ref, gst.at[pl.ds(0, 54 * all_tiles)], load_sem.at[planes])
    load_links.start()
    load_momenta = pltpu.make_async_copy(momenta_ref, mom_ref, mom_sem)
    load_momenta.start()
    barrier = pltpu.get_barrier_semaphore()
    for db in range(bricks):
        for ds in range(2):
            if db or ds:
                pl.semaphore_signal(
                    barrier, inc=1, device_id={"brick": (b + db) % bricks, "sub": (s + ds) % 2},
                    device_id_type=pl.DeviceIdType.MESH,
                )
    pl.semaphore_signal(
        barrier, inc=1, device_id={"vec": 1 - v}, device_id_type=pl.DeviceIdType.MESH
    )

    def unpack(t):
        flat = vst.at[t].reshape(rows * 3 * tiles * 2, 128)
        step = 3 * tiles * 2
        for c in range(3):
            for first in range(0, rows, 16):
                for part in range(2):
                    for lane in range(0, tiles, 2):
                        at = part * plane + lane * 128
                        quad = []
                        for h in range(2):
                            start = (first + 8 * h) * step + c * tiles * 2 + lane * 2 + part
                            quad.append(
                                jnp.concatenate(
                                    [flat[pl.ds(start + 2 * i, 8, stride=step), :] for i in range(2)], axis=1
                                )
                            )
                            field0[t + 1, c, first + 8 * h : first + 8 * h + 8, at : at + 256] = quad[h]
                        k = (position[t] * 3 + c) * wide + at
                        right[first : first + 16, k : k + 256] = jnp.concatenate(quad, axis=0).astype(low)

    def link_rows(t, part, group):
        return jnp.concatenate(
            [
                gst[pl.ds(group * 16 * all_tiles + (t * tiles + lane) * 2 + part, 8, stride=2 * all_tiles), :]
                for lane in range(tiles)
            ],
            axis=1,
        ) * KAPPA

    for t in outer:
        loads[t].wait()
        unpack(t)
    load_links.wait()
    for part in range(2):
        both = jnp.concatenate([link_rows(last, part, 0), link_rows(last, part, 1)], axis=0)
        lsend[16 * part : 16 * part + 16, :] = both.astype(low)
    pl.semaphore_wait(barrier, 2 * bricks)
    up, down = (b + 1) % bricks, (b + bricks - 1) % bricks

    def halos(step, h, low_src, high_src):
        sems = halo_sem.at[step, h]
        return (
            remote(high_src, halo.at[step, h, 0], sems.at[0], brick=up),
            remote(low_src, halo.at[step, h, 1], sems.at[1], brick=down),
        )

    def own(t, h):
        at = position[t] * 3 * wide
        return right.at[16 * h : 16 * h + 16, at : at + 3 * wide]

    copies = {}
    links_up = remote(lsend, lrecv, link_sem, brick=up)
    for h in range(halves):
        copies[0, h] = halos(0, h, own(0, h), own(last, h))
        copies[1, h] = halos(1, h, hsend.at[h, 0], hsend.at[h, 1])
        for copy in copies[0, h]:
            copy.start()
        if h == 0:
            links_up.start()
    for t in inner:
        loads[t].wait()
        unpack(t)
    parts = [slice(0, cut)] + [
        slice(cut + i * 3 * wide, cut + (i + 1) * 3 * wide) for i in range(2)
    ]
    unit = 2 * rows

    def raw_copy(index, from_slot, to_slot, ks, **ids):
        return remote(
            right.at[from_slot * unit : from_slot * unit + rows, ks],
            right.at[to_slot * unit : to_slot * unit + rows, ks],
            raw_sem.at[index], **ids,
        )

    across = [raw_copy(i, 0, 2, parts[i], vec=1 - v) for i in range(3)]
    beside = raw_copy(6, 0, 1, slice(0, span), sub=1 - s)
    onward = [raw_copy(3 + i, 2, 3, parts[i], sub=1 - s) for i in range(3)]
    for copy in across + [beside]:
        copy.start()

    depth_wide = lax.broadcasted_iota(jnp.int32, (8, plane), 1) % LZ
    depth = lax.broadcasted_iota(jnp.int32, (8, 128), 1) % LZ

    def spread(t, carry):
        for part in range(2):
            for group in range(4):
                here = link_rows(t, part, group)
                if group > 0:
                    by = pltpu.roll(here, LZ, 1)
                    bz = jnp.where(
                        depth_wide == 0, pltpu.roll(here, plane - (LZ - 1), 1), pltpu.roll(here, 1, 1)
                    )
                for j in range(min(8, 27 - 8 * group)):
                    index = group * 8 + j
                    row = jnp.broadcast_to(here[j : j + 1], (8, plane))
                    table[t, index * 2 + part] = row
                    if index < 9:
                        table[t + 1, 54 + index * 2 + part] = row
                    else:
                        back = by if index < 18 else bz
                        table[t, 54 + index * 2 + part] = jnp.broadcast_to(back[j : j + 1], (8, plane))
        return carry

    lax.fori_loop(0, planes, spread, 0)

    places = []
    for group in range(0, all_tiles, 8):
        height = min(8, all_tiles - group)
        site = (
            lax.broadcasted_iota(jnp.int32, (height, 128), 0) * 128
            + lax.broadcasted_iota(jnp.int32, (height, 128), 1)
            + group * 128
        )
        places.append(
            (
                (site // plane + b * planes).astype(f32) * (1.0 / (bricks * planes)),
                (site // LZ % LY).astype(f32) * (1.0 / LY),
                (site % LZ).astype(f32) * (1.0 / LZ),
            )
        )

    def phases(q, carry):
        n = [mom_ref[d, jnp.minimum(q, count - 1)].astype(f32) for d in range(3)]
        for group, (x, y, z) in enumerate(places):
            turns = n[0] * x + n[1] * y + n[2] * z
            half = jnp.round(2.0 * turns)
            sign = 1.0 - 2.0 * jnp.abs(half - 2.0 * jnp.round(0.5 * half))
            angle = (2.0 * math.pi) * (turns - 0.5 * half)
            square = angle * angle
            cosine, sine = 0.0, 0.0
            for i in range(7, 0, -1):
                cosine = (cosine * square) + (-1.0) ** i / math.factorial(2 * i)
            cosine = sign * (1.0 + cosine * square)
            for i in range(6, 0, -1):
                sine = (sine * square) + (-1.0) ** i / math.factorial(2 * i + 1)
            sine = sign * (angle + angle * (sine * square))
            for j in range(x.shape[0]):
                at = (group * 8 + j) * 128
                cosb[q, :, at : at + 128] = jnp.broadcast_to(cosine[j : j + 1], (16, 128)).astype(low)
                sinb[q, :, at : at + 128] = jnp.broadcast_to(sine[j : j + 1], (16, 128)).astype(low)
        return carry

    load_momenta.wait()
    lax.fori_loop(0, count, phases, 0)

    def shift(stage, k, to):
        step, t, h = stage
        rows_to = pl.ds(pl.multiple_of(k % 2 * 8, 8), 8)
        rows_at = pl.ds(pl.multiple_of(h * 16 + k % 2 * 8, 8), 8)
        first_lane = k // 2 * plane
        lanes = pl.ds(pl.multiple_of(first_lane, plane), plane)
        for c in range(3):
            w = fields[step][t + 1, c, rows_at, lanes]
            to[0, c, rows_to, lanes] = pltpu.roll(w, plane - LZ, 1)
            to[1, c, rows_to, lanes] = pltpu.roll(w, LZ, 1)
            for part in range(tiles):
                u = w[:, part * 128 : part * 128 + 128]
                here = pl.ds(pl.multiple_of(first_lane + part * 128, 128), 128)
                to[2, c, rows_to, here] = jnp.where(
                    depth == LZ - 1, pltpu.roll(u, LZ - 1, 1), pltpu.roll(u, 127, 1)
                )
                to[3, c, rows_to, here] = jnp.where(
                    depth == 0, pltpu.roll(u, 128 - (LZ - 1), 1), pltpu.roll(u, 1, 1)
                )

    def block(stage, lane, now):
        step, t, half = stage
        field = fields[step]
        lanes = (
            pl.ds(pl.multiple_of(lane * 128, 128), 128),
            pl.ds(pl.multiple_of(plane + lane * 128, 128), 128),
        )
        at_rows = [slice(half * 16 + 8 * h, half * 16 + 8 * h + 8) for h in range(2)]
        acc = {}
        for h in range(2):
            for r in range(3):
                for part in range(2):
                    mid = field[t + 1, r, at_rows[h], lanes[part]]
                    acc[h, r, part] = (1.0 - 6.0 * KAPPA) * mid
        for way in range(6):
            direction, back = way // 2, way % 2
            for c in range(3):
                sources = []
                for h in range(2):
                    if direction == 0:
                        p = t + 2 - 2 * back
                        sources.append([field[p, c, at_rows[h], lanes[i]] for i in range(2)])
                    else:
                        sources.append([now[way - 2, c, 8 * h : 8 * h + 8, lanes[i]] for i in range(2)])
                for r in range(3):
                    row = direction * 18 + (54 + c * 6 + r * 2 if back else r * 6 + c * 2)
                    ur = table[t, row, :, lanes[0]]
                    ui = table[t, row + 1, :, lanes[0]]
                    for h, (sr, si) in enumerate(sources):
                        if back:
                            acc[h, r, 0] = acc[h, r, 0] + (ur * sr + ui * si)
                            acc[h, r, 1] = acc[h, r, 1] + (ur * si - ui * sr)
                        else:
                            acc[h, r, 0] = acc[h, r, 0] + (ur * sr - ui * si)
                            acc[h, r, 1] = acc[h, r, 1] + (ur * si + ui * sr)
        both = slice(half * 16, half * 16 + 16)
        for r in range(3):
            for part in range(2):
                if step == 0:
                    for h in range(2):
                        field1[t + 1, r, at_rows[h], lanes[part]] = acc[h, r, part]
                if step == 1 or t in outer:
                    pair = jnp.concatenate([acc[0, r, part], acc[1, r, part]], axis=0).astype(low)
                    if step == 1:
                        smeared[position[t] * 3 + r, both, lanes[part]] = pair
                    else:
                        k_at = pl.ds(pl.multiple_of((2 * r + part) * plane + lane * 128, 128), 128)
                        hsend[half, outer.index(t), :, k_at] = pair

    stages = [(0, t, h) for h in range(halves) for t in inner]
    for h in range(halves):
        stages += [(0, t, h) for t in outer] + [(1, t, h) for t in inner]
    stages += [(1, t, h) for h in range(halves) for t in outer]

    def run(step, ts, h):
        for t in ts:
            i = stages.index((step, t, h))

            def trip(k, carry):
                shift(stages[(i + 1) % len(stages)], k, moved[(i + 1) % 2])
                block(stages[i], k, moved[i % 2])
                return carry

            lax.fori_loop(0, tiles, trip, 0)

    def begin(k, carry):
        shift(stages[0], k, moved[0])
        return carry

    lax.fori_loop(0, tiles, begin, 0)
    for h in range(halves):
        run(0, inner, h)

    def take(step, h, side):
        copies[step, h][side].wait_recv()
        for c in range(3):
            fields[step][planes + 1 if side else 0, c, 16 * h : 16 * h + 16] = (
                halo[step, h, side, :, c * wide : (c + 1) * wide].astype(f32)
            )

    links_up.wait_recv()
    for part in range(2):
        got = lrecv[16 * part : 16 * part + 16, :].astype(f32)
        for index in range(9):
            table[0, 54 + index * 2 + part] = jnp.broadcast_to(got[index : index + 1], (8, plane))
    for h in range(halves):
        for side in range(2):
            take(0, h, side)
            run(0, [outer[side]], h)
            copies[1, h][1 - side].start()
        if h == halves - 1:
            across[0].wait_recv()
            onward[0].start()
        run(1, inner, h)
    beside.wait_recv()
    onward[0].wait_recv()

    def fill(k, carry):
        re = pl.ds(pl.multiple_of(k * wide, wide), plane)
        im = pl.ds(pl.multiple_of(k * wide + plane, plane), plane)
        for slot in range(4):
            at_raw = slice(slot * unit, slot * unit + rows)
            at_turned = slice(slot * unit + rows, (slot + 1) * unit)
            right[at_turned, re] = -right[at_raw, im]
            right[at_turned, im] = right[at_raw, re]
        return carry

    members = (inner, outer)
    streamed = 16 * count
    per_half, used, spare, sizes = pieces_of(count, halves, ships, width)
    order = [(h, half, t) for half in range(2) for h in range(halves) for t in members[half]]
    per = width // 16

    def ready(i):
        return order[i][1] == 0 or order[i][2] != outer[0]

    def turn(i):
        h, half, t = order[i]
        to = left[i % 2]
        for q in range(count):
            for lane in range(0, plane, 256):
                cosine = cosb[q, :, t * plane + lane : t * plane + lane + 256]
                sine = sinb[q, :, t * plane + lane : t * plane + lane + 256]
                for c in range(3):
                    k = position[t] * 3 + c
                    sr = smeared[k, 16 * h : 16 * h + 16, lane : lane + 256]
                    si = smeared[k, 16 * h : 16 * h + 16, plane + lane : plane + lane + 256]
                    col = c * wide + lane
                    to[16 * q : 16 * q + 16, col : col + 256] = cosine * sr + sine * si
                    to[16 * q : 16 * q + 16, col + plane : col + plane + 256] = cosine * si - sine * sr

    def product(i, start=0, stop=streamed, ahead=True):
        h, half, t = order[i]
        first = position[t] * 3 * wide
        length = 3 * wide
        pieces = []
        for k in range(0, length, length // 2):
            pieces.append(
                lax.dot_general(
                    left[i % 2][start:stop, k : k + length // 2],
                    right[:, first + k : first + k + length // 2],
                    (((1,), (1,)), ((), ())), preferred_element_type=f32,
                )
            )
        if ahead and i + 1 < len(order) and ready(i + 1):
            turn(i + 1)
        part = pieces[0] * scale + pieces[1] * scale
        if t == inner[0]:
            total[h, start:stop] = part
        else:
            total[h, start:stop] += part

    def finish(e):
        at = e % per_half * width
        part = total[e // per_half, at : at + sizes[e], :].T.astype(low)
        parted[e, 0, :, 0 : sizes[e]] = part[0 : 2 * unit]
        crossing[e, :, 0 : sizes[e]] = part[2 * unit :]

    roots = (v * 2 + s, (1 - v) * 2 + s)

    def cross(e):
        return remote(
            crossing.at[e, :, 0 : sizes[e]], parted.at[e, 1, :, 0 : sizes[e]], cross_sem.at[e], vec=1 - v
        )

    def ends(e, hop, ds):
        src = parted.at[e, hop, ds * unit : (ds + 1) * unit, 0 : sizes[e]]
        return src, rx.at[e, b, :, 0 : sizes[e]]

    def far(e, hop, ds):
        src, dst = ends(e, hop, ds)
        return pltpu.make_async_remote_copy(
            src_ref=src, dst_ref=dst,
            send_sem=last_sem.at[e, bricks + hop * 2 + ds], recv_sem=last_sem.at[e, b],
            device_id={"brick": roots[hop], "sub": (s + ds) % 2}, device_id_type=pl.DeviceIdType.MESH,
        )

    def depart(e, hop):
        far(e, hop, 1).start()

        @pl.when(roots[hop] != b)
        def _():
            far(e, hop, 0).start()

        @pl.when(roots[hop] == b)
        def _():
            src, dst = ends(e, hop, 0)
            pltpu.make_async_copy(src, dst, last_sem.at[e, b]).start()

    def ship(e):
        finish(e)
        cross(e).start()
        depart(e, 0)

    def hand_on(e):
        cross(e).wait_recv()
        depart(e, 1)

    def arrive(e):
        for i in range(bricks):
            dst = rx.at[e, i, :, 0 : sizes[e]]
            pltpu.make_async_copy(dst, dst, last_sem.at[e, i]).wait()

    def fill_half(half):
        first = len(inner) * 3 if half else 0
        count_k = len(members[half]) * 3
        lax.fori_loop(first, first + count_k, fill, 0)

    for i, (h, half, t) in enumerate(order):
        opens = t == members[half][0]
        if i == 0:
            fill_half(0)
        if half and opens:
            if h == 0:
                for part in (1, 2):
                    across[part].wait_recv()
                    onward[part].start()
            for side in range(2):
                take(1, h, side)
                run(1, [outer[side]], h)
            if h == 0:
                for part in (1, 2):
                    onward[part].wait_recv()
                fill_half(1)
            else:
                for e in range(per_half * (h - 1), per_half * h):
                    hand_on(e)
        if i == 0 or not ready(i):
            turn(i)
        if half and h == halves - 1:
            if opens:
                for e in range(per_half):
                    start, stop = e * width, min((e + 1) * width, streamed)
                    product(i, start, stop, e == 0)
                    product(i + 1, start, stop, False)
                    if e == per_half - 1:
                        total[h, streamed : streamed + 16 * spare] = total[0, 16 * (count - spare) : streamed]
                    ship(per_half * h + e)
            continue
        product(i)
        if half and not opens:
            for e in range(per_half * h, per_half * (h + 1)):
                ship(e)
    for e in range(per_half * (halves - 1), ships):
        hand_on(e)
    for e in [i * per_half + j for j in range(per_half) for i in range(halves)]:
        arrive(e)
        got = [rx[e, i, :, 0 : sizes[e]].astype(f32) for i in range(bricks)]
        out_ref[:, e * width : e * width + sizes[e]] = (got[0] + got[1]) + (got[2] + got[3])
    sent = [links_up, *across, beside, *onward]
    for copy in copies.values():
        sent += copy
    sent += [cross(e) for e in range(ships)]
    for copy in sent:
        copy.wait_send()
    for e in range(ships):
        for hop in range(2):
            far(e, hop, 1).wait_send()

            @pl.when(roots[hop] != b)
            def _():
                far(e, hop, 0).wait_send()


def pieces_of(count, halves, ships, width):
    per_half = ships // halves
    used = 16 * count - (per_half - 1) * width
    spare = used % 128 // 16
    if used + 16 * spare > width:
        spare = 0
    sizes = [width] * ships
    if spare and used - 16 * spare:
        sizes[per_half - 1] = used - 16 * spare
    return per_half, used, spare, sizes


def rows_kernel(plan, sums_ref, out_ref):
    rows, count, ships, width = plan
    halves, unit = rows // 16, 2 * rows
    per = width // 16
    per_half, used, spare, _ = pieces_of(count, halves, ships, width)
    lane_at = lax.broadcasted_iota(jnp.int32, (8, 128), 1)
    for q in range(count):
        for first in range(0, unit, 8):
            pieces = []
            for h in range(halves):
                e, at = h * per_half + q // per, q % per * 16
                if h == 0 and q >= count - spare:
                    e, at = ships - 1, used + 16 * (q - count + spare)
                tile = e * width + at // 128 * 128
                got = sums_ref[first : first + 8, tile : tile + 128]
                turned = (16 * h - at) % 128
                pieces.append(pltpu.roll(got, turned, 1) if turned else got)
            value = jnp.where(lane_at < 16, pieces[0], pieces[1])
            start = (first % rows) * 2 * count + 2 * q + first // rows
            out_ref[pl.ds(start, 8, stride=2 * count), :] = value[:, 0:rows]


def shards_fused(vectors, gauge_links, momenta):
    plane = LY * LZ
    rows, local_sites = vectors.shape[0], vectors.shape[3]
    planes = local_sites // plane
    tiles = plane // 128
    bricks = lax.axis_size("brick")
    count = momenta.shape[0]
    halves = rows // 16
    width = 256
    per_half = -(-count * 16 // width)
    ships = halves * per_half
    low, f32 = jnp.bfloat16, jnp.float32
    v = vectors.reshape((rows, 3, 2, planes * tiles, 128)).transpose((0, 1, 3, 2, 4))
    v = v.reshape((rows * 3, planes, tiles * 2, 128))
    g = gauge_links.reshape((27, 2, planes * tiles, 128)).transpose((0, 2, 1, 3))
    g = g.reshape((54 * planes * tiles, 128))
    wide = 2 * plane
    scale = (3.0 * bricks * local_sites) ** (-0.5)
    vmem, dma = pltpu.VMEM, pltpu.SemaphoreType.DMA
    plan = (planes, rows, count, bricks, ships, width, scale)
    out = pl.pallas_call(
        functools.partial(fused_kernel, plan),
        out_shape=jax.ShapeDtypeStruct((2 * rows, ships * width), f32),
        in_specs=[
            pl.BlockSpec(memory_space=pl.ANY),
            pl.BlockSpec(memory_space=pl.ANY),
            pl.BlockSpec(memory_space=pl.ANY),
        ],
        out_specs=pl.BlockSpec(memory_space=pltpu.VMEM),
        scratch_shapes=[
            pltpu.SMEM((3, count), jnp.int32),
            dma,
            vmem((planes, rows * 3, tiles * 2, 128), f32),
            vmem((64 * planes * tiles, 128), f32),
            vmem((planes + 2, 3, rows, wide), f32),
            vmem((planes + 2, 3, rows, wide), f32),
            vmem((planes + 1, 108, 8, plane), f32),
            vmem((4, 3, 16, wide), f32),
            vmem((4, 3, 16, wide), f32),
            vmem((8 * rows, planes * 3 * wide), low),
            vmem((planes * 3, rows, wide), low),
            vmem((16 * count, 3 * wide), low),
            vmem((16 * count, 3 * wide), low),
            vmem((count, 16, local_sites), low),
            vmem((count, 16, local_sites), low),
            vmem((halves, per_half * width, 8 * rows), f32),
            vmem((ships, 2, 4 * rows, width), low),
            vmem((ships, 4 * rows, width), low),
            vmem((ships, bricks, 2 * rows, width), low),
            vmem((2, halves, 2, 16, 3 * wide), low),
            vmem((halves, 2, 16, 3 * wide), low),
            vmem((32, plane), low),
            vmem((32, plane), low),
            dma((planes + 1,)),
            dma((2, halves, 2, 2)),
            dma((2,)),
            dma((7, 2)),
            dma((ships, 2)),
            dma((ships, bricks + 4)),
        ],
        compiler_params=pltpu.CompilerParams(
            vmem_limit_bytes=60 * 2**20, collective_id=0, has_side_effects=True
        ),
        name="elementals",
    )(momenta.T, v, g)
    out = pl.pallas_call(
        functools.partial(rows_kernel, (rows, count, ships, width)),
        out_shape=jax.ShapeDtypeStruct((rows * count * 2, rows), f32),
        in_specs=[pl.BlockSpec(memory_space=pltpu.VMEM)],
        out_specs=pl.BlockSpec(memory_space=pltpu.VMEM),
        name="rows",
    )(out)
    return out.reshape((rows, count, 2, rows))


def choose(vectors, gauge_links, momenta):
    plane = LY * LZ
    bricks, vecs, subs = (lax.axis_size(a) for a in ("brick", "vec", "sub"))
    rows, local_sites = vectors.shape[0], vectors.shape[3]
    fits = local_sites % plane == 0 and local_sites // plane == 4 and rows == 32
    if fits and vecs == 2 and subs == 2 and bricks == 4 and 24 <= momenta.shape[0] < 32:
        return shards_fused(vectors, gauge_links, momenta)
    return shards(vectors, gauge_links, momenta)


def solution(mesh):
    in_specs = (
        P(("vec", "sub"), None, None, ("grp", "brick")),
        P(None, None, None, None, ("grp", "brick")),
        P(),
    )
    out_specs = P(("vec", "sub"), "grp", None, "brick")
    return jax.shard_map(choose, mesh=mesh, in_specs=in_specs, out_specs=out_specs, check_vma=False)
```

```python
import functools
import math

import jax
import jax.numpy as jnp
from jax import lax
from jax.experimental import pallas as pl
from jax.experimental.pallas import tpu as pltpu
from jax.sharding import PartitionSpec as P

LY = 64
LZ = 8
ITERS = 2


KAPPA = 0.125


def from_behind(array, axis, by):
    peers = lax.axis_size(axis)
    return lax.ppermute(array, axis, [(i, (i + by) % peers) for i in range(peers)])


def padded_2(array, sides, width):
    for axis, dim in sides:
        peers, length = (lax.axis_size(axis), array.shape[dim])
        up = [(i, (i + 1) % peers) for i in range(peers)]
        down = [(j, i) for i, j in up]
        last = lax.slice_in_dim(array, length - width, length, axis=dim)
        initial = lax.slice_in_dim(array, 0, width, axis=dim)
        before = lax.ppermute(last, axis, up)
        after = lax.ppermute(initial, axis, down)
        array = jnp.concatenate([before, array, after], axis=dim)
    return array


def matrix_apply(matrix, source):
    matrix_real = matrix[:, :, 0][None]
    matrix_imag = matrix[:, :, 1][None]
    source_real = source[:, None, :, 0]
    source_imag = source[:, None, :, 1]
    real_part = jnp.sum(matrix_real * source_real - matrix_imag * source_imag, axis=2)
    imag_part = jnp.sum(matrix_real * source_imag + matrix_imag * source_real, axis=2)
    return jnp.stack([real_part, imag_part], axis=2)


def adjoint(matrix):
    return jnp.stack(
        [jnp.swapaxes(matrix[:, :, 0], 0, 1), -jnp.swapaxes(matrix[:, :, 1], 0, 1)], axis=2
    )


def step_depth(values, offset):
    depth_index = lax.iota(jnp.int32, values.shape[-1]) % LZ
    if offset > 0:
        return jnp.where(
            depth_index == LZ - 1, jnp.roll(values, LZ - 1, -1), jnp.roll(values, -1, -1)
        )
    return jnp.where(depth_index == 0, jnp.roll(values, 1 - LZ, -1), jnp.roll(values, 1, -1))


def step_column(values, offset):
    plane = LY * LZ
    column_index = lax.iota(jnp.int32, values.shape[-1]) // LZ % LY
    if offset > 0:
        return jnp.where(
            column_index == LY - 1, jnp.roll(values, plane - LZ, -1), jnp.roll(values, -LZ, -1)
        )
    return jnp.where(column_index == 0, jnp.roll(values, LZ - plane, -1), jnp.roll(values, LZ, -1))


def laplace_step(center, ahead, behind, here_links, back_links):
    forward = matrix_apply(here_links[0], ahead)
    backward = matrix_apply(adjoint(back_links), behind)
    total = forward + backward
    for direction, stepper in ((1, step_column), (2, step_depth)):
        forward = matrix_apply(here_links[direction], stepper(center, 1))
        backward = matrix_apply(adjoint(stepper(here_links[direction], -1)), stepper(center, -1))
        total = total + (forward + backward)
    return center + KAPPA * (total - 6.0 * center)


def shards(vectors, gauge_links, momenta):
    plane = LY * LZ
    local_sites = vectors.shape[3]
    raw_low = vectors.astype(jnp.bfloat16)
    field = vectors
    x_links = gauge_links[0]
    rim = from_behind(x_links[..., local_sites - plane :], "brick", 1)
    back_links = jnp.concatenate([rim, x_links[..., : local_sites - plane]], axis=3)
    for step in range(ITERS):
        padded = padded_2(field, (("brick", 3),), plane)
        field = laplace_step(
            padded[..., plane : plane + local_sites],
            padded[..., 2 * plane :],
            padded[..., :local_sites],
            gauge_links,
            back_links,
        )
    smeared_low = field.astype(jnp.bfloat16)
    raw_sites, smeared_sites = (
        lax.all_to_all(raw_low, ("vec", "sub"), split_axis=3, concat_axis=0, tiled=True),
        lax.all_to_all(smeared_low, ("vec", "sub"), split_axis=3, concat_axis=0, tiled=True),
    )
    groups = lax.axis_size(("vec", "sub"))
    total_vec = raw_sites.shape[0]
    width = raw_sites.shape[3]
    total_x = lax.axis_size("brick") * (local_sites // plane)
    first_site = lax.axis_index("brick") * local_sites + lax.axis_index(("vec", "sub")) * width
    site = first_site + lax.iota(jnp.int32, width)
    layer_index = (site // plane)[None]
    column_index = (site // LZ % LY)[None]
    depth_index = (site % LZ)[None]
    fraction = (
        jnp.mod(momenta[:, 0:1] * layer_index, total_x).astype(jnp.float32) / total_x
        + jnp.mod(momenta[:, 1:2] * column_index, LY).astype(jnp.float32) / LY
        + jnp.mod(momenta[:, 2:3] * depth_index, LZ).astype(jnp.float32) / LZ
    )
    angle = 2.0 * math.pi * fraction
    cosines = jnp.cos(angle)
    sines = jnp.sin(angle)
    right = smeared_sites.reshape((total_vec, 6 * width))
    scale = (3.0 * total_x * plane) ** (-0.5)

    def one_momentum(angles):
        cosine, sine = angles
        real_part = raw_sites[:, :, 0] * cosine - raw_sites[:, :, 1] * sine
        imag_part = raw_sites[:, :, 0] * sine + raw_sites[:, :, 1] * cosine
        phased = jnp.stack([real_part, imag_part], axis=2).astype(jnp.bfloat16)
        turned = jnp.stack([-phased[:, :, 1], phased[:, :, 0]], axis=2)
        left = jnp.concatenate(
            [
                phased.reshape((lax.axis_size(("vec", "sub")) * (total_vec // groups), 6 * width)),
                turned.reshape((lax.axis_size(("vec", "sub")) * (total_vec // groups), 6 * width)),
            ],
            axis=0,
        )
        product = lax.dot_general(
            left, right, (((1,), (1,)), ((), ())), preferred_element_type=jnp.float32
        )
        return product.reshape(
            (2, lax.axis_size(("vec", "sub")) * (total_vec // groups), total_vec)
        )

    blocks = lax.map(one_momentum, (cosines, sines))
    shares = lax.psum_scatter(
        jnp.transpose(blocks, (2, 0, 1, 3)) * scale, ("vec", "sub"), scatter_dimension=0, tiled=True
    )
    return lax.psum_scatter(shares, "brick", scatter_dimension=3, tiled=True)


def fused_kernel(plan, momenta_ref, v_ref, g_ref, out_ref, *scratch):
    (mom_ref, mom_sem, vst, gst, field0, field1, table, moved0, moved1, right, smeared, left0, left1, cosb, sinb, total, parted,
     crossing, rx, halo, hsend, lsend, lrecv, load_sem, halo_sem, link_sem, raw_sem, cross_sem, last_sem) = scratch
    planes, rows, count, bricks, ships, width, scale = plan
    fields, moved = (field0, field1), (moved0, moved1)
    halves = rows // 16
    plane = LY * LZ
    tiles = plane // 128
    all_tiles = planes * tiles
    f32, low = jnp.float32, jnp.bfloat16
    wide = 2 * plane
    last = planes - 1
    inner = list(range(1, last))
    outer = [0, last]
    position = {t: i for i, t in enumerate(inner + outer)}
    cut = len(inner) * 3 * wide
    span = planes * 3 * wide
    b, v, s = (lax.axis_index(a) for a in ("brick", "vec", "sub"))
    left = (left0, left1)

    def remote(src, dst, sems, **ids):
        return pltpu.make_async_remote_copy(
            src_ref=src, dst_ref=dst, send_sem=sems.at[0], recv_sem=sems.at[1],
            device_id=ids, device_id_type=pl.DeviceIdType.MESH,
        )

    loads = {}
    for t in outer + inner:
        loads[t] = pltpu.make_async_copy(v_ref.at[:, t], vst.at[t], load_sem.at[t])
        loads[t].start()
    load_links = pltpu.make_async_copy(g_ref, gst.at[pl.ds(0, 54 * all_tiles)], load_sem.at[planes])
    load_links.start()
    load_momenta = pltpu.make_async_copy(momenta_ref, mom_ref, mom_sem)
    load_momenta.start()
    barrier = pltpu.get_barrier_semaphore()
    for db in range(bricks):
        for ds in range(2):
            if db or ds:
                pl.semaphore_signal(
                    barrier, inc=1, device_id={"brick": (b + db) % bricks, "sub": (s + ds) % 2},
                    device_id_type=pl.DeviceIdType.MESH,
                )
    pl.semaphore_signal(
        barrier, inc=1, device_id={"vec": 1 - v}, device_id_type=pl.DeviceIdType.MESH
    )

    def unpack(t):
        flat = vst.at[t].reshape(rows * 3 * tiles * 2, 128)
        step = 3 * tiles * 2
        for c in range(3):
            for first in range(0, rows, 16):
                for part in range(2):
                    for lane in range(0, tiles, 2):
                        at = part * plane + lane * 128
                        quad = []
                        for h in range(2):
                            start = (first + 8 * h) * step + c * tiles * 2 + lane * 2 + part
                            quad.append(
                                jnp.concatenate(
                                    [flat[pl.ds(start + 2 * i, 8, stride=step), :] for i in range(2)], axis=1
                                )
                            )
                            field0[t + 1, c, first + 8 * h : first + 8 * h + 8, at : at + 256] = quad[h]
                        k = (position[t] * 3 + c) * wide + at
                        right[first : first + 16, k : k + 256] = jnp.concatenate(quad, axis=0).astype(low)

    def link_rows(t, part, group):
        return jnp.concatenate(
            [
                gst[pl.ds(group * 16 * all_tiles + (t * tiles + lane) * 2 + part, 8, stride=2 * all_tiles), :]
                for lane in range(tiles)
            ],
            axis=1,
        ) * KAPPA

    for t in outer:
        loads[t].wait()
        unpack(t)
    load_links.wait()
    for part in range(2):
        both = jnp.concatenate([link_rows(last, part, 0), link_rows(last, part, 1)], axis=0)
        lsend[16 * part : 16 * part + 16, :] = both.astype(low)
    pl.semaphore_wait(barrier, 2 * bricks)
    up, down = (b + 1) % bricks, (b + bricks - 1) % bricks

    def halos(step, h, low_src, high_src):
        sems = halo_sem.at[step, h]
        return (
            remote(high_src, halo.at[step, h, 0], sems.at[0], brick=up),
            remote(low_src, halo.at[step, h, 1], sems.at[1], brick=down),
        )

    def own(t, h):
        at = position[t] * 3 * wide
        return right.at[16 * h : 16 * h + 16, at : at + 3 * wide]

    copies = {}
    links_up = remote(lsend, lrecv, link_sem, brick=up)
    for h in range(halves):
        copies[0, h] = halos(0, h, own(0, h), own(last, h))
        copies[1, h] = halos(1, h, hsend.at[h, 0], hsend.at[h, 1])
        for copy in copies[0, h]:
            copy.start()
        if h == 0:
            links_up.start()
    for t in inner:
        loads[t].wait()
        unpack(t)
    parts = [slice(0, cut)] + [
        slice(cut + i * 3 * wide, cut + (i + 1) * 3 * wide) for i in range(2)
    ]
    unit = 2 * rows

    def raw_copy(index, from_slot, to_slot, ks, **ids):
        return remote(
            right.at[from_slot * unit : from_slot * unit + rows, ks],
            right.at[to_slot * unit : to_slot * unit + rows, ks],
            raw_sem.at[index], **ids,
        )

    across = [raw_copy(i, 0, 2, parts[i], vec=1 - v) for i in range(3)]
    beside = raw_copy(6, 0, 1, slice(0, span), sub=1 - s)
    onward = [raw_copy(3 + i, 2, 3, parts[i], sub=1 - s) for i in range(3)]
    for copy in across + [beside]:
        copy.start()

    depth_wide = lax.broadcasted_iota(jnp.int32, (8, plane), 1) % LZ
    depth = lax.broadcasted_iota(jnp.int32, (8, 128), 1) % LZ

    def spread(t, carry):
        for part in range(2):
            for group in range(4):
                here = link_rows(t, part, group)
                if group > 0:
                    by = pltpu.roll(here, LZ, 1)
                    bz = jnp.where(
                        depth_wide == 0, pltpu.roll(here, plane - (LZ - 1), 1), pltpu.roll(here, 1, 1)
                    )
                for j in range(min(8, 27 - 8 * group)):
                    index = group * 8 + j
                    row = jnp.broadcast_to(here[j : j + 1], (8, plane))
                    table[t, index * 2 + part] = row
                    if index < 9:
                        table[t + 1, 54 + index * 2 + part] = row
                    else:
                        back = by if index < 18 else bz
                        table[t, 54 + index * 2 + part] = jnp.broadcast_to(back[j : j + 1], (8, plane))
        return carry

    lax.fori_loop(0, planes, spread, 0)

    places = []
    for group in range(0, all_tiles, 8):
        height = min(8, all_tiles - group)
        site = (
            lax.broadcasted_iota(jnp.int32, (height, 128), 0) * 128
            + lax.broadcasted_iota(jnp.int32, (height, 128), 1)
            + group * 128
        )
        places.append(
            (
                (site // plane + b * planes).astype(f32) * (1.0 / (bricks * planes)),
                (site // LZ % LY).astype(f32) * (1.0 / LY),
                (site % LZ).astype(f32) * (1.0 / LZ),
            )
        )

    def phases(q, carry):
        n = [mom_ref[d, jnp.minimum(q, count - 1)].astype(f32) for d in range(3)]
        for group, (x, y, z) in enumerate(places):
            turns = n[0] * x + n[1] * y + n[2] * z
            half = jnp.round(2.0 * turns)
            sign = 1.0 - 2.0 * jnp.abs(half - 2.0 * jnp.round(0.5 * half))
            angle = (2.0 * math.pi) * (turns - 0.5 * half)
            square = angle * angle
            cosine, sine = 0.0, 0.0
            for i in range(7, 0, -1):
                cosine = (cosine * square) + (-1.0) ** i / math.factorial(2 * i)
            cosine = sign * (1.0 + cosine * square)
            for i in range(6, 0, -1):
                sine = (sine * square) + (-1.0) ** i / math.factorial(2 * i + 1)
            sine = sign * (angle + angle * (sine * square))
            for j in range(x.shape[0]):
                at = (group * 8 + j) * 128
                cosb[q, :, at : at + 128] = jnp.broadcast_to(cosine[j : j + 1], (16, 128)).astype(low)
                sinb[q, :, at : at + 128] = jnp.broadcast_to(sine[j : j + 1], (16, 128)).astype(low)
        return carry

    load_momenta.wait()
    lax.fori_loop(0, count, phases, 0)

    def shift(stage, k, to):
        step, t, h = stage
        rows_to = pl.ds(pl.multiple_of(k % 2 * 8, 8), 8)
        rows_at = pl.ds(pl.multiple_of(h * 16 + k % 2 * 8, 8), 8)
        first_lane = k // 2 * plane
        lanes = pl.ds(pl.multiple_of(first_lane, plane), plane)
        for c in range(3):
            w = fields[step][t + 1, c, rows_at, lanes]
            to[0, c, rows_to, lanes] = pltpu.roll(w, plane - LZ, 1)
            to[1, c, rows_to, lanes] = pltpu.roll(w, LZ, 1)
            for part in range(tiles):
                u = w[:, part * 128 : part * 128 + 128]
                here = pl.ds(pl.multiple_of(first_lane + part * 128, 128), 128)
                to[2, c, rows_to, here] = jnp.where(
                    depth == LZ - 1, pltpu.roll(u, LZ - 1, 1), pltpu.roll(u, 127, 1)
                )
                to[3, c, rows_to, here] = jnp.where(
                    depth == 0, pltpu.roll(u, 128 - (LZ - 1), 1), pltpu.roll(u, 1, 1)
                )

    def block(stage, lane, now):
        step, t, half = stage
        field = fields[step]
        lanes = (
            pl.ds(pl.multiple_of(lane * 128, 128), 128),
            pl.ds(pl.multiple_of(plane + lane * 128, 128), 128),
        )
        at_rows = [slice(half * 16 + 8 * h, half * 16 + 8 * h + 8) for h in range(2)]
        acc = {}
        for h in range(2):
            for r in range(3):
                for part in range(2):
                    mid = field[t + 1, r, at_rows[h], lanes[part]]
                    acc[h, r, part] = (1.0 - 6.0 * KAPPA) * mid
        for way in range(6):
            direction, back = way // 2, way % 2
            for c in range(3):
                sources = []
                for h in range(2):
                    if direction == 0:
                        p = t + 2 - 2 * back
                        sources.append([field[p, c, at_rows[h], lanes[i]] for i in range(2)])
                    else:
                        sources.append([now[way - 2, c, 8 * h : 8 * h + 8, lanes[i]] for i in range(2)])
                for r in range(3):
                    row = direction * 18 + (54 + c * 6 + r * 2 if back else r * 6 + c * 2)
                    ur = table[t, row, :, lanes[0]]
                    ui = table[t, row + 1, :, lanes[0]]
                    for h, (sr, si) in enumerate(sources):
                        if back:
                            acc[h, r, 0] = acc[h, r, 0] + (ur * sr + ui * si)
                            acc[h, r, 1] = acc[h, r, 1] + (ur * si - ui * sr)
                        else:
                            acc[h, r, 0] = acc[h, r, 0] + (ur * sr - ui * si)
                            acc[h, r, 1] = acc[h, r, 1] + (ur * si + ui * sr)
        both = slice(half * 16, half * 16 + 16)
        for r in range(3):
            for part in range(2):
                if step == 0:
                    for h in range(2):
                        field1[t + 1, r, at_rows[h], lanes[part]] = acc[h, r, part]
                if step == 1 or t in outer:
                    pair = jnp.concatenate([acc[0, r, part], acc[1, r, part]], axis=0).astype(low)
                    if step == 1:
                        smeared[position[t] * 3 + r, both, lanes[part]] = pair
                    else:
                        k_at = pl.ds(pl.multiple_of((2 * r + part) * plane + lane * 128, 128), 128)
                        hsend[half, outer.index(t), :, k_at] = pair

    stages = [(0, t, h) for h in range(halves) for t in inner]
    for h in range(halves):
        stages += [(0, t, h) for t in outer] + [(1, t, h) for t in inner]
    stages += [(1, t, h) for h in range(halves) for t in outer]

    def run(step, ts, h):
        for t in ts:
            i = stages.index((step, t, h))

            def trip(k, carry):
                shift(stages[(i + 1) % len(stages)], k, moved[(i + 1) % 2])
                block(stages[i], k, moved[i % 2])
                return carry

            lax.fori_loop(0, tiles, trip, 0)

    def begin(k, carry):
        shift(stages[0], k, moved[0])
        return carry

    lax.fori_loop(0, tiles, begin, 0)
    for h in range(halves):
        run(0, inner, h)

    def take(step, h, side):
        copies[step, h][side].wait_recv()
        for c in range(3):
            fields[step][planes + 1 if side else 0, c, 16 * h : 16 * h + 16] = (
                halo[step, h, side, :, c * wide : (c + 1) * wide].astype(f32)
            )

    links_up.wait_recv()
    for part in range(2):
        got = lrecv[16 * part : 16 * part + 16, :].astype(f32)
        for index in range(9):
            table[0, 54 + index * 2 + part] = jnp.broadcast_to(got[index : index + 1], (8, plane))
    for h in range(halves):
        for side in range(2):
            take(0, h, side)
            run(0, [outer[side]], h)
            copies[1, h][1 - side].start()
        if h == halves - 1:
            across[0].wait_recv()
            onward[0].start()
        run(1, inner, h)
    beside.wait_recv()
    onward[0].wait_recv()

    def fill(k, carry):
        re = pl.ds(pl.multiple_of(k * wide, wide), plane)
        im = pl.ds(pl.multiple_of(k * wide + plane, plane), plane)
        for slot in range(4):
            at_raw = slice(slot * unit, slot * unit + rows)
            at_turned = slice(slot * unit + rows, (slot + 1) * unit)
            right[at_turned, re] = -right[at_raw, im]
            right[at_turned, im] = right[at_raw, re]
        return carry

    members = (inner, outer)
    streamed = 16 * count
    per_half, used, spare, sizes = pieces_of(count, halves, ships, width)
    order = [(h, half, t) for half in range(2) for h in range(halves) for t in members[half]]
    per = width // 16

    def ready(i):
        return order[i][1] == 0 or order[i][2] != outer[0]

    def turn(i):
        h, half, t = order[i]
        to = left[i % 2]
        for q in range(count):
            for lane in range(0, plane, 256):
                cosine = cosb[q, :, t * plane + lane : t * plane + lane + 256]
                sine = sinb[q, :, t * plane + lane : t * plane + lane + 256]
                for c in range(3):
                    k = position[t] * 3 + c
                    sr = smeared[k, 16 * h : 16 * h + 16, lane : lane + 256]
                    si = smeared[k, 16 * h : 16 * h + 16, plane + lane : plane + lane + 256]
                    col = c * wide + lane
                    to[16 * q : 16 * q + 16, col : col + 256] = cosine * sr + sine * si
                    to[16 * q : 16 * q + 16, col + plane : col + plane + 256] = cosine * si - sine * sr

    def product(i, start=0, stop=streamed, ahead=True):
        h, half, t = order[i]
        first = position[t] * 3 * wide
        length = 3 * wide
        pieces = []
        for k in range(0, length, length // 2):
            pieces.append(
                lax.dot_general(
                    left[i % 2][start:stop, k : k + length // 2],
                    right[:, first + k : first + k + length // 2],
                    (((1,), (1,)), ((), ())), preferred_element_type=f32,
                )
            )
        if ahead and i + 1 < len(order) and ready(i + 1):
            turn(i + 1)
        part = pieces[0] * scale + pieces[1] * scale
        if t == inner[0]:
            total[h, start:stop] = part
        else:
            total[h, start:stop] += part

    def finish(e):
        at = e % per_half * width
        part = total[e // per_half, at : at + sizes[e], :].T.astype(low)
        parted[e, 0, :, 0 : sizes[e]] = part[0 : 2 * unit]
        crossing[e, :, 0 : sizes[e]] = part[2 * unit :]

    roots = (v * 2 + s, (1 - v) * 2 + s)

    def cross(e):
        return remote(
            crossing.at[e, :, 0 : sizes[e]], parted.at[e, 1, :, 0 : sizes[e]], cross_sem.at[e], vec=1 - v
        )

    def ends(e, hop, ds):
        src = parted.at[e, hop, ds * unit : (ds + 1) * unit, 0 : sizes[e]]
        return src, rx.at[e, b, :, 0 : sizes[e]]

    def far(e, hop, ds):
        src, dst = ends(e, hop, ds)
        return pltpu.make_async_remote_copy(
            src_ref=src, dst_ref=dst,
            send_sem=last_sem.at[e, bricks + hop * 2 + ds], recv_sem=last_sem.at[e, b],
            device_id={"brick": roots[hop], "sub": (s + ds) % 2}, device_id_type=pl.DeviceIdType.MESH,
        )

    def depart(e, hop):
        far(e, hop, 1).start()

        @pl.when(roots[hop] != b)
        def _():
            far(e, hop, 0).start()

        @pl.when(roots[hop] == b)
        def _():
            src, dst = ends(e, hop, 0)
            pltpu.make_async_copy(src, dst, last_sem.at[e, b]).start()

    def ship(e):
        finish(e)
        cross(e).start()
        depart(e, 0)

    def hand_on(e):
        cross(e).wait_recv()
        depart(e, 1)

    def arrive(e):
        for i in range(bricks):
            dst = rx.at[e, i, :, 0 : sizes[e]]
            pltpu.make_async_copy(dst, dst, last_sem.at[e, i]).wait()

    def fill_half(half):
        first = len(inner) * 3 if half else 0
        count_k = len(members[half]) * 3
        lax.fori_loop(first, first + count_k, fill, 0)

    for i, (h, half, t) in enumerate(order):
        opens = t == members[half][0]
        if i == 0:
            fill_half(0)
        if half and opens:
            if h == 0:
                for part in (1, 2):
                    across[part].wait_recv()
                    onward[part].start()
            for side in range(2):
                take(1, h, side)
                run(1, [outer[side]], h)
            if h == 0:
                for part in (1, 2):
                    onward[part].wait_recv()
                fill_half(1)
        if i == 0 or not ready(i):
            turn(i)
        if half and h == halves - 1:
            if opens:
                for e in range(per_half):
                    start, stop = e * width, min((e + 1) * width, streamed)
                    product(i, start, stop, e == 0)
                    product(i + 1, start, stop, False)
                    if e == per_half - 1:
                        total[h, streamed : streamed + 16 * spare] = total[0, 16 * (count - spare) : streamed]
                    ship(per_half * h + e)
                    hand_on(per_half * (h - 1) + e)
            continue
        product(i)
        if half and not opens:
            for e in range(per_half * h, per_half * (h + 1)):
                ship(e)
    for e in range(per_half * (halves - 1), ships):
        hand_on(e)
    for e in [i * per_half + j for j in range(per_half) for i in range(halves)]:
        arrive(e)
        got = [rx[e, i, :, 0 : sizes[e]].astype(f32) for i in range(bricks)]
        out_ref[:, e * width : e * width + sizes[e]] = (got[0] + got[1]) + (got[2] + got[3])
    sent = [links_up, *across, beside, *onward]
    for copy in copies.values():
        sent += copy
    sent += [cross(e) for e in range(ships)]
    for copy in sent:
        copy.wait_send()
    for e in range(ships):
        for hop in range(2):
            far(e, hop, 1).wait_send()

            @pl.when(roots[hop] != b)
            def _():
                far(e, hop, 0).wait_send()


def pieces_of(count, halves, ships, width):
    per_half = ships // halves
    used = 16 * count - (per_half - 1) * width
    spare = used % 128 // 16
    if used + 16 * spare > width:
        spare = 0
    sizes = [width] * ships
    if spare and used - 16 * spare:
        sizes[per_half - 1] = used - 16 * spare
    return per_half, used, spare, sizes


def rows_kernel(plan, sums_ref, out_ref):
    rows, count, ships, width = plan
    halves, unit = rows // 16, 2 * rows
    per = width // 16
    per_half, used, spare, _ = pieces_of(count, halves, ships, width)
    lane_at = lax.broadcasted_iota(jnp.int32, (8, 128), 1)
    for q in range(count):
        for first in range(0, unit, 8):
            pieces = []
            for h in range(halves):
                e, at = h * per_half + q // per, q % per * 16
                if h == 0 and q >= count - spare:
                    e, at = ships - 1, used + 16 * (q - count + spare)
                tile = e * width + at // 128 * 128
                got = sums_ref[first : first + 8, tile : tile + 128]
                turned = (16 * h - at) % 128
                pieces.append(pltpu.roll(got, turned, 1) if turned else got)
            value = jnp.where(lane_at < 16, pieces[0], pieces[1])
            start = (first % rows) * 2 * count + 2 * q + first // rows
            out_ref[pl.ds(start, 8, stride=2 * count), :] = value[:, 0:rows]


def shards_fused(vectors, gauge_links, momenta):
    plane = LY * LZ
    rows, local_sites = vectors.shape[0], vectors.shape[3]
    planes = local_sites // plane
    tiles = plane // 128
    bricks = lax.axis_size("brick")
    count = momenta.shape[0]
    halves = rows // 16
    width = 256
    per_half = -(-count * 16 // width)
    ships = halves * per_half
    low, f32 = jnp.bfloat16, jnp.float32
    v = vectors.reshape((rows, 3, 2, planes * tiles, 128)).transpose((0, 1, 3, 2, 4))
    v = v.reshape((rows * 3, planes, tiles * 2, 128))
    g = gauge_links.reshape((27, 2, planes * tiles, 128)).transpose((0, 2, 1, 3))
    g = g.reshape((54 * planes * tiles, 128))
    wide = 2 * plane
    scale = (3.0 * bricks * local_sites) ** (-0.5)
    vmem, dma = pltpu.VMEM, pltpu.SemaphoreType.DMA
    plan = (planes, rows, count, bricks, ships, width, scale)
    out = pl.pallas_call(
        functools.partial(fused_kernel, plan),
        out_shape=jax.ShapeDtypeStruct((2 * rows, ships * width), f32),
        in_specs=[
            pl.BlockSpec(memory_space=pl.ANY),
            pl.BlockSpec(memory_space=pl.ANY),
            pl.BlockSpec(memory_space=pl.ANY),
        ],
        out_specs=pl.BlockSpec(memory_space=pltpu.VMEM),
        scratch_shapes=[
            pltpu.SMEM((3, count), jnp.int32),
            dma,
            vmem((planes, rows * 3, tiles * 2, 128), f32),
            vmem((64 * planes * tiles, 128), f32),
            vmem((planes + 2, 3, rows, wide), f32),
            vmem((planes + 2, 3, rows, wide), f32),
            vmem((planes + 1, 108, 8, plane), f32),
            vmem((4, 3, 16, wide), f32),
            vmem((4, 3, 16, wide), f32),
            vmem((8 * rows, planes * 3 * wide), low),
            vmem((planes * 3, rows, wide), low),
            vmem((16 * count, 3 * wide), low),
            vmem((16 * count, 3 * wide), low),
            vmem((count, 16, local_sites), low),
            vmem((count, 16, local_sites), low),
            vmem((halves, per_half * width, 8 * rows), f32),
            vmem((ships, 2, 4 * rows, width), low),
            vmem((ships, 4 * rows, width), low),
            vmem((ships, bricks, 2 * rows, width), low),
            vmem((2, halves, 2, 16, 3 * wide), low),
            vmem((halves, 2, 16, 3 * wide), low),
            vmem((32, plane), low),
            vmem((32, plane), low),
            dma((planes + 1,)),
            dma((2, halves, 2, 2)),
            dma((2,)),
            dma((7, 2)),
            dma((ships, 2)),
            dma((ships, bricks + 4)),
        ],
        compiler_params=pltpu.CompilerParams(
            vmem_limit_bytes=60 * 2**20, collective_id=0, has_side_effects=True
        ),
        name="elementals",
    )(momenta.T, v, g)
    out = pl.pallas_call(
        functools.partial(rows_kernel, (rows, count, ships, width)),
        out_shape=jax.ShapeDtypeStruct((rows * count * 2, rows), f32),
        in_specs=[pl.BlockSpec(memory_space=pltpu.VMEM)],
        out_specs=pl.BlockSpec(memory_space=pltpu.VMEM),
        name="rows",
    )(out)
    return out.reshape((rows, count, 2, rows))


def choose(vectors, gauge_links, momenta):
    plane = LY * LZ
    bricks, vecs, subs = (lax.axis_size(a) for a in ("brick", "vec", "sub"))
    rows, local_sites = vectors.shape[0], vectors.shape[3]
    fits = local_sites % plane == 0 and local_sites // plane == 4 and rows == 32
    if fits and vecs == 2 and subs == 2 and bricks == 4 and 24 <= momenta.shape[0] < 32:
        return shards_fused(vectors, gauge_links, momenta)
    return shards(vectors, gauge_links, momenta)


def solution(mesh):
    in_specs = (
        P(("vec", "sub"), None, None, ("grp", "brick")),
        P(None, None, None, None, ("grp", "brick")),
        P(),
    )
    out_specs = P(("vec", "sub"), "grp", None, "brick")
    return jax.shard_map(choose, mesh=mesh, in_specs=in_specs, out_specs=out_specs, check_vma=False)
```
